256 devices in a mesh: tm: 32 (over x_hi, z, core), space: 8 (over y, x_lo).
Axes of the slice: x: 4 (x_hi: 2, x_lo: 2; x = x_hi * 2 + x_lo), y: 4, z: 8, core: 2. Of those that a mesh axis runs over, the one named last changes fastest.
Arguments:
- state: bfloat16 [32, 128, 64, 128], P('tm', 'space'), may hold values from -4 to 4
- initial: bfloat16 [128, 64, 128], P('space'), may hold values from -4 to 4
- forcing: bfloat16 [32, 128, 64, 128], P('tm', 'space'), may hold values from -5 to 5
- kappa: bfloat16 [128, 64, 128], P('space'), may hold values from 0.5 to 2
- reaction: bfloat16 [128, 64, 128], P('space'), may hold values from 0.019897461 to 0.19921875
Outputs:
- updated: bfloat16 [32, 128, 64, 128], P('tm', 'space')
The draws below stay inside these ranges and needn't reach their ends.
All inputs are finite; a program needn't handle non-finite values.
Results may differ from the reference program's by a relative error of at most 0.006.
The reference program's roundings to bfloat16 on the way (of `previous`, `residual` and `correction`) count: a program that leaves them out, or rounds other values in their place, can miss the bound.
Values may be sent and summed in bfloat16 or wider, within the bound.
No kernel may reach another device: no remote copies, remote signals or barrier semaphores. Data moves between devices by JAX's collectives and lax.ppermute only.
A program may use at most 64 MiB of HBM per device.

```python
import math
import jax
import jax.numpy as jnp
from jax import lax

NY = 64
NZ = 128
SWEEPS = 6
STEPS = 32
NX = 128


def draw_forcing(key, part):
    rough = jnp.clip(jax.random.normal(key, (STEPS, NX, NY, NZ), jnp.float32), -4.0, 4.0)
    return rough.astype(jnp.bfloat16)


def levels(key, dims, pieces, smallest, largest):
    factor_of, own = 1.0, jax.random.fold_in(key, 6)
    for position, blocks in pieces:
        draws = jnp.exp(jax.random.uniform(jax.random.fold_in(own, position), (blocks,), jnp.float32, smallest / len(pieces), largest / len(pieces)))
        factor_of = factor_of * jnp.repeat(draws, dims[position] // blocks).reshape([-1 if axis == position else 1 for axis in range(len(dims))])
    return factor_of


def bell_draw(key, shape, width, most, cuts=(), held_as=jnp.bfloat16):
    drawn = width * jax.random.normal(key, shape, jnp.float32)
    if cuts:
        drawn = drawn * levels(key, shape, cuts, -0.22, 0.18)
    return jnp.clip(drawn, -most, most).astype(held_as)


def setup_inputs(seed: int = 0) -> dict:
    splits = jax.random.split(jax.random.key(seed), 6)
    state = bell_draw(splits[0], (STEPS, NX, NY, NZ), 1.0, 4.0, ((0, 32), (1, 8)))
    initial = bell_draw(splits[1], (NX, NY, NZ), 1.0, 4.0, ((0, 8),))
    forcing = draw_forcing(jax.random.fold_in(splits[5], 71), 0)
    kappa = jnp.clip(jnp.exp(math.log(2.0) - 1.3862944 * jax.random.uniform(splits[3], (NX, NY, NZ), jnp.float32) ** levels(splits[3], (NX, NY, NZ), ((0, 8),), -0.2, 0.2)), 0.5, 2.0).astype(jnp.bfloat16)
    reaction = jnp.clip(jnp.exp(math.log(0.19921875) - 2.3038113 * jax.random.uniform(splits[4], (NX, NY, NZ), jnp.float32) ** levels(splits[4], (NX, NY, NZ), ((0, 8),), -0.2, 0.2)), 0.019897461, 0.19921875).astype(jnp.bfloat16)
    return {"state": state, "initial": initial, "forcing": forcing, "kappa": kappa, "reaction": reaction}


alpha_ratio = 0.25
near_weight = 0.5
far_weight = 1.0
centre_weight = 6.0 * (near_weight + far_weight)
highest = lax.Precision.HIGHEST


def shifted(values, axis_number, offset):
    extent = values.shape[axis_number]
    widths = [(0, 0)] * values.ndim
    widths[axis_number] = (2, 2)
    padded = jnp.pad(values, widths)
    return lax.slice_in_dim(padded, 2 + offset, 2 + offset + extent, axis=axis_number)


def cycle_sums(values):
    leading = values.ndim - 3
    near_sum = shifted(values, leading, 1) + shifted(values, leading, -1)
    far_sum = shifted(values, leading, 2) + shifted(values, leading, -2)
    for axis_number in (leading + 1, leading + 2):
        near_sum = near_sum + shifted(values, axis_number, 1) + shifted(values, axis_number, -1)
        far_sum = far_sum + shifted(values, axis_number, 2) + shifted(values, axis_number, -2)
    return near_sum, far_sum


def residual_of(centre, near_sum, far_sum, before, source_term, kappa_part, reaction_part):
    return (source_term - centre + before
            - kappa_part * (centre_weight * centre - near_weight * near_sum - far_weight * far_sum)
            - reaction_part * centre * centre * centre)


def tables(length):
    counter = jnp.arange(length, dtype=jnp.int32)
    product = (counter[:, None] * counter[None, :]) % length
    angles = product.astype(jnp.float32) * (2.0 * math.pi / length)
    scaling = jnp.exp(counter.astype(jnp.float32) * (math.log(alpha_ratio) / length))
    forward_cos = jnp.cos(angles) * scaling[None, :]
    forward_sin = -jnp.sin(angles) * scaling[None, :]
    unscale = 1.0 / (scaling * length)
    inverse_cos = jnp.cos(angles) * unscale[:, None]
    inverse_sin = -jnp.sin(angles) * unscale[:, None]
    return forward_cos, forward_sin, inverse_cos, inverse_sin


def mode_shift(index_values, length):
    phases = index_values * (2.0 * math.pi / length)
    factor = math.exp(math.log(alpha_ratio) / length)
    return 1.0 - factor * jnp.cos(phases), factor * jnp.sin(phases)


def sweep_weights():
    return [1.0 / (1.0 + 0.4 * math.cos(math.pi * (2 * rounds + 1) / (2 * SWEEPS))) for rounds in range(SWEEPS)]


def divided(error_real, error_imag, base_part, shift_real, shift_imag):
    diag_real = shift_real + base_part
    magnitude = diag_real * diag_real + shift_imag * shift_imag
    return jnp.stack([(error_real * diag_real + error_imag * shift_imag) / magnitude,
                      (error_imag * diag_real - error_real * shift_imag) / magnitude])


def update(centre, near_sum, far_sum, target, kappa_part, base_part, shift_real, shift_imag, weight):
    applied = base_part * centre - kappa_part * (near_weight * near_sum + far_weight * far_sum)
    image_real = shift_real * centre[0] - shift_imag * centre[1] + applied[0]
    image_imag = shift_real * centre[1] + shift_imag * centre[0] + applied[1]
    error_real = target[0] - image_real
    error_imag = target[1] - image_imag
    return centre + weight * divided(error_real, error_imag, base_part, shift_real, shift_imag)


def reference(state, initial, forcing, kappa, reaction):
    kappa_full = kappa.astype(jnp.float32)
    reaction_full = reaction.astype(jnp.float32)
    start_state = initial.astype(jnp.float32)
    previous = jnp.concatenate([initial[None], state[:-1]], axis=0)

    def one_residual(item_set):
        current, earlier, source_term = item_set
        centre = current.astype(jnp.float32)
        near_sum, far_sum = cycle_sums(centre)
        result = residual_of(centre, near_sum, far_sum, earlier.astype(jnp.float32),
                             source_term.astype(jnp.float32), kappa_full, reaction_full)
        return result.astype(jnp.bfloat16)

    residual = lax.map(one_residual, (state, previous, forcing))
    forward_cos, forward_sin, inverse_cos, inverse_sin = tables(STEPS)
    flat_residual = residual.reshape(STEPS, -1).astype(jnp.float32)
    spec_real = jnp.dot(forward_cos, flat_residual, precision=highest).astype(jnp.bfloat16).reshape(state.shape)
    spec_imag = jnp.dot(forward_sin, flat_residual, precision=highest).astype(jnp.bfloat16).reshape(state.shape)
    sigma_rate = 3.0 * reaction_full * start_state * start_state
    base_rate = kappa_full * centre_weight + sigma_rate

    def one_mode(item_set):
        target_real, target_imag, mode_index = item_set
        target = jnp.stack([target_real, target_imag]).astype(jnp.float32)
        shift_real, shift_imag = mode_shift(mode_index.astype(jnp.float32), STEPS)
        iterate = divided(target[0], target[1], base_rate, shift_real, shift_imag)
        for weight in sweep_weights():
            near_sum, far_sum = cycle_sums(iterate)
            iterate = update(iterate, near_sum, far_sum, target, kappa_full, base_rate, shift_real, shift_imag, weight)
        return iterate.astype(jnp.bfloat16)

    solved = lax.map(one_mode, (spec_real, spec_imag, jnp.arange(STEPS, dtype=jnp.int32)))
    real_part = solved[:, 0].reshape(STEPS, -1).astype(jnp.float32)
    imag_part = solved[:, 1].reshape(STEPS, -1).astype(jnp.float32)
    correction = (jnp.dot(inverse_cos, real_part, precision=highest)
                  + jnp.dot(inverse_sin, imag_part, precision=highest)).astype(jnp.bfloat16).reshape(state.shape)
    return (state.astype(jnp.float32) + correction.astype(jnp.float32)).astype(jnp.bfloat16)
```

```python
import functools
import math

import jax
import jax.numpy as jnp
from jax import lax
from jax.experimental import pallas as pl
from jax.experimental.pallas import tpu as pltpu
from jax.sharding import Mesh
from jax.sharding import PartitionSpec as P

SWEEPS = 6
HALF = SWEEPS // 2
TM = ("tm_0", "tm_1", "tm_2")
CHIPS = ("tm_0", "tm_1")
CORE_SPACE = ("tm_2", "space")

alpha_ratio = 0.25
near_weight = 0.5
far_weight = 1.0
centre_weight = 6.0 * (near_weight + far_weight)
VMEM = pl.BlockSpec(memory_space=pltpu.VMEM)
SMEM = pl.BlockSpec(memory_space=pltpu.SMEM)
PAD = 8


def sweep_weights():
    return [
        1.0 / (1.0 + 0.4 * math.cos(math.pi * (2 * k + 1) / (2 * SWEEPS))) for k in range(SWEEPS)
    ]


def rotated(re, im, c, s):
    if abs(s) < 1e-12:
        return re * c, im * c
    if abs(c) < 1e-12:
        return -im * s, re * s
    return re * c - im * s, re * s + im * c


def real_dft(x):
    n = len(x)
    if n == 2:
        return [(x[0] + x[1], None), (x[0] - x[1], None)]
    even, odd = real_dft(x[0::2]), real_dft(x[1::2])
    half = n // 2
    out = [None] * (half + 1)
    out[0] = (even[0][0] + odd[0][0], None)
    out[half] = (even[0][0] - odd[0][0], None)
    for k in range(1, n // 4):
        angle = -2.0 * math.pi * k / n
        re, im = rotated(odd[k][0], odd[k][1], math.cos(angle), math.sin(angle))
        out[k] = (even[k][0] + re, even[k][1] + im)
        out[half - k] = (even[k][0] - re, im - even[k][1])
    quarter = n // 4
    out[quarter] = (even[quarter][0], -odd[quarter][0])
    return out


def real_inverse(X):
    half = len(X) - 1
    n = 2 * half
    if n == 2:
        return [X[0][0] + X[1][0], X[0][0] - X[1][0]]
    quarter = n // 4
    even, odd = [None] * (quarter + 1), [None] * (quarter + 1)
    even[0] = (X[0][0] + X[half][0], None)
    odd[0] = (X[0][0] - X[half][0], None)
    for k in range(1, quarter):
        a, b = X[k], X[half - k]
        even[k] = (a[0] + b[0], a[1] - b[1])
        angle = 2.0 * math.pi * k / n
        odd[k] = rotated(a[0] - b[0], a[1] + b[1], math.cos(angle), math.sin(angle))
    even[quarter] = (2.0 * X[quarter][0], None)
    odd[quarter] = (-2.0 * X[quarter][1], None)
    out = [None] * n
    out[0::2] = real_inverse(even)
    out[1::2] = real_inverse(odd)
    return out


def lane_masks(shape):
    lane = lax.broadcasted_iota(jnp.int32, shape, len(shape) - 1)
    last = shape[-1] - 1
    return (
        (1, jnp.where(lane >= 1, near_weight, 0.0)),
        (last, jnp.where(lane <= last - 1, near_weight, 0.0)),
        (2, jnp.where(lane >= 2, far_weight, 0.0)),
        (last - 1, jnp.where(lane <= last - 2, far_weight, 0.0)),
    )


def neighbour_sum(ref, lead, plane, rows, masks):
    def at(dp, dr):
        return ref[(*lead, plane + dp, pl.ds(PAD + dr, rows), slice(None))]

    centre = at(0, 0)
    near = (at(1, 0) + at(-1, 0)) + (at(0, 1) + at(0, -1))
    far = (at(2, 0) + at(-2, 0)) + (at(0, 2) + at(0, -2))
    total = near_weight * near + far_weight * far
    for amount, mask in masks:
        total = total + pltpu.roll(centre, amount, 1) * mask
    return centre, total


def residual_kernel(
    flag, u, lo, hi, before, initial, forcing, kappa, reaction, out, ext
):
    planes, rows, lanes = u.shape
    share = out.shape[2]
    per_plane = rows // share
    half = planes // 2
    zero = jnp.zeros((planes + 4, PAD, lanes), jnp.float32)
    ext[:, :PAD] = zero
    ext[:, PAD + rows :] = zero
    ext[:2, PAD : PAD + rows] = lo[...].astype(jnp.float32)
    ext[planes + 2 :, PAD : PAD + rows] = hi[...].astype(jnp.float32)

    def fill(p, _):
        ext[p + 2, PAD : PAD + rows] = u[p].astype(jnp.float32)
        return 0

    lax.fori_loop(0, planes, fill, 0)
    masks = lane_masks((rows, lanes))
    first = flag[0] == 0

    def one(p, _):
        centre, total = neighbour_sum(ext, (), p + 2, rows, masks)
        prior = jnp.where(first, initial[p], before[p]).astype(jnp.float32)
        value = (
            forcing[p].astype(jnp.float32)
            - centre
            + prior
            - kappa[p].astype(jnp.float32) * (centre_weight * centre - total)
            - reaction[p].astype(jnp.float32) * centre * centre * centre
        ).astype(jnp.bfloat16)
        part, inner = p // half, p % half
        for piece in range(per_plane):
            out[per_plane * inner + piece, part] = value[piece * share : (piece + 1) * share]
        return 0

    lax.fori_loop(0, planes, one, 0)


def forward_kernel(r, out):
    steps, rows, lanes = r.shape
    for start in range(0, rows, 16):
        part = pl.ds(start, 16)
        scaled = [
            r[n, part].astype(jnp.float32) * (alpha_ratio ** (n / steps)) for n in range(steps)
        ]
        spectrum = real_dft(scaled)
        out[0, 0, part] = spectrum[0][0].astype(jnp.bfloat16)
        out[0, 1, part] = spectrum[steps // 2][0].astype(jnp.bfloat16)
        for j in range(1, steps // 2):
            out[j, 0, part] = spectrum[j][0].astype(jnp.bfloat16)
            out[j, 1, part] = spectrum[j][1].astype(jnp.bfloat16)


def inverse_kernel(s, out):
    steps, rows, lanes = out.shape
    for start in range(0, rows, 16):
        part = pl.ds(start, 16)
        spectrum = [(s[0, 0, part].astype(jnp.float32), None)]
        for j in range(1, steps // 2):
            spectrum.append((s[j, 0, part].astype(jnp.float32), s[j, 1, part].astype(jnp.float32)))
        spectrum.append((s[0, 1, part].astype(jnp.float32), None))
        values = real_inverse(spectrum)
        for n in range(steps):
            scale = 1.0 / (alpha_ratio ** (n / steps) * steps)
            out[n, part] = (values[n] * scale).astype(jnp.bfloat16)


def coefficient_kernel(core, shift, kappa, initial, reaction, halo, p0, p1, q, k):
    width = halo.shape[1]
    ext = p0.shape[0]
    inner = ext - width
    side = core[0]

    def put(e, kv, iv, rv):
        kv, iv, rv = (v.astype(jnp.float32) for v in (kv, iv, rv))
        base = kv * centre_weight + 3.0 * rv * iv * iv
        si = shift[2]
        d0, d1 = shift[0] + base, shift[1] + base
        inv0 = 1.0 / (d0 * d0 + si * si)
        inv1 = 1.0 / (d1 * d1 + si * si)
        p0[e] = d0 * inv0
        p1[e] = d1 * inv1
        q[e] = si * inv0
        k[e] = kv

    def own(i, _):
        src = i + side * (kappa.shape[0] - inner)
        put(i + (1 - side) * width, kappa[src], initial[src], reaction[src])
        return 0

    def outer(i, _):
        put(i + side * inner, halo[0, i], halo[1, i], halo[2, i])
        return 0

    lax.fori_loop(0, inner, own, 0)
    lax.fori_loop(0, width, outer, 0)


def sweeps_kernel(second, core, y, ya, yb, p0, p1, q, k, *rest):
    if second:
        x_in, xa, xb, out, x0, kp, x = rest
    else:
        x_out, send_a, send_b, x0, kp, x = rest
    ext, rows, lanes = p0.shape
    share = y.shape[2]
    per_plane = rows // share
    width = ya.shape[0] // per_plane
    own = ext - 2 * width
    side = core[0]
    start_a = side * (ext - width)
    start_b = (1 - side) * (ext - width)
    inside = pl.ds(PAD, rows)

    zero = jnp.zeros((PAD, lanes), jnp.float32)

    def clear(p, _):
        for b in range(2):
            for c in range(2):
                x[b, c, p, :PAD] = zero
                x[b, c, p, PAD + rows :] = zero
        return 0

    lax.fori_loop(0, ext, clear, 0)

    def begin(ref, i, e):
        def comp(c):
            return jnp.concatenate(
                [ref[per_plane * i + h, c].astype(jnp.float32) for h in range(per_plane)], axis=0
            )

        re, im = comp(0), comp(1)
        c0, c1, cq, ck = p0[e], p1[e], q[e], k[e]
        x0_re = re * c0 + im * cq
        x0_im = im * c1 - re * cq
        x0[0, e], x0[1, e] = x0_re, x0_im
        kp[0, e], kp[1, e], kp[2, e] = ck * c0, ck * c1, ck * cq
        if not second:
            x[0, 0, e, inside], x[0, 1, e, inside] = x0_re, x0_im

    def fill(ref, base):
        def body(i, _):
            begin(ref, i, base + i)
            return 0

        return body

    lax.fori_loop(0, own, fill(y, width), 0)
    lax.fori_loop(0, width, fill(ya, start_a), 0)
    lax.fori_loop(0, width, fill(yb, start_b), 0)
    if second:

        def take_own(i, _):
            for c in range(2):
                x[0, c, width + i, inside] = x_in[c, i]
            return 0

        def take(i, _):
            for c in range(2):
                x[0, c, start_a + i, inside] = xa[c, i]
                x[0, c, start_b + i, inside] = xb[c, i]
            return 0

        lax.fori_loop(0, own, take_own, 0)
        lax.fori_loop(0, width, take, 0)

    masks = lane_masks((rows, lanes))
    weights = sweep_weights()[HALF:] if second else sweep_weights()[:HALF]
    for step, weight in enumerate(weights):
        src, dst = step % 2, (step + 1) % 2
        margin = 2 * (step + 1)
        last = step == len(weights) - 1

        def sweep(e, _, src=src, dst=dst, weight=weight, last=last):
            re, sum_re = neighbour_sum(x, (src, 0), e, rows, masks)
            im, sum_im = neighbour_sum(x, (src, 1), e, rows, masks)
            k0, k1, kq = kp[0, e], kp[1, e], kp[2, e]
            new_re = (1.0 - weight) * re + weight * (x0[0, e] + k0 * sum_re + kq * sum_im)
            new_im = (1.0 - weight) * im + weight * (x0[1, e] + k1 * sum_im - kq * sum_re)
            if not last:
                x[dst, 0, e, inside], x[dst, 1, e, inside] = new_re, new_im
            elif second:
                i = e - width
                for c, value in ((0, new_re), (1, new_im)):
                    value = value.astype(jnp.bfloat16)
                    for h in range(per_plane):
                        out[per_plane * i + h, c] = value[h * share : (h + 1) * share]
            else:
                x_out[0, e - width], x_out[1, e - width] = new_re, new_im
            return 0

        lax.fori_loop(margin, ext - margin, sweep, 0)
    if not second:
        gap = own - width

        def send(i, _):
            for c in range(2):
                send_a[c, i] = x_out[c, i + side * gap]
                send_b[c, i] = x_out[c, i + (1 - side) * gap]
            return 0

        lax.fori_loop(0, width, send, 0)


def final_kernel(state, correction, out):
    planes, rows, lanes = state.shape
    share = correction.shape[2]
    per_plane = rows // share
    half = planes // 2

    def one(p, _):
        part, inner = p // half, p % half
        value = jnp.concatenate(
            [
                correction[per_plane * inner + h, part].astype(jnp.float32)
                for h in range(per_plane)
            ],
            axis=0,
        )
        out[p] = (state[p].astype(jnp.float32) + value).astype(jnp.bfloat16)
        return 0

    lax.fori_loop(0, planes, one, 0)


def call(kernel, shapes, inputs, scratch=(), scalars=0, name=None):
    outs = [jax.ShapeDtypeStruct(s, d) for s, d in shapes]
    return pl.pallas_call(
        kernel,
        out_shape=outs,
        in_specs=[SMEM] * scalars + [VMEM] * (len(inputs) - scalars),
        out_specs=[VMEM] * len(outs),
        scratch_shapes=list(scratch),
        name=name,
        compiler_params=pltpu.CompilerParams(vmem_limit_bytes=24 << 20),
    )(*inputs)


def on_device(state, initial, forcing, kappa, reaction):
    _, planes, rows, lanes = state.shape
    members = lax.axis_size(TM)
    slots = lax.axis_size(CHIPS)
    slabs = lax.axis_size("space")
    own = planes // 2
    share = own * rows // slots
    per_plane = rows // share
    width = 2 * HALF
    ext = own + 2 * width
    bf16, f32 = jnp.bfloat16, jnp.float32
    position = lax.axis_index(TM)
    core = lax.axis_index("tm_2")
    slot = lax.axis_index(CHIPS)
    u = state[0]
    core_arg = core.astype(jnp.int32).reshape(1)

    forward = [(i, i + 1) for i in range(slabs - 1)]
    backward = [(t, s) for s, t in forward]
    outer = []
    for s in range(slabs - 1):
        outer += [(slabs + s, s + 1), (s + 1, slabs + s)]
    lo = lax.ppermute(u[planes - 2 :], "space", forward)
    hi = lax.ppermute(u[:2], "space", backward)
    before = lax.ppermute(u, TM, [(i, i + 1) for i in range(members - 1)])
    coefs = jnp.stack([kappa, initial, reaction])
    rim = jnp.where(core == 0, coefs[:, :width], coefs[:, planes - width :])
    rim = lax.ppermute(rim, CORE_SPACE, outer)

    (residual,) = call(
        residual_kernel,
        [((slots, 2, share, lanes), bf16)],
        [
            position.astype(jnp.int32).reshape(1),
            u,
            lo,
            hi,
            before,
            initial,
            forcing[0],
            kappa,
            reaction,
        ],
        [pltpu.VMEM((planes + 4, rows + 2 * PAD, lanes), f32)],
        scalars=1,
        name="residual",
    )
    cells = lax.all_to_all(residual.reshape(members, share, lanes), TM, 0, 0, tiled=True)
    (spectrum,) = call(forward_kernel, [((slots, 2, share, lanes), bf16)], [cells], name="forward")
    y = lax.all_to_all(spectrum, CHIPS, 0, 0, tiled=True)

    factor = math.exp(math.log(alpha_ratio) / members)
    table = []
    for j in range(slots):
        phase = 2.0 * math.pi * j / members
        sr = 1.0 - factor * math.cos(phase)
        table.append([sr, 1.0 + factor if j == 0 else sr, factor * math.sin(phase)])
    shift = lax.dynamic_slice_in_dim(jnp.asarray(table, f32), slot, 1, axis=0)[0]
    fields = call(
        coefficient_kernel,
        [((ext, rows, lanes), f32)] * 4,
        [core_arg, shift, kappa, initial, reaction, rim],
        scalars=2,
        name="coefficients",
    )

    swap = [(i, slabs + i) for i in range(slabs)] + [(slabs + i, i) for i in range(slabs)]
    pieces = per_plane * width
    gap = per_plane * (own - width)
    ya = lax.ppermute(
        jnp.where(core == 0, y[:pieces], y[gap:]), CORE_SPACE, outer
    )
    yb = lax.ppermute(
        jnp.where(core == 0, y[gap:], y[:pieces]), CORE_SPACE, swap
    )
    scratch = [
        pltpu.VMEM((2, ext, rows, lanes), f32),
        pltpu.VMEM((3, ext, rows, lanes), f32),
        pltpu.VMEM((2, 2, ext, rows + 2 * PAD, lanes), f32),
    ]
    x, send_a, send_b = call(
        functools.partial(sweeps_kernel, False),
        [
            ((2, own, rows, lanes), f32),
            ((2, width, rows, lanes), f32),
            ((2, width, rows, lanes), f32),
        ],
        [core_arg, y, ya, yb, *fields],
        scratch,
        scalars=1,
        name="sweeps_a",
    )
    xa = lax.ppermute(send_a, CORE_SPACE, outer)
    xb = lax.ppermute(send_b, CORE_SPACE, swap)
    (solved,) = call(
        functools.partial(sweeps_kernel, True),
        [((slots, 2, share, lanes), bf16)],
        [core_arg, y, ya, yb, *fields, x, xa, xb],
        scratch,
        scalars=1,
        name="sweeps_b",
    )
    modes = lax.all_to_all(solved, CHIPS, 0, 0, tiled=True)
    (correction,) = call(inverse_kernel, [((members, share, lanes), bf16)], [modes], name="inverse")
    returned = lax.all_to_all(correction, TM, 0, 0, tiled=True)
    (updated,) = call(
        final_kernel,
        [((planes, rows, lanes), bf16)],
        [u, returned.reshape(slots, 2, share, lanes)],
        name="final",
    )
    return updated[None]


def solution(mesh):
    torus = Mesh(
        mesh.devices.reshape(2, 8, 2, mesh.shape["space"]), ("tm_0", "tm_1", "tm_2", "space")
    )
    in_specs = (
        P(TM, "space", None, None),
        P("space", None, None),
        P(TM, "space", None, None),
        P("space", None, None),
        P("space", None, None),
    )
    out_specs = P(TM, "space", None, None)
    return jax.shard_map(
        on_device, mesh=torus, in_specs=in_specs, out_specs=out_specs, check_vma=False
    )
```

```python
import math

import jax
import jax.numpy as jnp
from jax import lax
from jax.experimental import pallas as pl
from jax.experimental.pallas import tpu as pltpu
from jax.sharding import Mesh
from jax.sharding import PartitionSpec as P

SWEEPS = 6
STEPS = 32
UNROLL = 2
TM = ("tm_0", "tm_1", "tm_2")
CHIPS = ("tm_0", "tm_1")
CORE_SPACE = ("tm_2", "space")

alpha_ratio = 0.25
near_weight = 0.5
far_weight = 1.0
centre_weight = 6.0 * (near_weight + far_weight)
VMEM = pl.BlockSpec(memory_space=pltpu.VMEM)
HBM = pl.BlockSpec(memory_space=pltpu.HBM)
SMEM = pl.BlockSpec(memory_space=pltpu.SMEM)
PAD = 8


def sweep_weights():
    return [
        1.0 / (1.0 + 0.4 * math.cos(math.pi * (2 * k + 1) / (2 * SWEEPS))) for k in range(SWEEPS)
    ]


def rotated(re, im, c, s):
    if abs(s) < 1e-12:
        return re * c, im * c
    if abs(c) < 1e-12:
        return -im * s, re * s
    return re * c - im * s, re * s + im * c


def real_dft(x):
    n = len(x)
    if n == 2:
        return [(x[0] + x[1], None), (x[0] - x[1], None)]
    even, odd = real_dft(x[0::2]), real_dft(x[1::2])
    half = n // 2
    out = [None] * (half + 1)
    out[0] = (even[0][0] + odd[0][0], None)
    out[half] = (even[0][0] - odd[0][0], None)
    for k in range(1, n // 4):
        angle = -2.0 * math.pi * k / n
        re, im = rotated(odd[k][0], odd[k][1], math.cos(angle), math.sin(angle))
        out[k] = (even[k][0] + re, even[k][1] + im)
        out[half - k] = (even[k][0] - re, im - even[k][1])
    quarter = n // 4
    out[quarter] = (even[quarter][0], -odd[quarter][0])
    return out


def real_inverse(X):
    half = len(X) - 1
    n = 2 * half
    if n == 2:
        return [X[0][0] + X[1][0], X[0][0] - X[1][0]]
    quarter = n // 4
    even, odd = [None] * (quarter + 1), [None] * (quarter + 1)
    even[0] = (X[0][0] + X[half][0], None)
    odd[0] = (X[0][0] - X[half][0], None)
    for k in range(1, quarter):
        a, b = X[k], X[half - k]
        even[k] = (a[0] + b[0], a[1] - b[1])
        angle = 2.0 * math.pi * k / n
        odd[k] = rotated(a[0] - b[0], a[1] + b[1], math.cos(angle), math.sin(angle))
    even[quarter] = (2.0 * X[quarter][0], None)
    odd[quarter] = (-2.0 * X[quarter][1], None)
    out = [None] * n
    out[0::2] = real_inverse(even)
    out[1::2] = real_inverse(odd)
    return out


def lane_masks(shape):
    lane = lax.broadcasted_iota(jnp.int32, shape, len(shape) - 1)
    last = shape[-1] - 1
    return (
        (1, jnp.where(lane >= 1, near_weight, 0.0)),
        (last, jnp.where(lane <= last - 1, near_weight, 0.0)),
        (2, jnp.where(lane >= 2, far_weight, 0.0)),
        (last - 1, jnp.where(lane <= last - 2, far_weight, 0.0)),
    )


def neighbour_sum(ref, lead, plane, rows, masks):
    def at(dp, dr):
        return ref[(*lead, plane + dp, pl.ds(PAD + dr, rows), slice(None))]

    centre = at(0, 0)
    near = (at(1, 0) + at(-1, 0)) + (at(0, 1) + at(0, -1))
    far = (at(2, 0) + at(-2, 0)) + (at(0, 2) + at(0, -2))
    total = near_weight * near + far_weight * far
    for amount, mask in masks:
        total = total + pltpu.roll(centre, amount, 1) * mask
    return centre, total


def local_kernel(flag, u_hbm, initial_hbm, forcing_hbm, kappa_hbm, reaction_hbm, part, rim, *rest):
    ext, u, initial, forcing, kappa, reaction, sems = rest
    planes, rows, lanes = u.shape
    pairs = ((u_hbm, u), (forcing_hbm, forcing), (kappa_hbm, kappa), (reaction_hbm, reaction))
    pairs += ((initial_hbm, initial),)
    copies = [pltpu.make_async_copy(src, dst, sems.at[i]) for i, (src, dst) in enumerate(pairs)]
    for copy in copies:
        copy.start()
    zero = jnp.zeros((PAD, lanes), jnp.float32)

    def clear(p, _):
        ext[p, :PAD] = zero
        ext[p, PAD + rows :] = zero
        return 0

    lax.fori_loop(0, planes + 4, clear, 0)
    blank = jnp.zeros((rows, lanes), jnp.float32)
    for p in (0, 1, planes + 2, planes + 3):
        ext[p, PAD : PAD + rows] = blank
    for copy in copies:
        copy.wait()

    def fill(p, _):
        ext[p + 2, PAD : PAD + rows] = u[p].astype(jnp.float32)
        return 0

    lax.fori_loop(0, planes, fill, 0)
    masks = lane_masks((rows, lanes))
    first = flag[0] == 0

    def one(p, _):
        centre, total = neighbour_sum(ext, (), p + 2, rows, masks)
        prior = jnp.where(first, initial[p].astype(jnp.float32), 0.0)
        part[p] = (
            forcing[p].astype(jnp.float32)
            - centre
            + prior
            - kappa[p].astype(jnp.float32) * (centre_weight * centre - total)
            - reaction[p].astype(jnp.float32) * centre * centre * centre
        )
        return 0

    lax.fori_loop(0, planes, one, 0)
    for i, p in enumerate((0, 1, planes - 2, planes - 1)):
        rim[i] = kappa[p].astype(jnp.float32)


def residual_kernel(part, rim, lo, hi, before, out):
    planes, rows, _ = part.shape
    share = out.shape[2]
    per_plane = rows // share
    half = planes // 2

    def put(p, value):
        value = value.astype(jnp.bfloat16)
        side, inner = p // half, p % half
        for piece in range(per_plane):
            out[per_plane * inner + piece, side] = value[piece * share : (piece + 1) * share]

    def one(p, _):
        put(p, part[p] + before[p].astype(jnp.float32))
        return 0

    lax.fori_loop(2, planes - 2, one, 0)
    l0, l1, h0, h1 = (v.astype(jnp.float32) for v in (lo[0], lo[1], hi[0], hi[1]))
    edges = (
        (0, near_weight * l1 + far_weight * l0),
        (1, far_weight * l1),
        (planes - 2, far_weight * h0),
        (planes - 1, near_weight * h0 + far_weight * h1),
    )
    for i, (p, total) in enumerate(edges):
        put(p, part[p] + rim[i] * total + before[p].astype(jnp.float32))


def forward_kernel(r, out):
    steps, rows, _ = r.shape
    for start in range(0, rows, 16):
        part = pl.ds(start, 16)
        scaled = [
            r[n, part].astype(jnp.float32) * (alpha_ratio ** (n / steps)) for n in range(steps)
        ]
        spectrum = real_dft(scaled)
        out[0, 0, part] = spectrum[0][0].astype(jnp.bfloat16)
        out[0, 1, part] = spectrum[steps // 2][0].astype(jnp.bfloat16)
        for j in range(1, steps // 2):
            out[j, 0, part] = spectrum[j][0].astype(jnp.bfloat16)
            out[j, 1, part] = spectrum[j][1].astype(jnp.bfloat16)


def inverse_kernel(s, out):
    steps, rows, _ = out.shape
    for start in range(0, rows, 16):
        part = pl.ds(start, 16)
        spectrum = [(s[0, 0, part].astype(jnp.float32), None)]
        for j in range(1, steps // 2):
            spectrum.append((s[j, 0, part].astype(jnp.float32), s[j, 1, part].astype(jnp.float32)))
        spectrum.append((s[0, 1, part].astype(jnp.float32), None))
        values = real_inverse(spectrum)
        for n in range(steps):
            scale = 1.0 / (alpha_ratio ** (n / steps) * steps)
            out[n, part] = (values[n] * scale).astype(jnp.bfloat16)


def coefficient_kernel(where, kappa, initial, reaction, outer, inner, p0, p1, q, k):
    planes = kappa.shape[0]
    wide, narrow = outer.shape[1], inner.shape[1]
    core, slot = where[0], where[1]
    members = STEPS
    factor = math.exp(math.log(alpha_ratio) / members)
    s0 = s1 = si = jnp.float32(0.0)
    for j in range(members // 2):
        phase = 2.0 * math.pi * j / members
        real, imag = 1.0 - factor * math.cos(phase), factor * math.sin(phase)
        hit = slot == j
        s0 = jnp.where(hit, jnp.float32(real), s0)
        s1 = jnp.where(hit, jnp.float32(real if j else 1.0 + factor), s1)
        si = jnp.where(hit, jnp.float32(imag if j else 0.0), si)

    def put(e, kv, iv, rv):
        kv, iv, rv = (v.astype(jnp.float32) for v in (kv, iv, rv))
        base = kv * centre_weight + 3.0 * rv * iv * iv
        d0, d1 = s0 + base, s1 + base
        inv0 = 1.0 / (d0 * d0 + si * si)
        inv1 = 1.0 / (d1 * d1 + si * si)
        p0[e] = d0 * inv0
        p1[e] = d1 * inv1
        q[e] = si * inv0
        k[e] = kv

    def own(i, _):
        put(i + jnp.where(core == 0, wide, narrow), kappa[i], initial[i], reaction[i])
        return 0

    def far(i, _):
        put(i + jnp.where(core == 0, 0, planes + narrow), outer[0, i], outer[1, i], outer[2, i])
        return 0

    def close(i, _):
        put(i + jnp.where(core == 0, planes + wide, 0), inner[0, i], inner[1, i], inner[2, i])
        return 0

    lax.fori_loop(0, planes, own, 0)
    lax.fori_loop(0, wide, far, 0)
    lax.fori_loop(0, narrow, close, 0)


def sweeps_kernel(where, y, ya, yb, yc, yd, p0, p1, q, k, out, x0, kp, xs, xt):
    ext, rows, lanes = p0.shape
    share = y.shape[2]
    per_plane = rows // share
    own = y.shape[0] // per_plane
    margin = (ext - own) // 2
    core = where[0]
    inside = pl.ds(PAD, rows)
    zero = jnp.zeros((PAD, lanes), jnp.float32)

    def clear(p, _):
        for x in (xs, xt):
            for c in range(2):
                x[c, p, :PAD] = zero
                x[c, p, PAD + rows :] = zero
        return 0

    lax.fori_loop(0, ext, clear, 0)

    def fill(ref, base):
        def body(i, _):
            e = base + i

            def comp(c):
                return jnp.concatenate(
                    [ref[per_plane * i + h, c].astype(jnp.float32) for h in range(per_plane)],
                    axis=0,
                )

            re, im = comp(0), comp(1)
            c0, c1, cq, ck = p0[e], p1[e], q[e], k[e]
            x0_re = re * c0 + im * cq
            x0_im = im * c1 - re * cq
            x0[0, e], x0[1, e] = x0_re, x0_im
            xs[0, e, inside], xs[1, e, inside] = x0_re, x0_im
            kp[0, e], kp[1, e], kp[2, e] = ck * c0, ck * c1, ck * cq
            return 0

        lax.fori_loop(0, ref.shape[0] // per_plane, body, 0)

    far = yc.shape[0] // per_plane
    fill(y, margin)
    fill(ya, jnp.where(core == 0, far, margin + own))
    fill(yb, jnp.where(core == 0, margin + own, far))
    fill(yc, jnp.where(core == 0, 0, ext - far))
    fill(yd, jnp.where(core == 0, ext - far, 0))

    masks = lane_masks((rows, lanes))
    weights = sweep_weights()
    for step, weight in enumerate(weights):
        src, dst = (xs, xt) if step % 2 == 0 else (xt, xs)
        edge = 2 * (step + 1)
        last = step == len(weights) - 1

        def value(e, src=src, weight=weight):
            re, sum_re = neighbour_sum(src, (0,), e, rows, masks)
            im, sum_im = neighbour_sum(src, (1,), e, rows, masks)
            k0, k1, kq = kp[0, e], kp[1, e], kp[2, e]
            new_re = (1.0 - weight) * re + weight * (x0[0, e] + k0 * sum_re + kq * sum_im)
            new_im = (1.0 - weight) * im + weight * (x0[1, e] + k1 * sum_im - kq * sum_re)
            return new_re, new_im

        def store(e, pair, dst=dst, last=last):
            for c in range(2):
                if not last:
                    dst[c, e, inside] = pair[c]
                    continue
                rounded = pair[c].astype(jnp.bfloat16)
                for h in range(per_plane):
                    out[per_plane * (e - margin) + h, c] = rounded[h * share : (h + 1) * share]

        def sweep(i, _, edge=edge, value=value, store=store):
            planes = [edge + UNROLL * i + r for r in range(UNROLL)]
            pairs = [value(e) for e in planes]
            for e, pair in zip(planes, pairs):
                store(e, pair)
            return 0

        lax.fori_loop(0, (ext - 2 * edge) // UNROLL, sweep, 0)


def final_kernel(state, correction, out):
    planes, rows, _ = state.shape
    share = correction.shape[2]
    per_plane = rows // share
    half = planes // 2

    def one(p, _):
        part, inner = p // half, p % half
        value = jnp.concatenate(
            [
                correction[per_plane * inner + h, part].astype(jnp.float32)
                for h in range(per_plane)
            ],
            axis=0,
        )
        out[p] = (state[p].astype(jnp.float32) + value).astype(jnp.bfloat16)
        return 0

    lax.fori_loop(0, planes, one, 0)


def call(kernel, shapes, inputs, scratch=(), scalars=0, anywhere=0, flops=None):
    outs = [jax.ShapeDtypeStruct(s, d) for s, d in shapes]
    cost = None
    if flops is not None:
        cost = pl.CostEstimate(flops=flops, transcendentals=0, bytes_accessed=flops // 8)
    rest = len(inputs) - scalars - anywhere
    return pl.pallas_call(
        kernel,
        out_shape=outs,
        in_specs=[SMEM] * scalars + [HBM] * anywhere + [VMEM] * rest,
        out_specs=[VMEM] * len(outs),
        scratch_shapes=list(scratch),
        cost_estimate=cost,
        compiler_params=pltpu.CompilerParams(vmem_limit_bytes=24 << 20),
    )(*inputs)


def iteration(state, initial, forcing, kappa, reaction):
    _, planes, rows, lanes = state.shape
    members = lax.axis_size(TM)
    slots = lax.axis_size(CHIPS)
    slabs = lax.axis_size("space")
    own = planes // 2
    share = own * rows // slots
    per_plane = rows // share
    wide = 2 * SWEEPS
    narrow = wide - own
    ext = own + 2 * wide
    bf16, f32, i32 = jnp.bfloat16, jnp.float32, jnp.int32
    position = lax.axis_index(TM).astype(i32).reshape(1)
    core = lax.axis_index("tm_2")
    slot = lax.axis_index(CHIPS)
    where = jnp.stack([core, slot]).astype(i32)
    u = state[0]

    forward = [(i, i + 1) for i in range(slabs - 1)]
    backward = [(t, s) for s, t in forward]
    outer = []
    for s in range(slabs - 1):
        outer += [(slabs + s, s + 1), (s + 1, slabs + s)]
    swap = [(i, slabs + i) for i in range(slabs)] + [(slabs + i, i) for i in range(slabs)]
    same = forward + [(slabs + s, slabs + t) for s, t in backward]
    lo = lax.ppermute(u[planes - 2 :], "space", forward)
    hi = lax.ppermute(u[:2], "space", backward)
    before = lax.ppermute(u, TM, [(i, i + 1) for i in range(members - 1)])
    coefs = jnp.stack([kappa, initial, reaction])
    rim = jnp.where(core == 0, coefs[:, :wide], coefs[:, planes - wide :])
    rim = lax.ppermute(rim, CORE_SPACE, outer)
    inner = jnp.where(core == 0, rim[:, wide - narrow :], rim[:, :narrow])
    inner = lax.ppermute(inner, CORE_SPACE, swap)

    block = ((planes, rows, lanes), bf16)
    part, edge = call(
        local_kernel,
        [((planes, rows, lanes), f32), ((4, rows, lanes), f32)],
        [position, u, initial, forcing[0], kappa, reaction],
        [pltpu.VMEM((planes + 4, rows + 2 * PAD, lanes), f32)]
        + [pltpu.VMEM(*block)] * 5
        + [pltpu.SemaphoreType.DMA((5,))],
        scalars=1,
        anywhere=5,
        flops=20_000_000,
    )
    (residual,) = call(
        residual_kernel, [((slots, 2, share, lanes), bf16)], [part, edge, lo, hi, before]
    )
    cells = lax.all_to_all(residual.reshape(members, share, lanes), TM, 0, 0, tiled=True)
    (spectrum,) = call(forward_kernel, [((slots, 2, share, lanes), bf16)], [cells])
    y = lax.all_to_all(spectrum, CHIPS, 0, 0, tiled=True)

    fields = call(
        coefficient_kernel,
        [((ext, rows, lanes), f32)] * 4,
        [where, kappa, initial, reaction, rim, inner],
        scalars=1,
    )
    n = per_plane * narrow
    first = core == 0
    ya = lax.ppermute(y, CORE_SPACE, outer)
    yc = lax.ppermute(jnp.where(first, y[-n:], y[:n]), CORE_SPACE, same)
    yb = lax.ppermute(y, CORE_SPACE, swap)
    yd = lax.ppermute(jnp.where(first, ya[-n:], ya[:n]), CORE_SPACE, swap)
    (solved,) = call(
        sweeps_kernel,
        [((slots, 2, share, lanes), bf16)],
        [where, y, ya, yb, yc, yd, *fields],
        [
            pltpu.VMEM((2, ext, rows, lanes), f32),
            pltpu.VMEM((3, ext, rows, lanes), f32),
            pltpu.VMEM((2, ext, rows + 2 * PAD, lanes), f32),
            pltpu.VMEM((2, ext, rows + 2 * PAD, lanes), f32),
        ],
        scalars=1,
    )
    modes = lax.all_to_all(solved, CHIPS, 0, 0, tiled=True)
    (correction,) = call(inverse_kernel, [((members, share, lanes), bf16)], [modes])
    returned = lax.all_to_all(correction, TM, 0, 0, tiled=True)
    (updated,) = call(
        final_kernel, [((planes, rows, lanes), bf16)], [u, returned.reshape(slots, 2, share, lanes)]
    )
    return updated[None]


def solution(mesh):
    torus = Mesh(
        mesh.devices.reshape(2, 8, 2, mesh.shape["space"]), ("tm_0", "tm_1", "tm_2", "space")
    )
    in_specs = (
        P(TM, "space", None, None),
        P("space", None, None),
        P(TM, "space", None, None),
        P("space", None, None),
        P("space", None, None),
    )
    out_specs = P(TM, "space", None, None)
    return jax.shard_map(
        iteration, mesh=torus, in_specs=in_specs, out_specs=out_specs, check_vma=False
    )
```

```python
import math

import jax
import jax.numpy as jnp
from jax import lax
from jax.experimental import pallas as pl
from jax.experimental.pallas import tpu as pltpu
from jax.sharding import Mesh
from jax.sharding import PartitionSpec as P

SWEEPS = 6
STEPS = 32
UNROLL = 2
LARGE = 24 * 2**20
TM = ("tm_0", "tm_1", "tm_2")
CHIPS = ("tm_0", "tm_1")
CORE_SPACE = ("tm_2", "space")

alpha_ratio = 0.25
near_weight = 0.5
far_weight = 1.0
centre_weight = 6.0 * (near_weight + far_weight)
VMEM = pl.BlockSpec(memory_space=pltpu.VMEM)
HBM = pl.BlockSpec(memory_space=pltpu.HBM)
SMEM = pl.BlockSpec(memory_space=pltpu.SMEM)
PAD = 8


def sweep_weights():
    return [
        1.0 / (1.0 + 0.4 * math.cos(math.pi * (2 * k + 1) / (2 * SWEEPS))) for k in range(SWEEPS)
    ]


def rotated(re, im, c, s):
    if abs(s) < 1e-12:
        return re * c, im * c
    if abs(c) < 1e-12:
        return -im * s, re * s
    return re * c - im * s, re * s + im * c


def real_dft(x):
    n = len(x)
    if n == 2:
        return [(x[0] + x[1], None), (x[0] - x[1], None)]
    even, odd = real_dft(x[0::2]), real_dft(x[1::2])
    half = n // 2
    out = [None] * (half + 1)
    out[0] = (even[0][0] + odd[0][0], None)
    out[half] = (even[0][0] - odd[0][0], None)
    for k in range(1, n // 4):
        angle = -2.0 * math.pi * k / n
        re, im = rotated(odd[k][0], odd[k][1], math.cos(angle), math.sin(angle))
        out[k] = (even[k][0] + re, even[k][1] + im)
        out[half - k] = (even[k][0] - re, im - even[k][1])
    quarter = n // 4
    out[quarter] = (even[quarter][0], -odd[quarter][0])
    return out


def real_inverse(X):
    half = len(X) - 1
    n = 2 * half
    if n == 2:
        return [X[0][0] + X[1][0], X[0][0] - X[1][0]]
    quarter = n // 4
    even, odd = [None] * (quarter + 1), [None] * (quarter + 1)
    even[0] = (X[0][0] + X[half][0], None)
    odd[0] = (X[0][0] - X[half][0], None)
    for k in range(1, quarter):
        a, b = X[k], X[half - k]
        even[k] = (a[0] + b[0], a[1] - b[1])
        angle = 2.0 * math.pi * k / n
        odd[k] = rotated(a[0] - b[0], a[1] + b[1], math.cos(angle), math.sin(angle))
    even[quarter] = (2.0 * X[quarter][0], None)
    odd[quarter] = (-2.0 * X[quarter][1], None)
    out = [None] * n
    out[0::2] = real_inverse(even)
    out[1::2] = real_inverse(odd)
    return out


def lane_masks(shape):
    lane = lax.broadcasted_iota(jnp.int32, shape, len(shape) - 1)
    last = shape[-1] - 1
    return (
        (1, jnp.where(lane >= 1, near_weight, 0.0)),
        (last, jnp.where(lane <= last - 1, near_weight, 0.0)),
        (2, jnp.where(lane >= 2, far_weight, 0.0)),
        (last - 1, jnp.where(lane <= last - 2, far_weight, 0.0)),
    )


def neighbour_sum(ref, lead, plane, rows, masks):
    def at(dp, dr):
        return ref[(*lead, plane + dp, pl.ds(PAD + dr, rows), slice(None))]

    centre = at(0, 0)
    near = (at(1, 0) + at(-1, 0)) + (at(0, 1) + at(0, -1))
    far = (at(2, 0) + at(-2, 0)) + (at(0, 2) + at(0, -2))
    total = near_weight * near + far_weight * far
    for amount, mask in masks:
        total = total + pltpu.roll(centre, amount, 1) * mask
    return centre, total


def local_kernel(
    where, u_hbm, initial_hbm, forcing_hbm, kappa_hbm, reaction_hbm, part, rim, coefs, *rest
):
    ext, u, initial, forcing, kappa, reaction, sems = rest
    planes, rows, lanes = u.shape
    pairs = ((u_hbm, u), (forcing_hbm, forcing), (kappa_hbm, kappa), (reaction_hbm, reaction))
    pairs += ((initial_hbm, initial),)
    copies = [pltpu.make_async_copy(src, dst, sems.at[i]) for i, (src, dst) in enumerate(pairs)]
    for copy in copies:
        copy.start()
    zero = jnp.zeros((PAD, lanes), jnp.float32)

    def clear(p, _):
        ext[p, :PAD] = zero
        ext[p, PAD + rows :] = zero
        return 0

    lax.fori_loop(0, planes + 4, clear, 0)
    blank = jnp.zeros((rows, lanes), jnp.float32)
    for p in (0, 1, planes + 2, planes + 3):
        ext[p, PAD : PAD + rows] = blank
    for copy in copies:
        copy.wait()

    def fill(p, _):
        ext[p + 2, PAD : PAD + rows] = u[p].astype(jnp.float32)
        return 0

    lax.fori_loop(0, planes, fill, 0)
    masks = lane_masks((rows, lanes))
    first = jnp.logical_and(where[0] == 0, where[1] == 0)

    def one(p, _):
        centre, total = neighbour_sum(ext, (), p + 2, rows, masks)
        prior = jnp.where(first, initial[p].astype(jnp.float32), 0.0)
        part[p] = (
            forcing[p].astype(jnp.float32)
            - centre
            + prior
            - kappa[p].astype(jnp.float32) * (centre_weight * centre - total)
            - reaction[p].astype(jnp.float32) * centre * centre * centre
        )
        return 0

    lax.fori_loop(0, planes, one, 0)
    for i, p in enumerate((0, 1, planes - 2, planes - 1)):
        rim[i] = kappa[p].astype(jnp.float32)
    width = coefs.shape[1]
    skip = where[0] * (planes - width)

    def send(i, _):
        for row, source in enumerate((kappa, initial, reaction)):
            coefs[row, i] = source[i + skip]
        return 0

    lax.fori_loop(0, width, send, 0)


def residual_kernel(where, part, rim, lo, hi, before, mine, theirs):
    planes, rows, _ = part.shape
    share = mine.shape[1]
    per_plane = rows // share
    half = planes // 2
    core = where[0]

    def put(out, inner, value):
        value = value.astype(jnp.bfloat16)
        for piece in range(per_plane):
            out[per_plane * inner + piece] = value[piece * share : (piece + 1) * share]

    def one(i, _):
        for out, side in ((mine, core), (theirs, 1 - core)):
            p = side * half + i
            put(out, i, part[p] + before[p].astype(jnp.float32))
        return 0

    lax.fori_loop(0, half, one, 0)
    l0, l1, h0, h1 = (v.astype(jnp.float32) for v in (lo[0], lo[1], hi[0], hi[1]))
    edges = (
        (0, near_weight * l1 + far_weight * l0),
        (1, far_weight * l1),
        (planes - 2, far_weight * h0),
        (planes - 1, near_weight * h0 + far_weight * h1),
    )
    values = [
        part[p] + rim[i] * total + before[p].astype(jnp.float32)
        for i, (p, total) in enumerate(edges)
    ]

    def lower(low, high):
        for i, p in enumerate((0, 1)):
            put(low, p, values[i])
        for i, p in enumerate((half - 2, half - 1)):
            put(high, p, values[2 + i])

    @pl.when(core == 0)
    def _():
        lower(mine, theirs)

    @pl.when(core != 0)
    def _():
        lower(theirs, mine)


def forward_kernel(where, r, out):
    chips, cores, rows, _ = r.shape
    steps = chips * cores
    core = where[0]
    for start in range(0, rows, 16):
        part = pl.ds(start, 16)
        scaled = []
        for n in range(steps):
            turn = core if n % cores == 0 else 1 - core
            scaled.append(
                r[n // cores, turn, part].astype(jnp.float32) * (alpha_ratio ** (n / steps))
            )
        spectrum = real_dft(scaled)
        out[0, 0, part] = spectrum[0][0].astype(jnp.bfloat16)
        out[0, 1, part] = spectrum[steps // 2][0].astype(jnp.bfloat16)
        for j in range(1, steps // 2):
            out[j, 0, part] = spectrum[j][0].astype(jnp.bfloat16)
            out[j, 1, part] = spectrum[j][1].astype(jnp.bfloat16)


def inverse_kernel(where, s, out):
    chips, cores, rows, _ = out.shape
    steps = chips * cores
    core = where[0]
    for start in range(0, rows, 16):
        part = pl.ds(start, 16)
        spectrum = [(s[0, 0, part].astype(jnp.float32), None)]
        for j in range(1, steps // 2):
            spectrum.append((s[j, 0, part].astype(jnp.float32), s[j, 1, part].astype(jnp.float32)))
        spectrum.append((s[0, 1, part].astype(jnp.float32), None))
        values = real_inverse(spectrum)
        for n in range(steps):
            turn = core if n % cores == 0 else 1 - core
            scale = 1.0 / (alpha_ratio ** (n / steps) * steps)
            out[n // cores, turn, part] = (values[n] * scale).astype(jnp.bfloat16)


def coefficient_kernel(where, kappa, initial, reaction, outer, inner, p0, p1, q, k):
    planes = kappa.shape[0]
    wide, narrow = outer.shape[1], inner.shape[1]
    core, slot = where[0], where[1]
    members = STEPS
    factor = math.exp(math.log(alpha_ratio) / members)
    s0 = s1 = si = jnp.float32(0.0)
    for j in range(members // 2):
        phase = 2.0 * math.pi * j / members
        real, imag = 1.0 - factor * math.cos(phase), factor * math.sin(phase)
        hit = slot == j
        s0 = jnp.where(hit, jnp.float32(real), s0)
        s1 = jnp.where(hit, jnp.float32(real if j else 1.0 + factor), s1)
        si = jnp.where(hit, jnp.float32(imag if j else 0.0), si)

    def put(e, kv, iv, rv):
        kv, iv, rv = (v.astype(jnp.float32) for v in (kv, iv, rv))
        base = kv * centre_weight + 3.0 * rv * iv * iv
        d0, d1 = s0 + base, s1 + base
        inv0 = 1.0 / (d0 * d0 + si * si)
        inv1 = 1.0 / (d1 * d1 + si * si)
        p0[e] = d0 * inv0
        p1[e] = d1 * inv1
        q[e] = si * inv0
        k[e] = kv

    def own(i, _):
        put(i + jnp.where(core == 0, wide, narrow), kappa[i], initial[i], reaction[i])
        return 0

    def far(i, _):
        put(i + jnp.where(core == 0, 0, planes + narrow), outer[0, i], outer[1, i], outer[2, i])
        return 0

    def close(i, _):
        put(i + jnp.where(core == 0, planes + wide, 0), inner[0, i], inner[1, i], inner[2, i])
        return 0

    lax.fori_loop(0, planes, own, 0)
    lax.fori_loop(0, wide, far, 0)
    lax.fori_loop(0, narrow, close, 0)


def sweeps_kernel(where, y, ya, yb, yc, yd, p0, p1, q, k, out, x0, kp, xs, xt):
    ext, rows, lanes = p0.shape
    share = y.shape[2]
    per_plane = rows // share
    own = y.shape[0] // per_plane
    margin = (ext - own) // 2
    core = where[0]
    inside = pl.ds(PAD, rows)
    zero = jnp.zeros((PAD, lanes), jnp.float32)

    def clear(p, _):
        for x in (xs, xt):
            for c in range(2):
                x[c, p, :PAD] = zero
                x[c, p, PAD + rows :] = zero
        return 0

    lax.fori_loop(0, ext, clear, 0)

    def fill(ref, base):
        def body(i, _):
            e = base + i

            def comp(c):
                return jnp.concatenate(
                    [ref[per_plane * i + h, c].astype(jnp.float32) for h in range(per_plane)],
                    axis=0,
                )

            re, im = comp(0), comp(1)
            c0, c1, cq, ck = p0[e], p1[e], q[e], k[e]
            x0_re = re * c0 + im * cq
            x0_im = im * c1 - re * cq
            x0[0, e], x0[1, e] = x0_re, x0_im
            xs[0, e, inside], xs[1, e, inside] = x0_re, x0_im
            kp[0, e], kp[1, e], kp[2, e] = ck * c0, ck * c1, ck * cq
            return 0

        lax.fori_loop(0, ref.shape[0] // per_plane, body, 0)

    far = yc.shape[0] // per_plane
    fill(y, margin)
    fill(ya, jnp.where(core == 0, far, margin + own))
    fill(yb, jnp.where(core == 0, margin + own, far))
    fill(yc, jnp.where(core == 0, 0, ext - far))
    fill(yd, jnp.where(core == 0, ext - far, 0))

    masks = lane_masks((rows, lanes))
    weights = sweep_weights()
    for step, weight in enumerate(weights):
        src, dst = (xs, xt) if step % 2 == 0 else (xt, xs)
        edge = 2 * (step + 1)
        last = step == len(weights) - 1

        def value(e, src=src, weight=weight):
            re, sum_re = neighbour_sum(src, (0,), e, rows, masks)
            im, sum_im = neighbour_sum(src, (1,), e, rows, masks)
            k0, k1, kq = kp[0, e], kp[1, e], kp[2, e]
            new_re = (1.0 - weight) * re + weight * (x0[0, e] + k0 * sum_re + kq * sum_im)
            new_im = (1.0 - weight) * im + weight * (x0[1, e] + k1 * sum_im - kq * sum_re)
            return new_re, new_im

        def store(e, pair, dst=dst, last=last):
            for c in range(2):
                if not last:
                    dst[c, e, inside] = pair[c]
                    continue
                rounded = pair[c].astype(jnp.bfloat16)
                for h in range(per_plane):
                    out[per_plane * (e - margin) + h, c] = rounded[h * share : (h + 1) * share]

        def sweep(i, _, edge=edge, value=value, store=store):
            planes = [edge + UNROLL * i + r for r in range(UNROLL)]
            pairs = [value(e) for e in planes]
            for e, pair in zip(planes, pairs):
                store(e, pair)
            return 0

        lax.fori_loop(0, (ext - 2 * edge) // UNROLL, sweep, 0)


def final_kernel(where, state, mine, theirs, out):
    planes, rows, _ = state.shape
    share = theirs.shape[1]
    per_plane = rows // share
    half = planes // 2
    core = where[0]

    def one(i, _):
        pieces = [per_plane * i + h for h in range(per_plane)]
        both = ((core, [mine[k, 0] for k in pieces]), (1 - core, [theirs[k] for k in pieces]))
        for side, values in both:
            p = side * half + i
            value = jnp.concatenate([v.astype(jnp.float32) for v in values], axis=0)
            out[p] = (state[p].astype(jnp.float32) + value).astype(jnp.bfloat16)
        return 0

    lax.fori_loop(0, half, one, 0)


def call(kernel, shapes, inputs, scratch=(), scalars=0, anywhere=0, flops=None, vmem=24 << 20):
    outs = [jax.ShapeDtypeStruct(s, d) for s, d in shapes]
    cost = None
    if flops is not None:
        cost = pl.CostEstimate(flops=flops, transcendentals=0, bytes_accessed=flops // 8)
    rest = len(inputs) - scalars - anywhere
    return pl.pallas_call(
        kernel,
        out_shape=outs,
        in_specs=[SMEM] * scalars + [HBM] * anywhere + [VMEM] * rest,
        out_specs=[VMEM] * len(outs),
        scratch_shapes=list(scratch),
        cost_estimate=cost,
        compiler_params=pltpu.CompilerParams(vmem_limit_bytes=vmem),
    )(*inputs)


def iteration(state, initial, forcing, kappa, reaction):
    _, planes, rows, lanes = state.shape
    members = lax.axis_size(TM)
    slots = lax.axis_size(CHIPS)
    slabs = lax.axis_size("space")
    own = planes // 2
    share = own * rows // slots
    per_plane = rows // share
    wide = 2 * SWEEPS
    narrow = wide - own
    ext = own + 2 * wide
    bf16, f32, i32 = jnp.bfloat16, jnp.float32, jnp.int32
    core = lax.axis_index("tm_2")
    slot = lax.axis_index(CHIPS)
    where = jnp.stack([core, slot]).astype(i32)
    u = state[0]

    forward = [(i, i + 1) for i in range(slabs - 1)]
    backward = [(t, s) for s, t in forward]
    outer = []
    for s in range(slabs - 1):
        outer += [(slabs + s, s + 1), (s + 1, slabs + s)]
    swap = [(i, slabs + i) for i in range(slabs)] + [(slabs + i, i) for i in range(slabs)]
    same = forward + [(slabs + s, slabs + t) for s, t in backward]
    lo = lax.ppermute(u[planes - 2 :], "space", forward)
    hi = lax.ppermute(u[:2], "space", backward)
    before = lax.ppermute(u, TM, [(i, i + 1) for i in range(members - 1)])
    block = ((planes, rows, lanes), bf16)
    part, edge, coefs = call(
        local_kernel,
        [
            ((planes, rows, lanes), f32),
            ((4, rows, lanes), f32),
            ((3, wide, rows, lanes), bf16),
        ],
        [where]
        + [
            pltpu.with_memory_space_constraint(v, pltpu.HBM)
            for v in (u, initial, forcing[0], kappa, reaction)
        ],
        [pltpu.VMEM((planes + 4, rows + 2 * PAD, lanes), f32)]
        + [pltpu.VMEM(*block)] * 5
        + [pltpu.SemaphoreType.DMA((5,))],
        scalars=1,
        anywhere=5,
        flops=20_000_000,
        vmem=LARGE,
    )
    rim = lax.ppermute(coefs, CORE_SPACE, outer)
    inner = jnp.where(core == 0, rim[:, wide - narrow :], rim[:, :narrow])
    inner = lax.ppermute(inner, CORE_SPACE, swap)

    thin = ((slots, share, lanes), bf16)
    pair = ((slots, 2, share, lanes), bf16)
    mine, theirs = call(
        residual_kernel, [thin, thin], [where, part, edge, lo, hi, before], scalars=1
    )
    theirs = lax.ppermute(theirs, CORE_SPACE, swap)
    times = jnp.stack([mine, theirs], axis=1)
    cells = lax.all_to_all(times, CHIPS, 0, 0, tiled=True)
    (spectrum,) = call(forward_kernel, [pair], [where, cells], scalars=1)
    y = lax.all_to_all(spectrum, CHIPS, 0, 0, tiled=True)

    fields = call(
        coefficient_kernel,
        [((ext, rows, lanes), f32)] * 4,
        [where, kappa, initial, reaction, rim, inner],
        scalars=1,
    )
    n = per_plane * narrow
    first = core == 0
    ya = lax.ppermute(y, CORE_SPACE, outer)
    yc = lax.ppermute(jnp.where(first, y[-n:], y[:n]), CORE_SPACE, same)
    yb = lax.ppermute(y, CORE_SPACE, swap)
    yd = lax.ppermute(jnp.where(first, ya[-n:], ya[:n]), CORE_SPACE, swap)
    (solved,) = call(
        sweeps_kernel,
        [((slots, 2, share, lanes), bf16)],
        [where, y, ya, yb, yc, yd, *fields],
        [
            pltpu.VMEM((2, ext, rows, lanes), f32),
            pltpu.VMEM((3, ext, rows, lanes), f32),
            pltpu.VMEM((2, ext, rows + 2 * PAD, lanes), f32),
            pltpu.VMEM((2, ext, rows + 2 * PAD, lanes), f32),
        ],
        scalars=1,
    )
    modes = lax.all_to_all(solved, CHIPS, 0, 0, tiled=True)
    (correction,) = call(inverse_kernel, [pair], [where, modes], scalars=1)
    returned = lax.all_to_all(correction, CHIPS, 0, 0, tiled=True)
    other = lax.ppermute(returned[:, 1], CORE_SPACE, swap)
    (updated,) = call(final_kernel, [block], [where, u, returned, other], scalars=1)
    return updated[None]


def solution(mesh):
    torus = Mesh(
        mesh.devices.reshape(2, 8, 2, mesh.shape["space"]), ("tm_0", "tm_1", "tm_2", "space")
    )
    in_specs = (
        P(TM, "space", None, None),
        P("space", None, None),
        P(TM, "space", None, None),
        P("space", None, None),
        P("space", None, None),
    )
    out_specs = P(TM, "space", None, None)
    return jax.shard_map(
        iteration, mesh=torus, in_specs=in_specs, out_specs=out_specs, check_vma=False
    )
```

```python
import math

import jax
import jax.numpy as jnp
from jax import lax
from jax.experimental import pallas as pl
from jax.experimental.pallas import tpu as pltpu
from jax.sharding import Mesh
from jax.sharding import PartitionSpec as P

SWEEPS = 6
STEPS = 32
CHUNK = 16
GROUPS = (14, 12, 10, 8, 12, 8)
TM = ("tm_0", "tm_1", "tm_2")
CHIPS = ("tm_0", "tm_1")
CORE_SPACE = ("tm_2", "space")

alpha_ratio = 0.25
near_weight = 0.5
far_weight = 1.0
centre_weight = 6.0 * (near_weight + far_weight)
VMEM = pl.BlockSpec(memory_space=pltpu.VMEM)
HBM = pl.BlockSpec(memory_space=pltpu.HBM)
SMEM = pl.BlockSpec(memory_space=pltpu.SMEM)
PAD = 8


def sweep_weights():
    return [
        1.0 / (1.0 + 0.4 * math.cos(math.pi * (2 * k + 1) / (2 * SWEEPS))) for k in range(SWEEPS)
    ]


def rotated(re, im, c, s):
    if abs(s) < 1e-12:
        return re * c, im * c
    if abs(c) < 1e-12:
        return -im * s, re * s
    return re * c - im * s, re * s + im * c


def real_dft(x):
    n = len(x)
    if n == 2:
        return [(x[0] + x[1], None), (x[0] - x[1], None)]
    even, odd = real_dft(x[0::2]), real_dft(x[1::2])
    half = n // 2
    out = [None] * (half + 1)
    out[0] = (even[0][0] + odd[0][0], None)
    out[half] = (even[0][0] - odd[0][0], None)
    for k in range(1, n // 4):
        angle = -2.0 * math.pi * k / n
        re, im = rotated(odd[k][0], odd[k][1], math.cos(angle), math.sin(angle))
        out[k] = (even[k][0] + re, even[k][1] + im)
        out[half - k] = (even[k][0] - re, im - even[k][1])
    quarter = n // 4
    out[quarter] = (even[quarter][0], -odd[quarter][0])
    return out


def real_inverse(X):
    half = len(X) - 1
    n = 2 * half
    if n == 2:
        return [X[0][0] + X[1][0], X[0][0] - X[1][0]]
    quarter = n // 4
    even, odd = [None] * (quarter + 1), [None] * (quarter + 1)
    even[0] = (X[0][0] + X[half][0], None)
    odd[0] = (X[0][0] - X[half][0], None)
    for k in range(1, quarter):
        a, b = X[k], X[half - k]
        even[k] = (a[0] + b[0], a[1] - b[1])
        angle = 2.0 * math.pi * k / n
        odd[k] = rotated(a[0] - b[0], a[1] + b[1], math.cos(angle), math.sin(angle))
    even[quarter] = (2.0 * X[quarter][0], None)
    odd[quarter] = (-2.0 * X[quarter][1], None)
    out = [None] * n
    out[0::2] = real_inverse(even)
    out[1::2] = real_inverse(odd)
    return out


def lane_masks(shape):
    lane = lax.broadcasted_iota(jnp.int32, shape, len(shape) - 1)
    last = shape[-1] - 1
    return (
        (1, jnp.where(lane >= 1, near_weight, 0.0)),
        (last, jnp.where(lane <= last - 1, near_weight, 0.0)),
        (2, jnp.where(lane >= 2, far_weight, 0.0)),
        (last - 1, jnp.where(lane <= last - 2, far_weight, 0.0)),
    )


def neighbour_sum(ref, lead, plane, rows, masks):
    def at(dp, dr):
        return ref[(*lead, plane + dp, pl.ds(PAD + dr, rows), slice(None))]

    centre = at(0, 0)
    near = (at(1, 0) + at(-1, 0)) + (at(0, 1) + at(0, -1))
    far = (at(2, 0) + at(-2, 0)) + (at(0, 2) + at(0, -2))
    total = near_weight * near + far_weight * far
    for amount, mask in masks:
        total = total + pltpu.roll(centre, amount, 1) * mask
    return centre, total


def local_kernel(flag, u_hbm, initial_hbm, forcing_hbm, kappa_hbm, reaction_hbm, part, rim, *rest):
    ext, u, initial, forcing, kappa, reaction, sems = rest
    planes, rows, lanes = u.shape
    pairs = ((u_hbm, u), (forcing_hbm, forcing), (kappa_hbm, kappa), (reaction_hbm, reaction))
    pairs += ((initial_hbm, initial),)
    copies = [pltpu.make_async_copy(src, dst, sems.at[i]) for i, (src, dst) in enumerate(pairs)]
    for copy in copies:
        copy.start()
    zero = jnp.zeros((PAD, lanes), jnp.float32)

    def clear(p, _):
        ext[p, :PAD] = zero
        ext[p, PAD + rows :] = zero
        return 0

    lax.fori_loop(0, planes + 4, clear, 0)
    blank = jnp.zeros((rows, lanes), jnp.float32)
    for p in (0, 1, planes + 2, planes + 3):
        ext[p, PAD : PAD + rows] = blank
    for copy in copies:
        copy.wait()

    def fill(p, _):
        ext[p + 2, PAD : PAD + rows] = u[p].astype(jnp.float32)
        return 0

    lax.fori_loop(0, planes, fill, 0)
    masks = lane_masks((rows, lanes))
    first = flag[0] == 0

    def one(p, _):
        centre, total = neighbour_sum(ext, (), p + 2, rows, masks)
        prior = jnp.where(first, initial[p].astype(jnp.float32), 0.0)
        part[p] = (
            forcing[p].astype(jnp.float32)
            - centre
            + prior
            - kappa[p].astype(jnp.float32) * (centre_weight * centre - total)
            - reaction[p].astype(jnp.float32) * centre * centre * centre
        )
        return 0

    lax.fori_loop(0, planes, one, 0)
    for i, p in enumerate((0, 1, planes - 2, planes - 1)):
        rim[i] = kappa[p].astype(jnp.float32)


def residual_kernel(part, rim, lo, hi, before, out):
    planes, rows, _ = part.shape
    share = out.shape[2]
    per_plane = rows // share
    half = planes // 2

    def put(p, value):
        value = value.astype(jnp.bfloat16)
        side, inner = p // half, p % half
        for piece in range(per_plane):
            out[per_plane * inner + piece, side] = value[piece * share : (piece + 1) * share]

    def one(p, _):
        put(p, part[p] + before[p].astype(jnp.float32))
        return 0

    lax.fori_loop(2, planes - 2, one, 0)
    l0, l1, h0, h1 = (v.astype(jnp.float32) for v in (lo[0], lo[1], hi[0], hi[1]))
    edges = (
        (0, near_weight * l1 + far_weight * l0),
        (1, far_weight * l1),
        (planes - 2, far_weight * h0),
        (planes - 1, near_weight * h0 + far_weight * h1),
    )
    for i, (p, total) in enumerate(edges):
        put(p, part[p] + rim[i] * total + before[p].astype(jnp.float32))


def forward_kernel(r, out):
    steps, rows, _ = r.shape
    for start in range(0, rows, 16):
        part = pl.ds(start, 16)
        scaled = [
            r[n, part].astype(jnp.float32) * (alpha_ratio ** (n / steps)) for n in range(steps)
        ]
        spectrum = real_dft(scaled)
        out[0, 0, part] = spectrum[0][0].astype(jnp.bfloat16)
        out[0, 1, part] = spectrum[steps // 2][0].astype(jnp.bfloat16)
        for j in range(1, steps // 2):
            out[j, 0, part] = spectrum[j][0].astype(jnp.bfloat16)
            out[j, 1, part] = spectrum[j][1].astype(jnp.bfloat16)


def inverse_kernel(s, out):
    steps, rows, _ = out.shape
    for start in range(0, rows, 16):
        part = pl.ds(start, 16)
        spectrum = [(s[0, 0, part].astype(jnp.float32), None)]
        for j in range(1, steps // 2):
            spectrum.append((s[j, 0, part].astype(jnp.float32), s[j, 1, part].astype(jnp.float32)))
        spectrum.append((s[0, 1, part].astype(jnp.float32), None))
        values = real_inverse(spectrum)
        for n in range(steps):
            scale = 1.0 / (alpha_ratio ** (n / steps) * steps)
            out[n, part] = (values[n] * scale).astype(jnp.bfloat16)


def coefficient_kernel(where, kappa, initial, reaction, outer, inner, inv, kinv):
    planes = kappa.shape[0]
    wide, narrow = outer.shape[1], inner.shape[1]
    core, slot = where[0], where[1]
    members = STEPS
    factor = math.exp(math.log(alpha_ratio) / members)
    s0 = s1 = si = jnp.float32(0.0)
    for j in range(members // 2):
        phase = 2.0 * math.pi * j / members
        real, imag = 1.0 - factor * math.cos(phase), factor * math.sin(phase)
        hit = slot == j
        s0 = jnp.where(hit, jnp.float32(real), s0)
        s1 = jnp.where(hit, jnp.float32(real if j else 1.0 + factor), s1)
        si = jnp.where(hit, jnp.float32(imag if j else 0.0), si)

    def put(e, kv, iv, rv):
        kv, iv, rv = (v.astype(jnp.float32) for v in (kv, iv, rv))
        base = kv * centre_weight + 3.0 * rv * iv * iv
        d0, d1 = s0 + base, s1 + base
        inv0 = 1.0 / (d0 * d0 + si * si)
        inv1 = 1.0 / (d1 * d1 + si * si)
        for c, value in enumerate((d0 * inv0, d1 * inv1, si * inv0)):
            inv[e, c] = value
            kinv[e, c] = kv * value

    def own(i, _):
        put(i + jnp.where(core == 0, wide, narrow), kappa[i], initial[i], reaction[i])
        return 0

    def far(i, _):
        put(i + jnp.where(core == 0, 0, planes + narrow), outer[0, i], outer[1, i], outer[2, i])
        return 0

    def close(i, _):
        put(i + jnp.where(core == 0, planes + wide, 0), inner[0, i], inner[1, i], inner[2, i])
        return 0

    lax.fori_loop(0, planes, own, 0)
    lax.fori_loop(0, wide, far, 0)
    lax.fori_loop(0, narrow, close, 0)


def sweeps_kernel(where, y, ya, yb, yc, yd, inv, kinv, out, x0, xs, xt, band):
    ext, _, rows, lanes = inv.shape
    share = y.shape[2]
    per_plane = rows // share
    own = y.shape[0] // per_plane
    margin = (ext - own) // 2
    core = where[0]
    starts = (PAD, 2 * PAD + rows)
    zero = jnp.zeros((PAD, lanes), jnp.float32)
    row = lax.broadcasted_iota(jnp.int32, (2 * lanes, lanes), 0)
    row = jnp.where(row >= lanes, row - lanes, row)
    gap = jnp.abs(row - lax.broadcasted_iota(jnp.int32, (2 * lanes, lanes), 1))
    band[...] = jnp.where(gap == 1, near_weight, jnp.where(gap == 2, far_weight, 0.0)).astype(
        jnp.bfloat16
    )

    def clear(e, _):
        for x in (xs, xt):
            for r in (0, PAD + rows, 2 * (PAD + rows)):
                x[e, pl.ds(r, PAD)] = zero
        return 0

    lax.fori_loop(0, ext, clear, 0)

    def fill(ref, base):
        def body(i, _):
            e = base + i
            for h in range(per_plane):
                part = pl.ds(h * share, share)
                re, im = (ref[per_plane * i + h, c].astype(jnp.float32) for c in range(2))
                i0, i1, iq = (inv[e, c, part] for c in range(3))
                for c, value in enumerate((re * i0 + im * iq, im * i1 - re * iq)):
                    x0[e, c, part] = value
                    xs[e, pl.ds(starts[c] + h * share, share)] = value
            return 0

        lax.fori_loop(0, ref.shape[0] // per_plane, body, 0)

    far = yc.shape[0] // per_plane
    fill(y, margin)
    fill(ya, jnp.where(core == 0, far, margin + own))
    fill(yb, jnp.where(core == 0, margin + own, far))
    fill(yc, jnp.where(core == 0, 0, ext - far))
    fill(yd, jnp.where(core == 0, ext - far, 0))

    for step, weight in enumerate(sweep_weights()):
        src, dst = (xs, xt) if step % 2 == 0 else (xt, xs)
        edge = 2 * (step + 1)
        last = step == SWEEPS - 1
        group = GROUPS[step]

        def sweep(i, _, src=src, dst=dst, edge=edge, last=last, group=group, weight=weight):
            first = edge + group * i
            parts = []
            for u in range(group):
                for start in starts:
                    value = src[first + u, pl.ds(start, rows)]
                    high = value.astype(jnp.bfloat16)
                    low = (value - high.astype(jnp.float32)).astype(jnp.bfloat16)
                    parts.append(jnp.concatenate([high, low], axis=1))
            along = jnp.dot(
                jnp.concatenate(parts, axis=0), band[...], preferred_element_type=jnp.float32
            )
            for r in range(0, rows, CHUNK):
                columns = [
                    [src[first + d, pl.ds(start + r, CHUNK)] for d in range(-2, group + 2)]
                    for start in starts
                ]
                for u in range(group):
                    e = first + u

                    def total(c):
                        x = columns[c]
                        side = [src[e, pl.ds(starts[c] + r + d, CHUNK)] for d in (1, -1, 2, -2)]
                        near = (x[u + 3] + x[u + 1]) + (side[0] + side[1])
                        far = (x[u + 4] + x[u]) + (side[2] + side[3])
                        k = (2 * u + c) * rows + r
                        return near_weight * near + far_weight * far + along[k : k + CHUNK]

                    re, im = columns[0][u + 2], columns[1][u + 2]
                    sum_re, sum_im = total(0), total(1)
                    part = pl.ds(r, CHUNK)
                    k0, k1, kq = (kinv[e, c, part] for c in range(3))
                    pair = (
                        (1.0 - weight) * re
                        + weight * (x0[e, 0, part] + k0 * sum_re + kq * sum_im),
                        (1.0 - weight) * im
                        + weight * (x0[e, 1, part] + k1 * sum_im - kq * sum_re),
                    )
                    for c, value in enumerate(pair):
                        if last:
                            k = per_plane * (e - margin) + r // share
                            out[k, c, pl.ds(r % share, CHUNK)] = value.astype(jnp.bfloat16)
                        else:
                            dst[e, pl.ds(starts[c] + r, CHUNK)] = value
            return 0

        lax.fori_loop(0, (ext - 2 * edge) // group, sweep, 0)


def final_kernel(state, correction, out):
    planes, rows, _ = state.shape
    share = correction.shape[2]
    per_plane = rows // share
    half = planes // 2

    def one(p, _):
        part, inner = p // half, p % half
        value = jnp.concatenate(
            [
                correction[per_plane * inner + h, part].astype(jnp.float32)
                for h in range(per_plane)
            ],
            axis=0,
        )
        out[p] = (state[p].astype(jnp.float32) + value).astype(jnp.bfloat16)
        return 0

    lax.fori_loop(0, planes, one, 0)


def call(kernel, shapes, inputs, scratch=(), scalars=0, anywhere=0, flops=None):
    outs = [jax.ShapeDtypeStruct(s, d) for s, d in shapes]
    cost = None
    if flops is not None:
        cost = pl.CostEstimate(flops=flops, transcendentals=0, bytes_accessed=flops // 8)
    rest = len(inputs) - scalars - anywhere
    return pl.pallas_call(
        kernel,
        out_shape=outs,
        in_specs=[SMEM] * scalars + [HBM] * anywhere + [VMEM] * rest,
        out_specs=[VMEM] * len(outs),
        scratch_shapes=list(scratch),
        cost_estimate=cost,
        compiler_params=pltpu.CompilerParams(vmem_limit_bytes=24 << 20),
    )(*inputs)


def iteration(state, initial, forcing, kappa, reaction):
    _, planes, rows, lanes = state.shape
    members = lax.axis_size(TM)
    slots = lax.axis_size(CHIPS)
    slabs = lax.axis_size("space")
    own = planes // 2
    share = own * rows // slots
    per_plane = rows // share
    wide = 2 * SWEEPS
    narrow = wide - own
    ext = own + 2 * wide
    bf16, f32, i32 = jnp.bfloat16, jnp.float32, jnp.int32
    position = lax.axis_index(TM).astype(i32).reshape(1)
    core = lax.axis_index("tm_2")
    slot = lax.axis_index(CHIPS)
    where = jnp.stack([core, slot]).astype(i32)
    u = state[0]

    forward = [(i, i + 1) for i in range(slabs - 1)]
    backward = [(t, s) for s, t in forward]
    outer = []
    for s in range(slabs - 1):
        outer += [(slabs + s, s + 1), (s + 1, slabs + s)]
    swap = [(i, slabs + i) for i in range(slabs)] + [(slabs + i, i) for i in range(slabs)]
    same = forward + [(slabs + s, slabs + t) for s, t in backward]
    lo = lax.ppermute(u[planes - 2 :], "space", forward)
    hi = lax.ppermute(u[:2], "space", backward)
    before = lax.ppermute(u, TM, [(i, i + 1) for i in range(members - 1)])
    coefs = jnp.stack([kappa, initial, reaction])
    rim = jnp.where(core == 0, coefs[:, :wide], coefs[:, planes - wide :])
    rim = lax.ppermute(rim, CORE_SPACE, outer)
    inner = jnp.where(core == 0, rim[:, wide - narrow :], rim[:, :narrow])
    inner = lax.ppermute(inner, CORE_SPACE, swap)

    block = ((planes, rows, lanes), bf16)
    part, edge = call(
        local_kernel,
        [((planes, rows, lanes), f32), ((4, rows, lanes), f32)],
        [position]
        + [
            pltpu.with_memory_space_constraint(v, pltpu.HBM)
            for v in (u, initial, forcing[0], kappa, reaction)
        ],
        [pltpu.VMEM((planes + 4, rows + 2 * PAD, lanes), f32)]
        + [pltpu.VMEM(*block)] * 5
        + [pltpu.SemaphoreType.DMA((5,))],
        scalars=1,
        anywhere=5,
        flops=20_000_000,
    )
    (residual,) = call(
        residual_kernel, [((slots, 2, share, lanes), bf16)], [part, edge, lo, hi, before]
    )
    cells = lax.all_to_all(residual.reshape(members, share, lanes), TM, 0, 0, tiled=True)
    (spectrum,) = call(forward_kernel, [((slots, 2, share, lanes), bf16)], [cells])
    y = lax.all_to_all(spectrum, CHIPS, 0, 0, tiled=True)

    fields = call(
        coefficient_kernel,
        [((ext, 3, rows, lanes), f32)] * 2,
        [where, kappa, initial, reaction, rim, inner],
        scalars=1,
    )
    n = per_plane * narrow
    first = core == 0
    ya = lax.ppermute(y, CORE_SPACE, outer)
    yc = lax.ppermute(jnp.where(first, y[-n:], y[:n]), CORE_SPACE, same)
    yb = lax.ppermute(y, CORE_SPACE, swap)
    yd = lax.ppermute(jnp.where(first, ya[-n:], ya[:n]), CORE_SPACE, swap)
    (solved,) = call(
        sweeps_kernel,
        [((slots, 2, share, lanes), bf16)],
        [where, y, ya, yb, yc, yd, *fields],
        [
            pltpu.VMEM((ext, 2, rows + PAD, lanes), f32),
            pltpu.VMEM((ext, 2 * rows + 3 * PAD, lanes), f32),
            pltpu.VMEM((ext, 2 * rows + 3 * PAD, lanes), f32),
            pltpu.VMEM((2 * lanes, lanes), bf16),
        ],
        scalars=1,
    )
    modes = lax.all_to_all(solved, CHIPS, 0, 0, tiled=True)
    (correction,) = call(inverse_kernel, [((members, share, lanes), bf16)], [modes])
    returned = lax.all_to_all(correction, TM, 0, 0, tiled=True)
    (updated,) = call(
        final_kernel, [((planes, rows, lanes), bf16)], [u, returned.reshape(slots, 2, share, lanes)]
    )
    return updated[None]


def solution(mesh):
    torus = Mesh(
        mesh.devices.reshape(2, 8, 2, mesh.shape["space"]), ("tm_0", "tm_1", "tm_2", "space")
    )
    in_specs = (
        P(TM, "space", None, None),
        P("space", None, None),
        P(TM, "space", None, None),
        P("space", None, None),
        P("space", None, None),
    )
    out_specs = P(TM, "space", None, None)
    return jax.shard_map(
        iteration, mesh=torus, in_specs=in_specs, out_specs=out_specs, check_vma=False
    )
```

```python
import math

import jax
import jax.numpy as jnp
from jax import lax
from jax.experimental import pallas as pl
from jax.experimental.pallas import tpu as pltpu
from jax.sharding import Mesh
from jax.sharding import PartitionSpec as P

SWEEPS = 6
STEPS = 32
CHUNK = 16
TM = ("tm_0", "tm_1", "tm_2")
CHIPS = ("tm_0", "tm_1")
CORE_SPACE = ("tm_2", "space")

alpha_ratio = 0.25
near_weight = 0.5
far_weight = 1.0
centre_weight = 6.0 * (near_weight + far_weight)
VMEM = pl.BlockSpec(memory_space=pltpu.VMEM)
HBM = pl.BlockSpec(memory_space=pltpu.HBM)
SMEM = pl.BlockSpec(memory_space=pltpu.SMEM)
PAD = 8


def sweep_weights():
    return [
        1.0 / (1.0 + 0.4 * math.cos(math.pi * (2 * k + 1) / (2 * SWEEPS))) for k in range(SWEEPS)
    ]


def in_groups(count, body, group=4):
    def step(i, _):
        for u in range(group):
            body(group * i + u)
        return 0

    lax.fori_loop(0, count // group, step, 0)


def rotated(re, im, c, s):
    if abs(s) < 1e-12:
        return re * c, im * c
    if abs(c) < 1e-12:
        return -im * s, re * s
    return re * c - im * s, re * s + im * c


def real_dft(x):
    n = len(x)
    if n == 2:
        return [(x[0] + x[1], None), (x[0] - x[1], None)]
    even, odd = real_dft(x[0::2]), real_dft(x[1::2])
    half = n // 2
    out = [None] * (half + 1)
    out[0] = (even[0][0] + odd[0][0], None)
    out[half] = (even[0][0] - odd[0][0], None)
    for k in range(1, n // 4):
        angle = -2.0 * math.pi * k / n
        re, im = rotated(odd[k][0], odd[k][1], math.cos(angle), math.sin(angle))
        out[k] = (even[k][0] + re, even[k][1] + im)
        out[half - k] = (even[k][0] - re, im - even[k][1])
    quarter = n // 4
    out[quarter] = (even[quarter][0], -odd[quarter][0])
    return out


def real_inverse(X):
    half = len(X) - 1
    n = 2 * half
    if n == 2:
        return [X[0][0] + X[1][0], X[0][0] - X[1][0]]
    quarter = n // 4
    even, odd = [None] * (quarter + 1), [None] * (quarter + 1)
    even[0] = (X[0][0] + X[half][0], None)
    odd[0] = (X[0][0] - X[half][0], None)
    for k in range(1, quarter):
        a, b = X[k], X[half - k]
        even[k] = (a[0] + b[0], a[1] - b[1])
        angle = 2.0 * math.pi * k / n
        odd[k] = rotated(a[0] - b[0], a[1] + b[1], math.cos(angle), math.sin(angle))
    even[quarter] = (2.0 * X[quarter][0], None)
    odd[quarter] = (-2.0 * X[quarter][1], None)
    out = [None] * n
    out[0::2] = real_inverse(even)
    out[1::2] = real_inverse(odd)
    return out


def lane_masks(shape):
    lane = lax.broadcasted_iota(jnp.int32, shape, len(shape) - 1)
    last = shape[-1] - 1
    return (
        (1, jnp.where(lane >= 1, near_weight, 0.0)),
        (last, jnp.where(lane <= last - 1, near_weight, 0.0)),
        (2, jnp.where(lane >= 2, far_weight, 0.0)),
        (last - 1, jnp.where(lane <= last - 2, far_weight, 0.0)),
    )


def neighbour_sum(ref, lead, plane, rows, masks):
    def at(dp, dr):
        return ref[(*lead, plane + dp, pl.ds(PAD + dr, rows), slice(None))]

    centre = at(0, 0)
    near = (at(1, 0) + at(-1, 0)) + (at(0, 1) + at(0, -1))
    far = (at(2, 0) + at(-2, 0)) + (at(0, 2) + at(0, -2))
    total = near_weight * near + far_weight * far
    for amount, mask in masks:
        total = total + pltpu.roll(centre, amount, 1) * mask
    return centre, total


def local_kernel(where, u_hbm, initial_hbm, forcing_hbm, kappa_hbm, reaction_hbm, part, rim, *rest):
    ext, u, initial, forcing, kappa, reaction, sems = rest
    planes, rows, lanes = u.shape
    pairs = ((u_hbm, u), (forcing_hbm, forcing), (kappa_hbm, kappa), (reaction_hbm, reaction))
    pairs += ((initial_hbm, initial),)
    copies = [pltpu.make_async_copy(src, dst, sems.at[i]) for i, (src, dst) in enumerate(pairs)]
    for copy in copies:
        copy.start()
    zero = jnp.zeros((PAD, lanes), jnp.float32)

    def clear(p):
        ext[p, :PAD] = zero
        ext[p, PAD + rows :] = zero

    in_groups(planes + 4, clear)
    blank = jnp.zeros((rows, lanes), jnp.float32)
    for p in (0, 1, planes + 2, planes + 3):
        ext[p, PAD : PAD + rows] = blank
    copies[0].wait()

    def fill(p):
        ext[p + 2, PAD : PAD + rows] = u[p].astype(jnp.float32)

    in_groups(planes, fill)
    for copy in copies[1:]:
        copy.wait()
    masks = lane_masks((rows, lanes))
    first = jnp.logical_and(where[0] == 0, where[1] == 0)

    def one(p):
        centre, total = neighbour_sum(ext, (), p + 2, rows, masks)
        prior = jnp.where(first, initial[p].astype(jnp.float32), 0.0)
        part[p] = (
            forcing[p].astype(jnp.float32)
            - centre
            + prior
            - kappa[p].astype(jnp.float32) * (centre_weight * centre - total)
            - reaction[p].astype(jnp.float32) * centre * centre * centre
        )

    in_groups(planes, one)
    for i, p in enumerate((0, 1, planes - 2, planes - 1)):
        rim[i] = kappa[p].astype(jnp.float32)


def residual_kernel(odd, part, rim, even_pair, odd_pair, before, out):
    planes, rows, _ = part.shape
    share = out.shape[2]
    per_plane = rows // share
    half = planes // 2

    def put(p, value):
        value = value.astype(jnp.bfloat16)
        side, inner = p // half, p % half
        for piece in range(per_plane):
            out[per_plane * inner + piece, side] = value[piece * share : (piece + 1) * share]

    for p in range(2, planes - 2):
        put(p, part[p] + before[p].astype(jnp.float32))
    upper = odd[0] == 1

    def chosen(a, b, i):
        return jnp.where(upper, a[i].astype(jnp.float32), b[i].astype(jnp.float32))

    l0, l1 = (chosen(even_pair, odd_pair, i) for i in range(2))
    h0, h1 = (chosen(odd_pair, even_pair, i) for i in range(2))
    edges = (
        (0, near_weight * l1 + far_weight * l0),
        (1, far_weight * l1),
        (planes - 2, far_weight * h0),
        (planes - 1, near_weight * h0 + far_weight * h1),
    )
    for i, (p, total) in enumerate(edges):
        put(p, part[p] + rim[i] * total + before[p].astype(jnp.float32))


def forward_kernel(r, out):
    steps, rows, _ = r.shape
    for start in range(0, rows, 16):
        part = pl.ds(start, 16)
        scaled = [
            r[n, part].astype(jnp.float32) * (alpha_ratio ** (n / steps)) for n in range(steps)
        ]
        spectrum = real_dft(scaled)
        out[0, 0, part] = spectrum[0][0].astype(jnp.bfloat16)
        out[0, 1, part] = spectrum[steps // 2][0].astype(jnp.bfloat16)
        for j in range(1, steps // 2):
            out[j, 0, part] = spectrum[j][0].astype(jnp.bfloat16)
            out[j, 1, part] = spectrum[j][1].astype(jnp.bfloat16)


def inverse_kernel(s, out):
    steps, rows, _ = out.shape
    for start in range(0, rows, 16):
        part = pl.ds(start, 16)
        spectrum = [(s[0, 0, part].astype(jnp.float32), None)]
        for j in range(1, steps // 2):
            spectrum.append((s[j, 0, part].astype(jnp.float32), s[j, 1, part].astype(jnp.float32)))
        spectrum.append((s[0, 1, part].astype(jnp.float32), None))
        values = real_inverse(spectrum)
        for n in range(steps):
            scale = 1.0 / (alpha_ratio ** (n / steps) * steps)
            out[n, part] = (values[n] * scale).astype(jnp.bfloat16)


def coefficient_kernel(where, kappa, initial, reaction, outer, inner, inv, kinv):
    planes = kappa.shape[0]
    wide, narrow = outer.shape[1], inner.shape[1]
    core, slot = where[0], where[1]
    members = STEPS
    factor = math.exp(math.log(alpha_ratio) / members)
    s0 = s1 = si = jnp.float32(0.0)
    for j in range(members // 2):
        phase = 2.0 * math.pi * j / members
        real, imag = 1.0 - factor * math.cos(phase), factor * math.sin(phase)
        hit = slot == j
        s0 = jnp.where(hit, jnp.float32(real), s0)
        s1 = jnp.where(hit, jnp.float32(real if j else 1.0 + factor), s1)
        si = jnp.where(hit, jnp.float32(imag if j else 0.0), si)

    def put(e, kv, iv, rv):
        kv, iv, rv = (v.astype(jnp.float32) for v in (kv, iv, rv))
        base = kv * centre_weight + 3.0 * rv * iv * iv
        d0, d1 = s0 + base, s1 + base
        inv0 = 1.0 / (d0 * d0 + si * si)
        inv1 = 1.0 / (d1 * d1 + si * si)
        for c, value in enumerate((d0 * inv0, d1 * inv1, si * inv0)):
            inv[e, c] = value
            kinv[e, c] = kv * value

    def own(i):
        put(i + jnp.where(core == 0, wide, narrow), kappa[i], initial[i], reaction[i])

    def far(i):
        put(i + jnp.where(core == 0, 0, planes + narrow), outer[0, i], outer[1, i], outer[2, i])

    def close(i):
        put(i + jnp.where(core == 0, planes + wide, 0), inner[0, i], inner[1, i], inner[2, i])

    in_groups(planes, own, 2)
    in_groups(wide, far, 2)
    in_groups(narrow, close, 2)


def sweeps_kernel(where, y, ya, yb, yc, yd, inv, kinv, out, x0, xs, xt, band):
    ext, _, rows, lanes = inv.shape
    share = y.shape[2]
    per_plane = rows // share
    own = y.shape[0] // per_plane
    margin = (ext - own) // 2
    core = where[0]
    starts = (PAD, 2 * PAD + rows)
    zero = jnp.zeros((PAD, lanes), jnp.float32)
    row = lax.broadcasted_iota(jnp.int32, (2 * lanes, lanes), 0)
    row = jnp.where(row >= lanes, row - lanes, row)
    gap = jnp.abs(row - lax.broadcasted_iota(jnp.int32, (2 * lanes, lanes), 1))
    band[...] = jnp.where(gap == 1, near_weight, jnp.where(gap == 2, far_weight, 0.0)).astype(
        jnp.bfloat16
    )

    def clear(e):
        for x in (xs, xt):
            for r in (0, PAD + rows, 2 * (PAD + rows)):
                x[e, pl.ds(r, PAD)] = zero

    in_groups(ext, clear)

    def fill(ref, base):
        def body(i):
            e = base + i
            for h in range(per_plane):
                part = pl.ds(h * share, share)
                re, im = (ref[per_plane * i + h, c].astype(jnp.float32) for c in range(2))
                i0, i1, iq = (inv[e, c, part] for c in range(3))
                for c, value in enumerate((re * i0 + im * iq, im * i1 - re * iq)):
                    x0[e, c, part] = value
                    xs[e, pl.ds(starts[c] + h * share, share)] = value

        in_groups(ref.shape[0] // per_plane, body)

    far = yc.shape[0] // per_plane
    fill(y, margin)
    fill(ya, jnp.where(core == 0, far, margin + own))
    fill(yb, jnp.where(core == 0, margin + own, far))
    fill(yc, jnp.where(core == 0, 0, ext - far))
    fill(yd, jnp.where(core == 0, ext - far, 0))

    for step, weight in enumerate(sweep_weights()):
        src, dst = (xs, xt) if step % 2 == 0 else (xt, xs)
        edge = 2 * (step + 1)
        last = step == SWEEPS - 1
        group = ext - 2 * edge

        def sweep(src=src, dst=dst, first=edge, last=last, group=group, weight=weight):
            parts = []
            for u in range(group):
                for start in starts:
                    value = src[first + u, pl.ds(start, rows)]
                    high = value.astype(jnp.bfloat16)
                    low = (value - high.astype(jnp.float32)).astype(jnp.bfloat16)
                    parts.append(jnp.concatenate([high, low], axis=1))
            along = jnp.dot(
                jnp.concatenate(parts, axis=0), band[...], preferred_element_type=jnp.float32
            )
            for r in range(0, rows, CHUNK):
                columns = [
                    [src[first + d, pl.ds(start + r, CHUNK)] for d in range(-2, group + 2)]
                    for start in starts
                ]
                for u in range(group):
                    e = first + u

                    def total(c):
                        x = columns[c]
                        side = [src[e, pl.ds(starts[c] + r + d, CHUNK)] for d in (1, -1, 2, -2)]
                        near = (x[u + 3] + x[u + 1]) + (side[0] + side[1])
                        far = (x[u + 4] + x[u]) + (side[2] + side[3])
                        k = (2 * u + c) * rows + r
                        return near_weight * near + far_weight * far + along[k : k + CHUNK]

                    re, im = columns[0][u + 2], columns[1][u + 2]
                    sum_re, sum_im = total(0), total(1)
                    part = pl.ds(r, CHUNK)
                    k0, k1, kq = (kinv[e, c, part] for c in range(3))
                    pair = (
                        (1.0 - weight) * re
                        + weight * (x0[e, 0, part] + k0 * sum_re + kq * sum_im),
                        (1.0 - weight) * im
                        + weight * (x0[e, 1, part] + k1 * sum_im - kq * sum_re),
                    )
                    for c, value in enumerate(pair):
                        if last:
                            k = per_plane * (e - margin) + r // share
                            out[k, c, pl.ds(r % share, CHUNK)] = value.astype(jnp.bfloat16)
                        else:
                            dst[e, pl.ds(starts[c] + r, CHUNK)] = value

        sweep()


def final_kernel(state, correction, out):
    planes, rows, _ = state.shape
    share = correction.shape[2]
    per_plane = rows // share
    half = planes // 2

    for p in range(planes):
        part, inner = p // half, p % half
        value = jnp.concatenate(
            [
                correction[per_plane * inner + h, part].astype(jnp.float32)
                for h in range(per_plane)
            ],
            axis=0,
        )
        out[p] = (state[p].astype(jnp.float32) + value).astype(jnp.bfloat16)


def call(kernel, shapes, inputs, scratch=(), scalars=0, anywhere=0, flops=None):
    outs = [jax.ShapeDtypeStruct(s, d) for s, d in shapes]
    cost = None
    if flops is not None:
        cost = pl.CostEstimate(flops=flops, transcendentals=0, bytes_accessed=flops // 8)
    rest = len(inputs) - scalars - anywhere
    return pl.pallas_call(
        kernel,
        out_shape=outs,
        in_specs=[SMEM] * scalars + [HBM] * anywhere + [VMEM] * rest,
        out_specs=[VMEM] * len(outs),
        scratch_shapes=list(scratch),
        cost_estimate=cost,
        compiler_params=pltpu.CompilerParams(vmem_limit_bytes=24 << 20),
    )(*inputs)


def iteration(state, initial, forcing, kappa, reaction):
    _, planes, rows, lanes = state.shape
    members = lax.axis_size(TM)
    slots = lax.axis_size(CHIPS)
    slabs = lax.axis_size("space")
    own = planes // 2
    share = own * rows // slots
    per_plane = rows // share
    wide = 2 * SWEEPS
    narrow = wide - own
    ext = own + 2 * wide
    bf16, f32, i32 = jnp.bfloat16, jnp.float32, jnp.int32
    core = lax.axis_index("tm_2")
    slot = lax.axis_index(CHIPS)
    where = jnp.stack([core, slot]).astype(i32)
    u = state[0]

    forward = [(i, i + 1) for i in range(slabs - 1)]
    backward = [(t, s) for s, t in forward]
    outer = []
    for s in range(slabs - 1):
        outer += [(slabs + s, s + 1), (s + 1, slabs + s)]
    swap = [(i, slabs + i) for i in range(slabs)] + [(slabs + i, i) for i in range(slabs)]
    same = forward + [(slabs + s, slabs + t) for s, t in backward]
    odd = lax.axis_index("space") % 2
    even_first = [p for s in range(0, slabs - 1, 2) for p in ((s, s + 1), (s + 1, s))]
    odd_first = [p for s in range(1, slabs - 1, 2) for p in ((s, s + 1), (s + 1, s))]
    low, high = u[:2], u[planes - 2 :]
    even_pair = lax.ppermute(jnp.where(odd == 1, low, high), "space", even_first)
    odd_pair = lax.ppermute(jnp.where(odd == 1, high, low), "space", odd_first)
    before = lax.ppermute(u, TM, [(i, i + 1) for i in range(members - 1)])
    coefs = jnp.stack([kappa, initial, reaction])
    rim = jnp.where(core == 0, coefs[:, :wide], coefs[:, planes - wide :])
    rim = lax.ppermute(rim, CORE_SPACE, outer)
    inner = jnp.where(core == 0, rim[:, wide - narrow :], rim[:, :narrow])
    inner = lax.ppermute(inner, CORE_SPACE, swap)

    block = ((planes, rows, lanes), bf16)
    part, edge = call(
        local_kernel,
        [((planes, rows, lanes), f32), ((4, rows, lanes), f32)],
        [where]
        + [
            pltpu.with_memory_space_constraint(v, pltpu.HBM)
            for v in (u, initial, forcing[0], kappa, reaction)
        ],
        [pltpu.VMEM((planes + 4, rows + 2 * PAD, lanes), f32)]
        + [pltpu.VMEM(*block)] * 5
        + [pltpu.SemaphoreType.DMA((5,))],
        scalars=1,
        anywhere=5,
        flops=20_000_000,
    )
    (residual,) = call(
        residual_kernel,
        [((slots, 2, share, lanes), bf16)],
        [odd.astype(i32).reshape(1), part, edge, even_pair, odd_pair, before],
        scalars=1,
    )
    cells = lax.all_to_all(residual.reshape(members, share, lanes), TM, 0, 0, tiled=True)
    (spectrum,) = call(forward_kernel, [((slots, 2, share, lanes), bf16)], [cells])
    y = lax.all_to_all(spectrum, CHIPS, 0, 0, tiled=True)

    fields = call(
        coefficient_kernel,
        [((ext, 3, rows, lanes), f32)] * 2,
        [where, kappa, initial, reaction, rim, inner],
        scalars=1,
    )
    n = per_plane * narrow
    first = core == 0
    ya = lax.ppermute(y, CORE_SPACE, outer)
    yc = lax.ppermute(jnp.where(first, y[-n:], y[:n]), CORE_SPACE, same)
    yb = lax.ppermute(y, CORE_SPACE, swap)
    yd = lax.ppermute(jnp.where(first, ya[-n:], ya[:n]), CORE_SPACE, swap)
    (solved,) = call(
        sweeps_kernel,
        [((slots, 2, share, lanes), bf16)],
        [where, y, ya, yb, yc, yd, *fields],
        [
            pltpu.VMEM((ext, 2, rows + PAD, lanes), f32),
            pltpu.VMEM((ext, 2 * rows + 3 * PAD, lanes), f32),
            pltpu.VMEM((ext, 2 * rows + 3 * PAD, lanes), f32),
            pltpu.VMEM((2 * lanes, lanes), bf16),
        ],
        scalars=1,
    )
    modes = lax.all_to_all(solved, CHIPS, 0, 0, tiled=True)
    (correction,) = call(inverse_kernel, [((members, share, lanes), bf16)], [modes])
    returned = lax.all_to_all(correction, TM, 0, 0, tiled=True)
    (updated,) = call(
        final_kernel, [((planes, rows, lanes), bf16)], [u, returned.reshape(slots, 2, share, lanes)]
    )
    return updated[None]


def solution(mesh):
    torus = Mesh(
        mesh.devices.reshape(2, 8, 2, mesh.shape["space"]), ("tm_0", "tm_1", "tm_2", "space")
    )
    in_specs = (
        P(TM, "space", None, None),
        P("space", None, None),
        P(TM, "space", None, None),
        P("space", None, None),
        P("space", None, None),
    )
    out_specs = P(TM, "space", None, None)
    return jax.shard_map(
        iteration, mesh=torus, in_specs=in_specs, out_specs=out_specs, check_vma=False
    )
```

```python
import math

import jax
import jax.numpy as jnp
from jax import lax
from jax.experimental import pallas as pl
from jax.experimental.pallas import tpu as pltpu
from jax.sharding import Mesh
from jax.sharding import PartitionSpec as P

SWEEPS = 6
STEPS = 32
CHUNK = 16
EARLY = 3
TM = ("tm_0", "tm_1", "tm_2")
CHIPS = ("tm_0", "tm_1")
CORE_SPACE = ("tm_2", "space")

alpha_ratio = 0.25
near_weight = 0.5
far_weight = 1.0
centre_weight = 6.0 * (near_weight + far_weight)
VMEM = pl.BlockSpec(memory_space=pltpu.VMEM)
HBM = pl.BlockSpec(memory_space=pltpu.HBM)
SMEM = pl.BlockSpec(memory_space=pltpu.SMEM)
PAD = 8


def sweep_weights():
    return [
        1.0 / (1.0 + 0.4 * math.cos(math.pi * (2 * k + 1) / (2 * SWEEPS))) for k in range(SWEEPS)
    ]


def in_groups(count, body, group=4):
    def step(i, _):
        for u in range(group):
            body(group * i + u)
        return 0

    lax.fori_loop(0, count // group, step, 0)


def rotated(re, im, c, s):
    if abs(s) < 1e-12:
        return re * c, im * c
    if abs(c) < 1e-12:
        return -im * s, re * s
    return re * c - im * s, re * s + im * c


def real_dft(x):
    n = len(x)
    if n == 2:
        return [(x[0] + x[1], None), (x[0] - x[1], None)]
    even, odd = real_dft(x[0::2]), real_dft(x[1::2])
    half = n // 2
    out = [None] * (half + 1)
    out[0] = (even[0][0] + odd[0][0], None)
    out[half] = (even[0][0] - odd[0][0], None)
    for k in range(1, n // 4):
        angle = -2.0 * math.pi * k / n
        re, im = rotated(odd[k][0], odd[k][1], math.cos(angle), math.sin(angle))
        out[k] = (even[k][0] + re, even[k][1] + im)
        out[half - k] = (even[k][0] - re, im - even[k][1])
    quarter = n // 4
    out[quarter] = (even[quarter][0], -odd[quarter][0])
    return out


def real_inverse(X):
    half = len(X) - 1
    n = 2 * half
    if n == 2:
        return [X[0][0] + X[1][0], X[0][0] - X[1][0]]
    quarter = n // 4
    even, odd = [None] * (quarter + 1), [None] * (quarter + 1)
    even[0] = (X[0][0] + X[half][0], None)
    odd[0] = (X[0][0] - X[half][0], None)
    for k in range(1, quarter):
        a, b = X[k], X[half - k]
        even[k] = (a[0] + b[0], a[1] - b[1])
        angle = 2.0 * math.pi * k / n
        odd[k] = rotated(a[0] - b[0], a[1] + b[1], math.cos(angle), math.sin(angle))
    even[quarter] = (2.0 * X[quarter][0], None)
    odd[quarter] = (-2.0 * X[quarter][1], None)
    out = [None] * n
    out[0::2] = real_inverse(even)
    out[1::2] = real_inverse(odd)
    return out


def lane_masks(shape):
    lane = lax.broadcasted_iota(jnp.int32, shape, len(shape) - 1)
    last = shape[-1] - 1
    return (
        (1, jnp.where(lane >= 1, near_weight, 0.0)),
        (last, jnp.where(lane <= last - 1, near_weight, 0.0)),
        (2, jnp.where(lane >= 2, far_weight, 0.0)),
        (last - 1, jnp.where(lane <= last - 2, far_weight, 0.0)),
    )


def neighbour_sum(ref, lead, plane, rows, masks):
    def at(dp, dr):
        return ref[(*lead, plane + dp, pl.ds(PAD + dr, rows), slice(None))]

    centre = at(0, 0)
    near = (at(1, 0) + at(-1, 0)) + (at(0, 1) + at(0, -1))
    far = (at(2, 0) + at(-2, 0)) + (at(0, 2) + at(0, -2))
    total = near_weight * near + far_weight * far
    for amount, mask in masks:
        total = total + pltpu.roll(centre, amount, 1) * mask
    return centre, total


def local_kernel(where, u_hbm, initial_hbm, forcing_hbm, kappa_hbm, reaction_hbm, part, rim, *rest):
    ext, u, initial, forcing, kappa, reaction, sems = rest
    planes, rows, lanes = u.shape
    pairs = ((u_hbm, u), (forcing_hbm, forcing), (kappa_hbm, kappa), (reaction_hbm, reaction))
    pairs += ((initial_hbm, initial),)
    copies = [pltpu.make_async_copy(src, dst, sems.at[i]) for i, (src, dst) in enumerate(pairs)]
    for copy in copies:
        copy.start()
    zero = jnp.zeros((PAD, lanes), jnp.float32)

    def clear(p):
        ext[p, :PAD] = zero
        ext[p, PAD + rows :] = zero

    in_groups(planes + 4, clear)
    blank = jnp.zeros((rows, lanes), jnp.float32)
    for p in (0, 1, planes + 2, planes + 3):
        ext[p, PAD : PAD + rows] = blank
    copies[0].wait()

    def fill(p):
        ext[p + 2, PAD : PAD + rows] = u[p].astype(jnp.float32)

    in_groups(planes, fill)
    for copy in copies[1:]:
        copy.wait()
    masks = lane_masks((rows, lanes))
    first = jnp.logical_and(where[0] == 0, where[1] == 0)

    def one(p):
        centre, total = neighbour_sum(ext, (), p + 2, rows, masks)
        prior = jnp.where(first, initial[p].astype(jnp.float32), 0.0)
        part[p] = (
            forcing[p].astype(jnp.float32)
            - centre
            + prior
            - kappa[p].astype(jnp.float32) * (centre_weight * centre - total)
            - reaction[p].astype(jnp.float32) * centre * centre * centre
        )

    in_groups(planes, one)
    for i, p in enumerate((0, 1, planes - 2, planes - 1)):
        rim[i] = kappa[p].astype(jnp.float32)


def residual_kernel(odd, part, rim, even_pair, odd_pair, before, out):
    planes, rows, _ = part.shape
    share = out.shape[2]
    per_plane = rows // share
    half = planes // 2

    def put(p, value):
        value = value.astype(jnp.bfloat16)
        side, inner = p // half, p % half
        for piece in range(per_plane):
            out[per_plane * inner + piece, side] = value[piece * share : (piece + 1) * share]

    for p in range(2, planes - 2):
        put(p, part[p] + before[p].astype(jnp.float32))
    upper = odd[0] == 1

    def chosen(a, b, i):
        return jnp.where(upper, a[i].astype(jnp.float32), b[i].astype(jnp.float32))

    l0, l1 = (chosen(even_pair, odd_pair, i) for i in range(2))
    h0, h1 = (chosen(odd_pair, even_pair, i) for i in range(2))
    edges = (
        (0, near_weight * l1 + far_weight * l0),
        (1, far_weight * l1),
        (planes - 2, far_weight * h0),
        (planes - 1, near_weight * h0 + far_weight * h1),
    )
    for i, (p, total) in enumerate(edges):
        put(p, part[p] + rim[i] * total + before[p].astype(jnp.float32))


def forward_kernel(r, out):
    steps, rows, _ = r.shape
    for start in range(0, rows, 16):
        part = pl.ds(start, 16)
        scaled = [
            r[n, part].astype(jnp.float32) * (alpha_ratio ** (n / steps)) for n in range(steps)
        ]
        spectrum = real_dft(scaled)
        out[0, 0, part] = spectrum[0][0].astype(jnp.bfloat16)
        out[0, 1, part] = spectrum[steps // 2][0].astype(jnp.bfloat16)
        for j in range(1, steps // 2):
            out[j, 0, part] = spectrum[j][0].astype(jnp.bfloat16)
            out[j, 1, part] = spectrum[j][1].astype(jnp.bfloat16)


def inverse_kernel(s, out):
    steps, rows, _ = out.shape
    for start in range(0, rows, 16):
        part = pl.ds(start, 16)
        spectrum = [(s[0, 0, part].astype(jnp.float32), None)]
        for j in range(1, steps // 2):
            spectrum.append((s[j, 0, part].astype(jnp.float32), s[j, 1, part].astype(jnp.float32)))
        spectrum.append((s[0, 1, part].astype(jnp.float32), None))
        values = real_inverse(spectrum)
        for n in range(steps):
            scale = 1.0 / (alpha_ratio ** (n / steps) * steps)
            out[n, part] = (values[n] * scale).astype(jnp.bfloat16)


def mirrored(core, i, count):
    return jnp.where(core == 0, i, count - 1 - i)


def coefficient_kernel(where, kappa, initial, reaction, outer, inner, inv, kinv):
    planes = kappa.shape[0]
    wide, narrow = outer.shape[1], inner.shape[1]
    core, slot = where[0], where[1]
    members = STEPS
    factor = math.exp(math.log(alpha_ratio) / members)
    s0 = s1 = si = jnp.float32(0.0)
    for j in range(members // 2):
        phase = 2.0 * math.pi * j / members
        real, imag = 1.0 - factor * math.cos(phase), factor * math.sin(phase)
        hit = slot == j
        s0 = jnp.where(hit, jnp.float32(real), s0)
        s1 = jnp.where(hit, jnp.float32(real if j else 1.0 + factor), s1)
        si = jnp.where(hit, jnp.float32(imag if j else 0.0), si)

    def put(e, kv, iv, rv):
        kv, iv, rv = (v.astype(jnp.float32) for v in (kv, iv, rv))
        base = kv * centre_weight + 3.0 * rv * iv * iv
        d0, d1 = s0 + base, s1 + base
        inv0 = 1.0 / (d0 * d0 + si * si)
        inv1 = 1.0 / (d1 * d1 + si * si)
        for c, value in enumerate((d0 * inv0, d1 * inv1, si * inv0)):
            inv[e, c] = value
            kinv[e, c] = kv * value

    def own(i):
        put(wide + mirrored(core, i, planes), kappa[i], initial[i], reaction[i])

    def far(i):
        put(mirrored(core, i, wide), outer[0, i], outer[1, i], outer[2, i])

    def close(i):
        put(wide + planes + mirrored(core, i, narrow), inner[0, i], inner[1, i], inner[2, i])

    in_groups(planes, own, 2)
    in_groups(wide, far, 2)
    in_groups(narrow, close, 2)


def row_starts(rows):
    return (PAD, 2 * PAD + rows)


def write_band(band):
    double, lanes = band.shape
    row = lax.broadcasted_iota(jnp.int32, (double, lanes), 0)
    row = jnp.where(row >= lanes, row - lanes, row)
    gap = jnp.abs(row - lax.broadcasted_iota(jnp.int32, (double, lanes), 1))
    weights = jnp.where(gap == 1, near_weight, jnp.where(gap == 2, far_weight, 0.0))
    band[...] = weights.astype(jnp.bfloat16)


def fill(core, ref, base, inv, x0, x):
    share, rows = ref.shape[2], inv.shape[2]
    per_plane = rows // share
    count = ref.shape[0] // per_plane
    starts = row_starts(rows)

    def body(i):
        e = base + mirrored(core, i, count)
        for h in range(per_plane):
            part = pl.ds(h * share, share)
            re, im = (ref[per_plane * i + h, c].astype(jnp.float32) for c in range(2))
            i0, i1, iq = (inv[e, c, part] for c in range(3))
            for c, value in enumerate((re * i0 + im * iq, im * i1 - re * iq)):
                x0[e, c, part] = value
                x[e, pl.ds(starts[c] + h * share, share)] = value

    in_groups(count, body)


def sweep(step, first, stop, x0, kinv, band, buffers, emit=None):
    rows = kinv.shape[2]
    starts = row_starts(rows)
    src, dst = buffers[step % 2], buffers[(step + 1) % 2]
    weight = sweep_weights()[step]
    group = stop - first
    parts = []
    for u in range(group):
        for start in starts:
            value = src[first + u, pl.ds(start, rows)]
            high = value.astype(jnp.bfloat16)
            low = (value - high.astype(jnp.float32)).astype(jnp.bfloat16)
            parts.append(jnp.concatenate([high, low], axis=1))
    along = jnp.dot(jnp.concatenate(parts, axis=0), band[...], preferred_element_type=jnp.float32)
    for r in range(0, rows, CHUNK):
        columns = [
            [src[first + d, pl.ds(start + r, CHUNK)] for d in range(-2, group + 2)]
            for start in starts
        ]
        for u in range(group):
            e = first + u

            def total(c):
                x = columns[c]
                side = [src[e, pl.ds(starts[c] + r + d, CHUNK)] for d in (1, -1, 2, -2)]
                near = (x[u + 3] + x[u + 1]) + (side[0] + side[1])
                far = (x[u + 4] + x[u]) + (side[2] + side[3])
                k = (2 * u + c) * rows + r
                return near_weight * near + far_weight * far + along[k : k + CHUNK]

            re, im = columns[0][u + 2], columns[1][u + 2]
            sum_re, sum_im = total(0), total(1)
            part = pl.ds(r, CHUNK)
            k0, k1, kq = (kinv[e, c, part] for c in range(3))
            pair = (
                (1.0 - weight) * re + weight * (x0[e, 0, part] + k0 * sum_re + kq * sum_im),
                (1.0 - weight) * im + weight * (x0[e, 1, part] + k1 * sum_im - kq * sum_re),
            )
            for c, value in enumerate(pair):
                if emit is None:
                    dst[e, pl.ds(starts[c] + r, CHUNK)] = value
                else:
                    emit(e, r, c, value)


def inside_kernel(where, y, yb, inv, kinv, x0, xs, xt, band):
    rows, lanes = inv.shape[2:]
    own = y.shape[0] * y.shape[2] // rows
    core = where[0]
    base = (inv.shape[0] - own) // 2
    write_band(band)
    zero = jnp.zeros((PAD, lanes), jnp.float32)

    def clear(e):
        for x in (xs, xt):
            for r in (0, PAD + rows, 2 * (PAD + rows)):
                x[e, pl.ds(r, PAD)] = zero

    in_groups(inv.shape[0], clear)
    fill(core, y, base, inv, x0, xs)
    fill(core, yb, base + own, inv, x0, xs)
    for step in range(EARLY):
        edge = 2 * (step + 1)
        sweep(step, base + edge, base + 2 * own - edge, x0, kinv, band, (xs, xt))


def sweeps_kernel(where, y_a, yc, yd, inv, kinv, _x0, _xs, _xt, out, x0, xs, xt, band):
    ext, _, rows, _ = inv.shape
    share = y_a.shape[2]
    per_plane = rows // share
    own = y_a.shape[0] // per_plane
    core = where[0]
    base = (ext - own) // 2
    write_band(band)
    fill(core, y_a, base - own, inv, x0, xs)
    fill(core, yc, 0, inv, x0, xs)
    fill(core, yd, base + 2 * own, inv, x0, xs)

    def emit(e, r, c, value):
        i = mirrored(core, e - base, own)
        out[per_plane * i + r // share, c, pl.ds(r % share, CHUNK)] = value.astype(jnp.bfloat16)

    for step in range(SWEEPS):
        edge = 2 * (step + 1)
        if step < EARLY:
            sweep(step, edge, base + edge, x0, kinv, band, (xs, xt))
            sweep(step, base + 2 * own - edge, ext - edge, x0, kinv, band, (xs, xt))
        else:
            last = step == SWEEPS - 1
            sweep(step, edge, ext - edge, x0, kinv, band, (xs, xt), emit if last else None)


def final_kernel(state, correction, out):
    planes, rows, _ = state.shape
    share = correction.shape[2]
    per_plane = rows // share
    half = planes // 2

    for p in range(planes):
        part, inner = p // half, p % half
        value = jnp.concatenate(
            [
                correction[per_plane * inner + h, part].astype(jnp.float32)
                for h in range(per_plane)
            ],
            axis=0,
        )
        out[p] = (state[p].astype(jnp.float32) + value).astype(jnp.bfloat16)


def call(kernel, shapes, inputs, scratch=(), scalars=0, anywhere=0, flops=None, aliases=None):
    outs = [jax.ShapeDtypeStruct(s, d) for s, d in shapes]
    cost = None
    if flops is not None:
        cost = pl.CostEstimate(flops=flops, transcendentals=0, bytes_accessed=flops // 8)
    rest = len(inputs) - scalars - anywhere
    return pl.pallas_call(
        kernel,
        out_shape=outs,
        in_specs=[SMEM] * scalars + [HBM] * anywhere + [VMEM] * rest,
        out_specs=[VMEM] * len(outs),
        scratch_shapes=list(scratch),
        cost_estimate=cost,
        input_output_aliases=aliases or {},
        compiler_params=pltpu.CompilerParams(vmem_limit_bytes=24 << 20),
    )(*inputs)


def iteration(state, initial, forcing, kappa, reaction):
    _, planes, rows, lanes = state.shape
    members = lax.axis_size(TM)
    slots = lax.axis_size(CHIPS)
    slabs = lax.axis_size("space")
    own = planes // 2
    share = own * rows // slots
    per_plane = rows // share
    wide = 2 * SWEEPS
    narrow = wide - own
    ext = own + 2 * wide
    bf16, f32, i32 = jnp.bfloat16, jnp.float32, jnp.int32
    core = lax.axis_index("tm_2")
    slot = lax.axis_index(CHIPS)
    where = jnp.stack([core, slot]).astype(i32)
    u = state[0]

    forward = [(i, i + 1) for i in range(slabs - 1)]
    backward = [(t, s) for s, t in forward]
    outer = []
    for s in range(slabs - 1):
        outer += [(slabs + s, s + 1), (s + 1, slabs + s)]
    swap = [(i, slabs + i) for i in range(slabs)] + [(slabs + i, i) for i in range(slabs)]
    same = forward + [(slabs + s, slabs + t) for s, t in backward]
    odd = lax.axis_index("space") % 2
    even_first = [p for s in range(0, slabs - 1, 2) for p in ((s, s + 1), (s + 1, s))]
    odd_first = [p for s in range(1, slabs - 1, 2) for p in ((s, s + 1), (s + 1, s))]
    low, high = u[:2], u[planes - 2 :]
    even_pair = lax.ppermute(jnp.where(odd == 1, low, high), "space", even_first)
    odd_pair = lax.ppermute(jnp.where(odd == 1, high, low), "space", odd_first)
    before = lax.ppermute(u, TM, [(i, i + 1) for i in range(members - 1)])
    coefs = jnp.stack([kappa, initial, reaction])
    rim = jnp.where(core == 0, coefs[:, :wide], coefs[:, planes - wide :])
    rim = lax.ppermute(rim, CORE_SPACE, outer)
    inner = jnp.where(core == 0, rim[:, wide - narrow :], rim[:, :narrow])
    inner = lax.ppermute(inner, CORE_SPACE, swap)

    block = ((planes, rows, lanes), bf16)
    part, edge = call(
        local_kernel,
        [((planes, rows, lanes), f32), ((4, rows, lanes), f32)],
        [where]
        + [
            pltpu.with_memory_space_constraint(v, pltpu.HBM)
            for v in (u, initial, forcing[0], kappa, reaction)
        ],
        [pltpu.VMEM((planes + 4, rows + 2 * PAD, lanes), f32)]
        + [pltpu.VMEM(*block)] * 5
        + [pltpu.SemaphoreType.DMA((5,))],
        scalars=1,
        anywhere=5,
        flops=20_000_000,
    )
    (residual,) = call(
        residual_kernel,
        [((slots, 2, share, lanes), bf16)],
        [odd.astype(i32).reshape(1), part, edge, even_pair, odd_pair, before],
        scalars=1,
    )
    cells = lax.all_to_all(residual.reshape(members, share, lanes), TM, 0, 0, tiled=True)
    (spectrum,) = call(forward_kernel, [((slots, 2, share, lanes), bf16)], [cells])
    y = lax.all_to_all(spectrum, CHIPS, 0, 0, tiled=True)

    fields = call(
        coefficient_kernel,
        [((ext, 3, rows, lanes), f32)] * 2,
        [where, kappa, initial, reaction, rim, inner],
        scalars=1,
    )
    n = per_plane * narrow
    first = core == 0
    ya = lax.ppermute(y, CORE_SPACE, outer)
    yc = lax.ppermute(jnp.where(first, y[-n:], y[:n]), CORE_SPACE, same)
    yb = lax.ppermute(y, CORE_SPACE, swap)
    yd = lax.ppermute(jnp.where(first, ya[-n:], ya[:n]), CORE_SPACE, swap)
    tall = 2 * rows + 3 * PAD
    buffers = [((ext, 2, rows + PAD, lanes), f32), ((ext, tall, lanes), f32), ((ext, tall, lanes), f32)]
    band = [pltpu.VMEM((2 * lanes, lanes), bf16)]
    state_arrays = call(inside_kernel, buffers, [where, y, yb, *fields], band, scalars=1)
    solved = call(
        sweeps_kernel,
        [((slots, 2, share, lanes), bf16), *buffers],
        [where, ya, yc, yd, *fields, *state_arrays],
        band,
        scalars=1,
        aliases={6: 1, 7: 2, 8: 3},
    )[0]
    modes = lax.all_to_all(solved, CHIPS, 0, 0, tiled=True)
    (correction,) = call(inverse_kernel, [((members, share, lanes), bf16)], [modes])
    returned = lax.all_to_all(correction, TM, 0, 0, tiled=True)
    (updated,) = call(
        final_kernel, [((planes, rows, lanes), bf16)], [u, returned.reshape(slots, 2, share, lanes)]
    )
    return updated[None]


def solution(mesh):
    torus = Mesh(
        mesh.devices.reshape(2, 8, 2, mesh.shape["space"]), ("tm_0", "tm_1", "tm_2", "space")
    )
    in_specs = (
        P(TM, "space", None, None),
        P("space", None, None),
        P(TM, "space", None, None),
        P("space", None, None),
        P("space", None, None),
    )
    out_specs = P(TM, "space", None, None)
    return jax.shard_map(
        iteration, mesh=torus, in_specs=in_specs, out_specs=out_specs, check_vma=False
    )
```

```python
import math

import jax
import jax.numpy as jnp
from jax import lax
from jax.experimental import pallas as pl
from jax.experimental.pallas import tpu as pltpu
from jax.sharding import Mesh
from jax.sharding import PartitionSpec as P

SWEEPS = 6
STEPS = 32
CHUNK = 16
EARLY = 3
TM = ("tm_0", "tm_1", "tm_2")
CHIPS = ("tm_0", "tm_1")
CORE_SPACE = ("tm_2", "space")
SIDE_CORE_SPACE = ("tm_0", "tm_2", "space")

alpha_ratio = 0.25
near_weight = 0.5
far_weight = 1.0
centre_weight = 6.0 * (near_weight + far_weight)
VMEM = pl.BlockSpec(memory_space=pltpu.VMEM)
HBM = pl.BlockSpec(memory_space=pltpu.HBM)
SMEM = pl.BlockSpec(memory_space=pltpu.SMEM)
PAD = 8


def sweep_weights():
    return [
        1.0 / (1.0 + 0.4 * math.cos(math.pi * (2 * k + 1) / (2 * SWEEPS))) for k in range(SWEEPS)
    ]


def in_groups(count, body, group=4):
    def step(i, _):
        for u in range(group):
            body(group * i + u)
        return 0

    lax.fori_loop(0, count // group, step, 0)


def rotated(re, im, c, s):
    if abs(s) < 1e-12:
        return re * c, im * c
    if abs(c) < 1e-12:
        return -im * s, re * s
    return re * c - im * s, re * s + im * c


def real_dft(x):
    n = len(x)
    if n == 2:
        return [(x[0] + x[1], None), (x[0] - x[1], None)]
    even, odd = real_dft(x[0::2]), real_dft(x[1::2])
    half = n // 2
    out = [None] * (half + 1)
    out[0] = (even[0][0] + odd[0][0], None)
    out[half] = (even[0][0] - odd[0][0], None)
    for k in range(1, n // 4):
        angle = -2.0 * math.pi * k / n
        re, im = rotated(odd[k][0], odd[k][1], math.cos(angle), math.sin(angle))
        out[k] = (even[k][0] + re, even[k][1] + im)
        out[half - k] = (even[k][0] - re, im - even[k][1])
    quarter = n // 4
    out[quarter] = (even[quarter][0], -odd[quarter][0])
    return out


def real_inverse(X):
    half = len(X) - 1
    n = 2 * half
    if n == 2:
        return [X[0][0] + X[1][0], X[0][0] - X[1][0]]
    quarter = n // 4
    even, odd = [None] * (quarter + 1), [None] * (quarter + 1)
    even[0] = (X[0][0] + X[half][0], None)
    odd[0] = (X[0][0] - X[half][0], None)
    for k in range(1, quarter):
        a, b = X[k], X[half - k]
        even[k] = (a[0] + b[0], a[1] - b[1])
        angle = 2.0 * math.pi * k / n
        odd[k] = rotated(a[0] - b[0], a[1] + b[1], math.cos(angle), math.sin(angle))
    even[quarter] = (2.0 * X[quarter][0], None)
    odd[quarter] = (-2.0 * X[quarter][1], None)
    out = [None] * n
    out[0::2] = real_inverse(even)
    out[1::2] = real_inverse(odd)
    return out


def lane_masks(shape):
    lane = lax.broadcasted_iota(jnp.int32, shape, len(shape) - 1)
    last = shape[-1] - 1
    return (
        (1, jnp.where(lane >= 1, near_weight, 0.0)),
        (last, jnp.where(lane <= last - 1, near_weight, 0.0)),
        (2, jnp.where(lane >= 2, far_weight, 0.0)),
        (last - 1, jnp.where(lane <= last - 2, far_weight, 0.0)),
    )


def neighbour_sum(ref, lead, plane, rows, masks):
    def at(dp, dr):
        return ref[(*lead, plane + dp, pl.ds(PAD + dr, rows), slice(None))]

    centre = at(0, 0)
    near = (at(1, 0) + at(-1, 0)) + (at(0, 1) + at(0, -1))
    far = (at(2, 0) + at(-2, 0)) + (at(0, 2) + at(0, -2))
    total = near_weight * near + far_weight * far
    for amount, mask in masks:
        total = total + pltpu.roll(centre, amount, 1) * mask
    return centre, total


def local_kernel(where, u_hbm, initial_hbm, forcing_hbm, kappa_hbm, reaction_hbm, part, rim, *rest):
    ext, u, initial, forcing, kappa, reaction, sems = rest
    planes, rows, lanes = u.shape
    pairs = ((u_hbm, u), (forcing_hbm, forcing), (kappa_hbm, kappa), (reaction_hbm, reaction))
    pairs += ((initial_hbm, initial),)
    copies = [pltpu.make_async_copy(src, dst, sems.at[i]) for i, (src, dst) in enumerate(pairs)]
    for copy in copies:
        copy.start()
    zero = jnp.zeros((PAD, lanes), jnp.float32)

    def clear(p):
        ext[p, :PAD] = zero
        ext[p, PAD + rows :] = zero

    in_groups(planes + 4, clear)
    blank = jnp.zeros((rows, lanes), jnp.float32)
    for p in (0, 1, planes + 2, planes + 3):
        ext[p, PAD : PAD + rows] = blank
    copies[0].wait()

    def fill(p):
        ext[p + 2, PAD : PAD + rows] = u[p].astype(jnp.float32)

    in_groups(planes, fill)
    for copy in copies[1:]:
        copy.wait()
    masks = lane_masks((rows, lanes))
    first = where[3] == 0

    def one(p):
        centre, total = neighbour_sum(ext, (), p + 2, rows, masks)
        prior = jnp.where(first, initial[p].astype(jnp.float32), 0.0)
        part[p] = (
            forcing[p].astype(jnp.float32)
            - centre
            + prior
            - kappa[p].astype(jnp.float32) * (centre_weight * centre - total)
            - reaction[p].astype(jnp.float32) * centre * centre * centre
        )

    in_groups(planes, one)
    for i, p in enumerate((0, 1, planes - 2, planes - 1)):
        rim[i] = kappa[p].astype(jnp.float32)


def residual_kernel(odd, part, rim, even_pair, odd_pair, before, out):
    planes, rows, _ = part.shape
    share = out.shape[2]
    per_plane = rows // share
    half = planes // 2

    def put(p, value):
        value = value.astype(jnp.bfloat16)
        side, inner = p // half, p % half
        for piece in range(per_plane):
            out[per_plane * inner + piece, side] = value[piece * share : (piece + 1) * share]

    for p in range(2, planes - 2):
        put(p, part[p] + before[p].astype(jnp.float32))
    upper = odd[0] == 1

    def chosen(a, b, i):
        return jnp.where(upper, a[i].astype(jnp.float32), b[i].astype(jnp.float32))

    l0, l1 = (chosen(even_pair, odd_pair, i) for i in range(2))
    h0, h1 = (chosen(odd_pair, even_pair, i) for i in range(2))
    edges = (
        (0, near_weight * l1 + far_weight * l0),
        (1, far_weight * l1),
        (planes - 2, far_weight * h0),
        (planes - 1, near_weight * h0 + far_weight * h1),
    )
    for i, (p, total) in enumerate(edges):
        put(p, part[p] + rim[i] * total + before[p].astype(jnp.float32))


def slot_place(where, j, slots):
    return jnp.where(where[2] == 0, j, (j + slots // 2) % slots)


def forward_kernel(where, r, out):
    steps, rows, _ = r.shape
    slots = steps // 2
    places = [slot_place(where, j, slots) for j in range(slots)]
    for start in range(0, rows, 16):
        part = pl.ds(start, 16)
        scaled = [
            r[n, part].astype(jnp.float32) * (alpha_ratio ** (n / steps)) for n in range(steps)
        ]
        spectrum = real_dft(scaled)
        out[places[0], 0, part] = spectrum[0][0].astype(jnp.bfloat16)
        out[places[0], 1, part] = spectrum[slots][0].astype(jnp.bfloat16)
        for j in range(1, slots):
            out[places[j], 0, part] = spectrum[j][0].astype(jnp.bfloat16)
            out[places[j], 1, part] = spectrum[j][1].astype(jnp.bfloat16)


def inverse_kernel(where, s, out):
    steps, rows, _ = out.shape
    slots = steps // 2
    places = [slot_place(where, j, slots) for j in range(slots)]
    for start in range(0, rows, 16):
        part = pl.ds(start, 16)

        def given(j, c):
            return s[places[j], c, part].astype(jnp.float32)

        spectrum = [(given(0, 0), None)]
        spectrum += [(given(j, 0), given(j, 1)) for j in range(1, slots)]
        spectrum.append((given(0, 1), None))
        values = real_inverse(spectrum)
        for n in range(steps):
            scale = 1.0 / (alpha_ratio ** (n / steps) * steps)
            out[n, part] = (values[n] * scale).astype(jnp.bfloat16)


def mirrored(core, i, count):
    return jnp.where(core == 0, i, count - 1 - i)


def coefficient_kernel(where, kappa, initial, reaction, outer, inner, inv, kinv):
    planes = kappa.shape[0]
    wide, narrow = outer.shape[1], inner.shape[1]
    core, slot = where[0], where[1]
    members = STEPS
    factor = math.exp(math.log(alpha_ratio) / members)
    s0 = s1 = si = jnp.float32(0.0)
    for j in range(members // 2):
        phase = 2.0 * math.pi * j / members
        real, imag = 1.0 - factor * math.cos(phase), factor * math.sin(phase)
        hit = slot == j
        s0 = jnp.where(hit, jnp.float32(real), s0)
        s1 = jnp.where(hit, jnp.float32(real if j else 1.0 + factor), s1)
        si = jnp.where(hit, jnp.float32(imag if j else 0.0), si)

    def put(e, kv, iv, rv):
        kv, iv, rv = (v.astype(jnp.float32) for v in (kv, iv, rv))
        base = kv * centre_weight + 3.0 * rv * iv * iv
        d0, d1 = s0 + base, s1 + base
        inv0 = 1.0 / (d0 * d0 + si * si)
        inv1 = 1.0 / (d1 * d1 + si * si)
        for c, value in enumerate((d0 * inv0, d1 * inv1, si * inv0)):
            inv[e, c] = value
            kinv[e, c] = kv * value

    def own(i):
        put(wide + mirrored(core, i, planes), kappa[i], initial[i], reaction[i])

    def far(i):
        put(mirrored(core, i, wide), outer[0, i], outer[1, i], outer[2, i])

    def close(i):
        put(wide + planes + mirrored(core, i, narrow), inner[0, i], inner[1, i], inner[2, i])

    in_groups(planes, own, 2)
    in_groups(wide, far, 2)
    in_groups(narrow, close, 2)


def row_starts(rows):
    return (PAD, 2 * PAD + rows)


def write_band(band):
    double, lanes = band.shape
    row = lax.broadcasted_iota(jnp.int32, (double, lanes), 0)
    row = jnp.where(row >= lanes, row - lanes, row)
    gap = jnp.abs(row - lax.broadcasted_iota(jnp.int32, (double, lanes), 1))
    weights = jnp.where(gap == 1, near_weight, jnp.where(gap == 2, far_weight, 0.0))
    band[...] = weights.astype(jnp.bfloat16)


def fill(core, ref, base, inv, x0, x):
    share, rows = ref.shape[2], inv.shape[2]
    per_plane = rows // share
    count = ref.shape[0] // per_plane
    starts = row_starts(rows)

    def body(i):
        e = base + mirrored(core, i, count)
        for h in range(per_plane):
            part = pl.ds(h * share, share)
            re, im = (ref[per_plane * i + h, c].astype(jnp.float32) for c in range(2))
            i0, i1, iq = (inv[e, c, part] for c in range(3))
            for c, value in enumerate((re * i0 + im * iq, im * i1 - re * iq)):
                x0[e, c, part] = value
                x[e, pl.ds(starts[c] + h * share, share)] = value

    in_groups(count, body)


def sweep(step, first, stop, x0, kinv, band, buffers, emit=None):
    rows = kinv.shape[2]
    starts = row_starts(rows)
    src, dst = buffers[step % 2], buffers[(step + 1) % 2]
    weight = sweep_weights()[step]
    group = stop - first
    parts = []
    for u in range(group):
        for start in starts:
            value = src[first + u, pl.ds(start, rows)]
            high = value.astype(jnp.bfloat16)
            low = (value - high.astype(jnp.float32)).astype(jnp.bfloat16)
            parts.append(jnp.concatenate([high, low], axis=1))
    along = jnp.dot(jnp.concatenate(parts, axis=0), band[...], preferred_element_type=jnp.float32)
    for r in range(0, rows, CHUNK):
        columns = [
            [src[first + d, pl.ds(start + r, CHUNK)] for d in range(-2, group + 2)]
            for start in starts
        ]
        for u in range(group):
            e = first + u

            def total(c):
                x = columns[c]
                side = [src[e, pl.ds(starts[c] + r + d, CHUNK)] for d in (1, -1, 2, -2)]
                near = (x[u + 3] + x[u + 1]) + (side[0] + side[1])
                far = (x[u + 4] + x[u]) + (side[2] + side[3])
                k = (2 * u + c) * rows + r
                return near_weight * near + far_weight * far + along[k : k + CHUNK]

            re, im = columns[0][u + 2], columns[1][u + 2]
            sum_re, sum_im = total(0), total(1)
            part = pl.ds(r, CHUNK)
            k0, k1, kq = (kinv[e, c, part] for c in range(3))
            pair = (
                (1.0 - weight) * re + weight * (x0[e, 0, part] + k0 * sum_re + kq * sum_im),
                (1.0 - weight) * im + weight * (x0[e, 1, part] + k1 * sum_im - kq * sum_re),
            )
            for c, value in enumerate(pair):
                if emit is None:
                    dst[e, pl.ds(starts[c] + r, CHUNK)] = value
                else:
                    emit(e, r, c, value)


def inside_kernel(where, y, yb, inv, kinv, x0, xs, xt, band):
    rows, lanes = inv.shape[2:]
    own = y.shape[0] * y.shape[2] // rows
    core = where[0]
    base = (inv.shape[0] - own) // 2
    write_band(band)
    zero = jnp.zeros((PAD, lanes), jnp.float32)

    def clear(e):
        for x in (xs, xt):
            for r in (0, PAD + rows, 2 * (PAD + rows)):
                x[e, pl.ds(r, PAD)] = zero

    in_groups(inv.shape[0], clear)
    fill(core, y, base, inv, x0, xs)
    fill(core, yb, base + own, inv, x0, xs)
    for step in range(EARLY):
        edge = 2 * (step + 1)
        sweep(step, base + edge, base + 2 * own - edge, x0, kinv, band, (xs, xt))


def sweeps_kernel(where, y_a, yc, yd, inv, kinv, _x0, _xs, _xt, out, x0, xs, xt, band):
    ext, _, rows, _ = inv.shape
    share = y_a.shape[2]
    per_plane = rows // share
    own = y_a.shape[0] // per_plane
    core = where[0]
    base = (ext - own) // 2
    write_band(band)
    fill(core, y_a, base - own, inv, x0, xs)
    fill(core, yc, 0, inv, x0, xs)
    fill(core, yd, base + 2 * own, inv, x0, xs)

    def emit(e, r, c, value):
        i = mirrored(core, e - base, own)
        out[per_plane * i + r // share, c, pl.ds(r % share, CHUNK)] = value.astype(jnp.bfloat16)

    for step in range(SWEEPS):
        edge = 2 * (step + 1)
        if step < EARLY:
            sweep(step, edge, base + edge, x0, kinv, band, (xs, xt))
            sweep(step, base + 2 * own - edge, ext - edge, x0, kinv, band, (xs, xt))
        else:
            last = step == SWEEPS - 1
            sweep(step, edge, ext - edge, x0, kinv, band, (xs, xt), emit if last else None)


def final_kernel(state, correction, out):
    planes, rows, _ = state.shape
    share = correction.shape[2]
    per_plane = rows // share
    half = planes // 2

    for p in range(planes):
        part, inner = p // half, p % half
        value = jnp.concatenate(
            [
                correction[per_plane * inner + h, part].astype(jnp.float32)
                for h in range(per_plane)
            ],
            axis=0,
        )
        out[p] = (state[p].astype(jnp.float32) + value).astype(jnp.bfloat16)


def call(kernel, shapes, inputs, scratch=(), scalars=0, anywhere=0, flops=None, aliases=None):
    outs = [jax.ShapeDtypeStruct(s, d) for s, d in shapes]
    cost = None
    if flops is not None:
        cost = pl.CostEstimate(flops=flops, transcendentals=0, bytes_accessed=flops // 8)
    rest = len(inputs) - scalars - anywhere
    return pl.pallas_call(
        kernel,
        out_shape=outs,
        in_specs=[SMEM] * scalars + [HBM] * anywhere + [VMEM] * rest,
        out_specs=[VMEM] * len(outs),
        scratch_shapes=list(scratch),
        cost_estimate=cost,
        input_output_aliases=aliases or {},
        compiler_params=pltpu.CompilerParams(vmem_limit_bytes=24 << 20),
    )(*inputs)


def iteration(state, initial, forcing, kappa, reaction):
    _, planes, rows, lanes = state.shape
    members = lax.axis_size(TM)
    slots = lax.axis_size(CHIPS)
    slabs = lax.axis_size("space")
    own = planes // 2
    share = own * rows // slots
    per_plane = rows // share
    wide = 2 * SWEEPS
    narrow = wide - own
    ext = own + 2 * wide
    bf16, f32, i32 = jnp.bfloat16, jnp.float32, jnp.int32
    core = lax.axis_index("tm_2")
    flip = lax.axis_index("space") // 2 % 2
    half_slots = slots // 2
    slot = lax.axis_index(CHIPS)
    slot = jnp.where(flip == 0, slot, (slot + half_slots) % slots)
    where = jnp.stack([core, slot, flip, lax.axis_index(TM)]).astype(i32)
    u = state[0]

    outer, same = [], []
    for side in range(2):
        for t in range(slabs - 1):
            near, beside = side * 2 * slabs, (side ^ (t % 2)) * 2 * slabs
            low, high = near + slabs + t, beside + t + 1
            outer += [(low, high), (high, low)]
            same += [(near + t, beside + t + 1), (beside + slabs + t + 1, near + slabs + t)]
    swap = [(i, slabs + i) for i in range(slabs)] + [(slabs + i, i) for i in range(slabs)]
    odd = lax.axis_index("space") % 2
    even_first = [p for s in range(0, slabs - 1, 2) for p in ((s, s + 1), (s + 1, s))]
    odd_first = [p for s in range(1, slabs - 1, 2) for p in ((s, s + 1), (s + 1, s))]
    low, high = u[:2], u[planes - 2 :]
    even_pair = lax.ppermute(jnp.where(odd == 1, low, high), "space", even_first)
    odd_pair = lax.ppermute(jnp.where(odd == 1, high, low), "space", odd_first)
    before = lax.ppermute(u, TM, [(i, i + 1) for i in range(members - 1)])
    coefs = jnp.stack([kappa, initial, reaction])
    rim = jnp.where(core == 0, coefs[:, :wide], coefs[:, planes - wide :])
    rim = lax.ppermute(rim, SIDE_CORE_SPACE, outer)
    inner = jnp.where(core == 0, rim[:, wide - narrow :], rim[:, :narrow])
    inner = lax.ppermute(inner, CORE_SPACE, swap)

    block = ((planes, rows, lanes), bf16)
    part, edge = call(
        local_kernel,
        [((planes, rows, lanes), f32), ((4, rows, lanes), f32)],
        [where]
        + [
            pltpu.with_memory_space_constraint(v, pltpu.HBM)
            for v in (u, initial, forcing[0], kappa, reaction)
        ],
        [pltpu.VMEM((planes + 4, rows + 2 * PAD, lanes), f32)]
        + [pltpu.VMEM(*block)] * 5
        + [pltpu.SemaphoreType.DMA((5,))],
        scalars=1,
        anywhere=5,
        flops=20_000_000,
    )
    (residual,) = call(
        residual_kernel,
        [((slots, 2, share, lanes), bf16)],
        [odd.astype(i32).reshape(1), part, edge, even_pair, odd_pair, before],
        scalars=1,
    )
    cells = lax.all_to_all(residual.reshape(members, share, lanes), TM, 0, 0, tiled=True)
    (spectrum,) = call(
        forward_kernel, [((slots, 2, share, lanes), bf16)], [where, cells], scalars=1
    )
    y = lax.all_to_all(spectrum, CHIPS, 0, 0, tiled=True)

    fields = call(
        coefficient_kernel,
        [((ext, 3, rows, lanes), f32)] * 2,
        [where, kappa, initial, reaction, rim, inner],
        scalars=1,
    )
    n = per_plane * narrow
    first = core == 0
    ya = lax.ppermute(y, SIDE_CORE_SPACE, outer)
    yc = lax.ppermute(jnp.where(first, y[-n:], y[:n]), SIDE_CORE_SPACE, same)
    yb = lax.ppermute(y, CORE_SPACE, swap)
    yd = lax.ppermute(jnp.where(first, ya[-n:], ya[:n]), CORE_SPACE, swap)
    tall = 2 * rows + 3 * PAD
    buffers = [((ext, 2, rows + PAD, lanes), f32), ((ext, tall, lanes), f32), ((ext, tall, lanes), f32)]
    band = [pltpu.VMEM((2 * lanes, lanes), bf16)]
    state_arrays = call(inside_kernel, buffers, [where, y, yb, *fields], band, scalars=1)
    solved = call(
        sweeps_kernel,
        [((slots, 2, share, lanes), bf16), *buffers],
        [where, ya, yc, yd, *fields, *state_arrays],
        band,
        scalars=1,
        aliases={6: 1, 7: 2, 8: 3},
    )[0]
    modes = lax.all_to_all(solved, CHIPS, 0, 0, tiled=True)
    (correction,) = call(
        inverse_kernel, [((members, share, lanes), bf16)], [where, modes], scalars=1
    )
    returned = lax.all_to_all(correction, TM, 0, 0, tiled=True)
    (updated,) = call(
        final_kernel, [((planes, rows, lanes), bf16)], [u, returned.reshape(slots, 2, share, lanes)]
    )
    return updated[None]


def solution(mesh):
    torus = Mesh(
        mesh.devices.reshape(2, 8, 2, mesh.shape["space"]), ("tm_0", "tm_1", "tm_2", "space")
    )
    in_specs = (
        P(TM, "space", None, None),
        P("space", None, None),
        P(TM, "space", None, None),
        P("space", None, None),
        P("space", None, None),
    )
    out_specs = P(TM, "space", None, None)
    return jax.shard_map(
        iteration, mesh=torus, in_specs=in_specs, out_specs=out_specs, check_vma=False
    )
```

```python
import math

import jax
import jax.numpy as jnp
from jax import lax
from jax.experimental import pallas as pl
from jax.experimental.pallas import tpu as pltpu
from jax.sharding import Mesh
from jax.sharding import PartitionSpec as P

SWEEPS = 6
STEPS = 32
CHUNK = 16
EARLY = 1
TM = ("tm_0", "tm_1", "tm_2")
CHIPS = ("tm_0", "tm_1")
CORE_SPACE = ("tm_2", "space")
SIDE_CORE_SPACE = ("tm_0", "tm_2", "space")

alpha_ratio = 0.25
near_weight = 0.5
far_weight = 1.0
centre_weight = 6.0 * (near_weight + far_weight)
VMEM = pl.BlockSpec(memory_space=pltpu.VMEM)
HBM = pl.BlockSpec(memory_space=pltpu.HBM)
SMEM = pl.BlockSpec(memory_space=pltpu.SMEM)
PAD = 8


def sweep_weights():
    return [
        1.0 / (1.0 + 0.4 * math.cos(math.pi * (2 * k + 1) / (2 * SWEEPS))) for k in range(SWEEPS)
    ]


def in_groups(count, body, group=4):
    def step(i, _):
        for u in range(group):
            body(group * i + u)
        return 0

    lax.fori_loop(0, count // group, step, 0)


def rotated(re, im, c, s):
    if abs(s) < 1e-12:
        return re * c, im * c
    if abs(c) < 1e-12:
        return -im * s, re * s
    return re * c - im * s, re * s + im * c


def real_dft(x):
    n = len(x)
    if n == 2:
        return [(x[0] + x[1], None), (x[0] - x[1], None)]
    even, odd = real_dft(x[0::2]), real_dft(x[1::2])
    half = n // 2
    out = [None] * (half + 1)
    out[0] = (even[0][0] + odd[0][0], None)
    out[half] = (even[0][0] - odd[0][0], None)
    for k in range(1, n // 4):
        angle = -2.0 * math.pi * k / n
        re, im = rotated(odd[k][0], odd[k][1], math.cos(angle), math.sin(angle))
        out[k] = (even[k][0] + re, even[k][1] + im)
        out[half - k] = (even[k][0] - re, im - even[k][1])
    quarter = n // 4
    out[quarter] = (even[quarter][0], -odd[quarter][0])
    return out


def real_inverse(X):
    half = len(X) - 1
    n = 2 * half
    if n == 2:
        return [X[0][0] + X[1][0], X[0][0] - X[1][0]]
    quarter = n // 4
    even, odd = [None] * (quarter + 1), [None] * (quarter + 1)
    even[0] = (X[0][0] + X[half][0], None)
    odd[0] = (X[0][0] - X[half][0], None)
    for k in range(1, quarter):
        a, b = X[k], X[half - k]
        even[k] = (a[0] + b[0], a[1] - b[1])
        angle = 2.0 * math.pi * k / n
        odd[k] = rotated(a[0] - b[0], a[1] + b[1], math.cos(angle), math.sin(angle))
    even[quarter] = (2.0 * X[quarter][0], None)
    odd[quarter] = (-2.0 * X[quarter][1], None)
    out = [None] * n
    out[0::2] = real_inverse(even)
    out[1::2] = real_inverse(odd)
    return out


def lane_masks(shape):
    lane = lax.broadcasted_iota(jnp.int32, shape, len(shape) - 1)
    last = shape[-1] - 1
    return (
        (1, jnp.where(lane >= 1, near_weight, 0.0)),
        (last, jnp.where(lane <= last - 1, near_weight, 0.0)),
        (2, jnp.where(lane >= 2, far_weight, 0.0)),
        (last - 1, jnp.where(lane <= last - 2, far_weight, 0.0)),
    )


def neighbour_sum(ref, lead, plane, rows, masks):
    def at(dp, dr):
        return ref[(*lead, plane + dp, pl.ds(PAD + dr, rows), slice(None))]

    centre = at(0, 0)
    near = (at(1, 0) + at(-1, 0)) + (at(0, 1) + at(0, -1))
    far = (at(2, 0) + at(-2, 0)) + (at(0, 2) + at(0, -2))
    total = near_weight * near + far_weight * far
    for amount, mask in masks:
        total = total + pltpu.roll(centre, amount, 1) * mask
    return centre, total


def local_kernel(where, u_hbm, initial_hbm, forcing_hbm, kappa_hbm, reaction_hbm, part, rim, *rest):
    ext, u, initial, forcing, kappa, reaction, sems = rest
    planes, rows, lanes = u.shape
    pairs = ((u_hbm, u), (forcing_hbm, forcing), (kappa_hbm, kappa), (reaction_hbm, reaction))
    pairs += ((initial_hbm, initial),)
    copies = [pltpu.make_async_copy(src, dst, sems.at[i]) for i, (src, dst) in enumerate(pairs)]
    for copy in copies:
        copy.start()
    zero = jnp.zeros((PAD, lanes), jnp.float32)

    def clear(p):
        ext[p, :PAD] = zero
        ext[p, PAD + rows :] = zero

    in_groups(planes + 4, clear)
    blank = jnp.zeros((rows, lanes), jnp.float32)
    for p in (0, 1, planes + 2, planes + 3):
        ext[p, PAD : PAD + rows] = blank
    copies[0].wait()

    def fill(p):
        ext[p + 2, PAD : PAD + rows] = u[p].astype(jnp.float32)

    in_groups(planes, fill)
    for copy in copies[1:]:
        copy.wait()
    masks = lane_masks((rows, lanes))
    first = where[3] == 0

    def one(p):
        centre, total = neighbour_sum(ext, (), p + 2, rows, masks)
        prior = jnp.where(first, initial[p].astype(jnp.float32), 0.0)
        part[p] = (
            forcing[p].astype(jnp.float32)
            - centre
            + prior
            - kappa[p].astype(jnp.float32) * (centre_weight * centre - total)
            - reaction[p].astype(jnp.float32) * centre * centre * centre
        )

    in_groups(planes, one)
    for i, p in enumerate((0, 1, planes - 2, planes - 1)):
        rim[i] = kappa[p].astype(jnp.float32)


def residual_kernel(odd, part, rim, even_pair, odd_pair, before, out):
    planes, rows, _ = part.shape
    share = out.shape[2]
    per_plane = rows // share
    half = planes // 2

    def put(p, value):
        value = value.astype(jnp.bfloat16)
        side, inner = p // half, p % half
        for piece in range(per_plane):
            out[per_plane * inner + piece, side] = value[piece * share : (piece + 1) * share]

    for p in range(2, planes - 2):
        put(p, part[p] + before[p].astype(jnp.float32))
    upper = odd[0] == 1

    def chosen(a, b, i):
        return jnp.where(upper, a[i].astype(jnp.float32), b[i].astype(jnp.float32))

    l0, l1 = (chosen(even_pair, odd_pair, i) for i in range(2))
    h0, h1 = (chosen(odd_pair, even_pair, i) for i in range(2))
    edges = (
        (0, near_weight * l1 + far_weight * l0),
        (1, far_weight * l1),
        (planes - 2, far_weight * h0),
        (planes - 1, near_weight * h0 + far_weight * h1),
    )
    for i, (p, total) in enumerate(edges):
        put(p, part[p] + rim[i] * total + before[p].astype(jnp.float32))


def either_order(where, body, slots):
    @pl.when(where[2] == 0)
    def _():
        body(list(range(slots)))

    @pl.when(where[2] != 0)
    def _():
        body([(j + slots // 2) % slots for j in range(slots)])


def forward_kernel(where, r, out):
    steps, rows, _ = r.shape
    slots = steps // 2

    def body(places):
        for start in range(0, rows, 16):
            part = pl.ds(start, 16)
            scaled = [
                r[n, part].astype(jnp.float32) * (alpha_ratio ** (n / steps)) for n in range(steps)
            ]
            spectrum = real_dft(scaled)
            out[places[0], 0, part] = spectrum[0][0].astype(jnp.bfloat16)
            out[places[0], 1, part] = spectrum[slots][0].astype(jnp.bfloat16)
            for j in range(1, slots):
                out[places[j], 0, part] = spectrum[j][0].astype(jnp.bfloat16)
                out[places[j], 1, part] = spectrum[j][1].astype(jnp.bfloat16)

    either_order(where, body, slots)


def inverse_kernel(where, s, out):
    steps, rows, _ = out.shape
    slots = steps // 2

    def body(places):
        for start in range(0, rows, 16):
            part = pl.ds(start, 16)

            def given(j, c):
                return s[places[j], c, part].astype(jnp.float32)

            spectrum = [(given(0, 0), None)]
            spectrum += [(given(j, 0), given(j, 1)) for j in range(1, slots)]
            spectrum.append((given(0, 1), None))
            values = real_inverse(spectrum)
            for n in range(steps):
                scale = 1.0 / (alpha_ratio ** (n / steps) * steps)
                out[n, part] = (values[n] * scale).astype(jnp.bfloat16)

    either_order(where, body, slots)


def mirrored(core, i, count):
    return jnp.where(core == 0, i, count - 1 - i)


def coefficient_kernel(where, kappa, initial, reaction, outer, inner, inv, kinv):
    planes = kappa.shape[0]
    wide, narrow = outer.shape[1], inner.shape[1]
    core, slot = where[0], where[1]
    members = STEPS
    factor = math.exp(math.log(alpha_ratio) / members)
    s0 = s1 = si = jnp.float32(0.0)
    for j in range(members // 2):
        phase = 2.0 * math.pi * j / members
        real, imag = 1.0 - factor * math.cos(phase), factor * math.sin(phase)
        hit = slot == j
        s0 = jnp.where(hit, jnp.float32(real), s0)
        s1 = jnp.where(hit, jnp.float32(real if j else 1.0 + factor), s1)
        si = jnp.where(hit, jnp.float32(imag if j else 0.0), si)

    def put(e, kv, iv, rv):
        kv, iv, rv = (v.astype(jnp.float32) for v in (kv, iv, rv))
        base = kv * centre_weight + 3.0 * rv * iv * iv
        d0, d1 = s0 + base, s1 + base
        m0, m1 = d0 * d0 + si * si, d1 * d1 + si * si
        both = 1.0 / (m0 * m1)
        inv0, inv1 = m1 * both, m0 * both
        for c, value in enumerate((d0 * inv0, d1 * inv1, si * inv0)):
            inv[e, c] = value
            kinv[e, c] = kv * value

    def own(i):
        put(wide + mirrored(core, i, planes), kappa[i], initial[i], reaction[i])

    def far(i):
        put(mirrored(core, i, wide), outer[0, i], outer[1, i], outer[2, i])

    def close(i):
        put(wide + planes + mirrored(core, i, narrow), inner[0, i], inner[1, i], inner[2, i])

    in_groups(planes, own)
    in_groups(wide, far)
    in_groups(narrow, close)


def row_starts(rows):
    return (PAD, 2 * PAD + rows)


def write_band(band):
    double, lanes = band.shape
    row = lax.broadcasted_iota(jnp.int32, (double, lanes), 0)
    row = jnp.where(row >= lanes, row - lanes, row)
    gap = jnp.abs(row - lax.broadcasted_iota(jnp.int32, (double, lanes), 1))
    weights = jnp.where(gap == 1, near_weight, jnp.where(gap == 2, far_weight, 0.0))
    band[...] = weights.astype(jnp.bfloat16)


def fill(core, ref, base, inv, x0, x):
    share, rows = ref.shape[2], inv.shape[2]
    per_plane = rows // share
    count = ref.shape[0] // per_plane
    starts = row_starts(rows)

    def body(i):
        e = base + mirrored(core, i, count)
        for h in range(per_plane):
            part = pl.ds(h * share, share)
            re, im = (ref[per_plane * i + h, c].astype(jnp.float32) for c in range(2))
            i0, i1, iq = (inv[e, c, part] for c in range(3))
            for c, value in enumerate((re * i0 + im * iq, im * i1 - re * iq)):
                x0[e, c, part] = value
                x[e, pl.ds(starts[c] + h * share, share)] = value

    in_groups(count, body)


def sweep(step, first, stop, x0, kinv, band, buffers, emit=None):
    rows = kinv.shape[2]
    starts = row_starts(rows)
    src, dst = buffers[step % 2], buffers[(step + 1) % 2]
    weight = sweep_weights()[step]
    group = stop - first
    parts = []
    for u in range(group):
        for start in starts:
            value = src[first + u, pl.ds(start, rows)]
            high = value.astype(jnp.bfloat16)
            low = (value - high.astype(jnp.float32)).astype(jnp.bfloat16)
            parts.append(jnp.concatenate([high, low], axis=1))
    along = jnp.dot(jnp.concatenate(parts, axis=0), band[...], preferred_element_type=jnp.float32)
    for r in range(0, rows, CHUNK):
        columns = [
            [src[first + d, pl.ds(start + r, CHUNK)] for d in range(-2, group + 2)]
            for start in starts
        ]
        for u in range(group):
            e = first + u

            def total(c):
                x = columns[c]
                side = [src[e, pl.ds(starts[c] + r + d, CHUNK)] for d in (1, -1, 2, -2)]
                near = (x[u + 3] + x[u + 1]) + (side[0] + side[1])
                far = (x[u + 4] + x[u]) + (side[2] + side[3])
                k = (2 * u + c) * rows + r
                return near_weight * near + far_weight * far + along[k : k + CHUNK]

            re, im = columns[0][u + 2], columns[1][u + 2]
            sum_re, sum_im = total(0), total(1)
            part = pl.ds(r, CHUNK)
            k0, k1, kq = (kinv[e, c, part] for c in range(3))
            pair = (
                (1.0 - weight) * re + weight * (x0[e, 0, part] + k0 * sum_re + kq * sum_im),
                (1.0 - weight) * im + weight * (x0[e, 1, part] + k1 * sum_im - kq * sum_re),
            )
            for c, value in enumerate(pair):
                if emit is None:
                    dst[e, pl.ds(starts[c] + r, CHUNK)] = value
                else:
                    emit(e, r, c, value)


def inside_kernel(where, y, yb, inv, kinv, x0, xs, xt, band):
    rows, lanes = inv.shape[2:]
    own = y.shape[0] * y.shape[2] // rows
    core = where[0]
    base = (inv.shape[0] - own) // 2
    write_band(band)
    zero = jnp.zeros((PAD, lanes), jnp.float32)

    def clear(e):
        for x in (xs, xt):
            for r in (0, PAD + rows, 2 * (PAD + rows)):
                x[e, pl.ds(r, PAD)] = zero

    in_groups(inv.shape[0], clear)
    fill(core, y, base, inv, x0, xs)
    fill(core, yb, base + own, inv, x0, xs)
    for step in range(EARLY):
        edge = 2 * (step + 1)
        sweep(step, base + edge, base + 2 * own - edge, x0, kinv, band, (xs, xt))


def sweeps_kernel(where, y_a, yc, yd, inv, kinv, _x0, _xs, _xt, out, x0, xs, xt, band):
    ext, _, rows, _ = inv.shape
    share = y_a.shape[2]
    per_plane = rows // share
    own = y_a.shape[0] // per_plane
    core = where[0]
    base = (ext - own) // 2
    write_band(band)
    fill(core, y_a, base - own, inv, x0, xs)
    fill(core, yc, 0, inv, x0, xs)
    fill(core, yd, base + 2 * own, inv, x0, xs)

    def emit(e, r, c, value):
        i = mirrored(core, e - base, own)
        out[per_plane * i + r // share, c, pl.ds(r % share, CHUNK)] = value.astype(jnp.bfloat16)

    for step in range(SWEEPS):
        edge = 2 * (step + 1)
        if step < EARLY:
            sweep(step, edge, base + edge, x0, kinv, band, (xs, xt))
            sweep(step, base + 2 * own - edge, ext - edge, x0, kinv, band, (xs, xt))
        else:
            last = step == SWEEPS - 1
            sweep(step, edge, ext - edge, x0, kinv, band, (xs, xt), emit if last else None)


def final_kernel(state, correction, out):
    planes, rows, _ = state.shape
    share = correction.shape[2]
    per_plane = rows // share
    half = planes // 2

    for p in range(planes):
        part, inner = p // half, p % half
        value = jnp.concatenate(
            [
                correction[per_plane * inner + h, part].astype(jnp.float32)
                for h in range(per_plane)
            ],
            axis=0,
        )
        out[p] = (state[p].astype(jnp.float32) + value).astype(jnp.bfloat16)


def call(kernel, shapes, inputs, scratch=(), scalars=0, anywhere=0, flops=None, aliases=None):
    outs = [jax.ShapeDtypeStruct(s, d) for s, d in shapes]
    cost = None
    if flops is not None:
        cost = pl.CostEstimate(flops=flops, transcendentals=0, bytes_accessed=flops // 8)
    rest = len(inputs) - scalars - anywhere
    return pl.pallas_call(
        kernel,
        out_shape=outs,
        in_specs=[SMEM] * scalars + [HBM] * anywhere + [VMEM] * rest,
        out_specs=[VMEM] * len(outs),
        scratch_shapes=list(scratch),
        cost_estimate=cost,
        input_output_aliases=aliases or {},
        compiler_params=pltpu.CompilerParams(vmem_limit_bytes=24 << 20),
    )(*inputs)


def iteration(state, initial, forcing, kappa, reaction):
    _, planes, rows, lanes = state.shape
    members = lax.axis_size(TM)
    slots = lax.axis_size(CHIPS)
    slabs = lax.axis_size("space")
    own = planes // 2
    share = own * rows // slots
    per_plane = rows // share
    wide = 2 * SWEEPS
    narrow = wide - own
    ext = own + 2 * wide
    bf16, f32, i32 = jnp.bfloat16, jnp.float32, jnp.int32
    core = lax.axis_index("tm_2")
    flip = lax.axis_index("space") // 2 % 2
    half_slots = slots // 2
    slot = lax.axis_index(CHIPS)
    slot = jnp.where(flip == 0, slot, (slot + half_slots) % slots)
    where = jnp.stack([core, slot, flip, lax.axis_index(TM)]).astype(i32)
    u = state[0]

    outer, same = [], []
    for side in range(2):
        for t in range(slabs - 1):
            near, beside = side * 2 * slabs, (side ^ (t % 2)) * 2 * slabs
            low, high = near + slabs + t, beside + t + 1
            outer += [(low, high), (high, low)]
            same += [(near + t, beside + t + 1), (beside + slabs + t + 1, near + slabs + t)]
    swap = [(i, slabs + i) for i in range(slabs)] + [(slabs + i, i) for i in range(slabs)]
    odd = lax.axis_index("space") % 2
    even_first = [p for s in range(0, slabs - 1, 2) for p in ((s, s + 1), (s + 1, s))]
    odd_first = [p for s in range(1, slabs - 1, 2) for p in ((s, s + 1), (s + 1, s))]
    low, high = u[:2], u[planes - 2 :]
    even_pair = lax.ppermute(jnp.where(odd == 1, low, high), "space", even_first)
    odd_pair = lax.ppermute(jnp.where(odd == 1, high, low), "space", odd_first)
    before = lax.ppermute(u, TM, [(i, i + 1) for i in range(members - 1)])
    coefs = jnp.stack([kappa, initial, reaction])
    rim = jnp.where(core == 0, coefs[:, :wide], coefs[:, planes - wide :])
    rim = lax.ppermute(rim, SIDE_CORE_SPACE, outer)
    inner = jnp.where(core == 0, rim[:, wide - narrow :], rim[:, :narrow])
    inner = lax.ppermute(inner, CORE_SPACE, swap)

    block = ((planes, rows, lanes), bf16)
    part, edge = call(
        local_kernel,
        [((planes, rows, lanes), f32), ((4, rows, lanes), f32)],
        [where]
        + [
            pltpu.with_memory_space_constraint(v, pltpu.HBM)
            for v in (u, initial, forcing[0], kappa, reaction)
        ],
        [pltpu.VMEM((planes + 4, rows + 2 * PAD, lanes), f32)]
        + [pltpu.VMEM(*block)] * 5
        + [pltpu.SemaphoreType.DMA((5,))],
        scalars=1,
        anywhere=5,
        flops=20_000_000,
    )
    (residual,) = call(
        residual_kernel,
        [((slots, 2, share, lanes), bf16)],
        [odd.astype(i32).reshape(1), part, edge, even_pair, odd_pair, before],
        scalars=1,
    )
    cells = lax.all_to_all(residual.reshape(members, share, lanes), TM, 0, 0, tiled=True)
    (spectrum,) = call(
        forward_kernel, [((slots, 2, share, lanes), bf16)], [where, cells], scalars=1
    )
    y = lax.all_to_all(spectrum, CHIPS, 0, 0, tiled=True)

    fields = call(
        coefficient_kernel,
        [((ext, 3, rows, lanes), f32)] * 2,
        [where, kappa, initial, reaction, rim, inner],
        scalars=1,
    )
    n = per_plane * narrow
    first = core == 0
    ya = lax.ppermute(y, SIDE_CORE_SPACE, outer)
    yc = lax.ppermute(jnp.where(first, y[-n:], y[:n]), SIDE_CORE_SPACE, same)
    yb = lax.ppermute(y, CORE_SPACE, swap)
    yd = lax.ppermute(jnp.where(first, ya[-n:], ya[:n]), CORE_SPACE, swap)
    tall = 2 * rows + 3 * PAD
    buffers = [((ext, 2, rows + PAD, lanes), f32), ((ext, tall, lanes), f32), ((ext, tall, lanes), f32)]
    band = [pltpu.VMEM((2 * lanes, lanes), bf16)]
    state_arrays = call(inside_kernel, buffers, [where, y, yb, *fields], band, scalars=1)
    solved = call(
        sweeps_kernel,
        [((slots, 2, share, lanes), bf16), *buffers],
        [where, ya, yc, yd, *fields, *state_arrays],
        band,
        scalars=1,
        aliases={6: 1, 7: 2, 8: 3},
    )[0]
    modes = lax.all_to_all(solved, CHIPS, 0, 0, tiled=True)
    (correction,) = call(
        inverse_kernel, [((members, share, lanes), bf16)], [where, modes], scalars=1
    )
    returned = lax.all_to_all(correction, TM, 0, 0, tiled=True)
    (updated,) = call(
        final_kernel, [((planes, rows, lanes), bf16)], [u, returned.reshape(slots, 2, share, lanes)]
    )
    return updated[None]


def solution(mesh):
    torus = Mesh(
        mesh.devices.reshape(2, 8, 2, mesh.shape["space"]), ("tm_0", "tm_1", "tm_2", "space")
    )
    in_specs = (
        P(TM, "space", None, None),
        P("space", None, None),
        P(TM, "space", None, None),
        P("space", None, None),
        P("space", None, None),
    )
    out_specs = P(TM, "space", None, None)
    return jax.shard_map(
        iteration, mesh=torus, in_specs=in_specs, out_specs=out_specs, check_vma=False
    )
```

```python
import math

import jax
import jax.numpy as jnp
from jax import lax
from jax.experimental import pallas as pl
from jax.experimental.pallas import tpu as pltpu
from jax.sharding import Mesh
from jax.sharding import PartitionSpec as P

SWEEPS = 6
STEPS = 32
CHUNK = 16
EARLY = 1
TM = ("tm_0", "tm_1", "tm_2")
CHIPS = ("tm_0", "tm_1")
CORE_SPACE = ("tm_2", "space")
SIDE_CORE_SPACE = ("tm_0", "tm_2", "space")

alpha_ratio = 0.25
near_weight = 0.5
far_weight = 1.0
centre_weight = 6.0 * (near_weight + far_weight)
VMEM = pl.BlockSpec(memory_space=pltpu.VMEM)
HBM = pl.BlockSpec(memory_space=pltpu.HBM)
PAD = 8


def sweep_weights():
    return [
        1.0 / (1.0 + 0.4 * math.cos(math.pi * (2 * k + 1) / (2 * SWEEPS))) for k in range(SWEEPS)
    ]


def in_groups(count, body, group=4):
    def step(i, _):
        for u in range(group):
            body(group * i + u)
        return 0

    lax.fori_loop(0, count // group, step, 0)


def rotated(re, im, c, s):
    if abs(s) < 1e-12:
        return re * c, im * c
    if abs(c) < 1e-12:
        return -im * s, re * s
    return re * c - im * s, re * s + im * c


def real_dft(x):
    n = len(x)
    if n == 2:
        return [(x[0] + x[1], None), (x[0] - x[1], None)]
    even, odd = real_dft(x[0::2]), real_dft(x[1::2])
    half = n // 2
    out = [None] * (half + 1)
    out[0] = (even[0][0] + odd[0][0], None)
    out[half] = (even[0][0] - odd[0][0], None)
    for k in range(1, n // 4):
        angle = -2.0 * math.pi * k / n
        re, im = rotated(odd[k][0], odd[k][1], math.cos(angle), math.sin(angle))
        out[k] = (even[k][0] + re, even[k][1] + im)
        out[half - k] = (even[k][0] - re, im - even[k][1])
    quarter = n // 4
    out[quarter] = (even[quarter][0], -odd[quarter][0])
    return out


def real_inverse(X):
    half = len(X) - 1
    n = 2 * half
    if n == 2:
        return [X[0][0] + X[1][0], X[0][0] - X[1][0]]
    quarter = n // 4
    even, odd = [None] * (quarter + 1), [None] * (quarter + 1)
    even[0] = (X[0][0] + X[half][0], None)
    odd[0] = (X[0][0] - X[half][0], None)
    for k in range(1, quarter):
        a, b = X[k], X[half - k]
        even[k] = (a[0] + b[0], a[1] - b[1])
        angle = 2.0 * math.pi * k / n
        odd[k] = rotated(a[0] - b[0], a[1] + b[1], math.cos(angle), math.sin(angle))
    even[quarter] = (2.0 * X[quarter][0], None)
    odd[quarter] = (-2.0 * X[quarter][1], None)
    out = [None] * n
    out[0::2] = real_inverse(even)
    out[1::2] = real_inverse(odd)
    return out


def lane_masks(shape):
    lane = lax.broadcasted_iota(jnp.int32, shape, len(shape) - 1)
    last = shape[-1] - 1
    return (
        (1, jnp.where(lane >= 1, near_weight, 0.0)),
        (last, jnp.where(lane <= last - 1, near_weight, 0.0)),
        (2, jnp.where(lane >= 2, far_weight, 0.0)),
        (last - 1, jnp.where(lane <= last - 2, far_weight, 0.0)),
    )


def neighbour_sum(ref, lead, plane, rows, masks):
    def at(dp, dr):
        return ref[(*lead, plane + dp, pl.ds(PAD + dr, rows), slice(None))]

    centre = at(0, 0)
    near = (at(1, 0) + at(-1, 0)) + (at(0, 1) + at(0, -1))
    far = (at(2, 0) + at(-2, 0)) + (at(0, 2) + at(0, -2))
    total = near_weight * near + far_weight * far
    for amount, mask in masks:
        total = total + pltpu.roll(centre, amount, 1) * mask
    return centre, total


def local_kernel(where, u_hbm, initial_hbm, forcing_hbm, kappa_hbm, reaction_hbm, part, rim, *rest):
    ext, u, initial, forcing, kappa, reaction, sems = rest
    planes, rows, lanes = u.shape
    pairs = ((u_hbm, u), (forcing_hbm, forcing), (kappa_hbm, kappa), (reaction_hbm, reaction))
    pairs += ((initial_hbm, initial),)
    copies = [pltpu.make_async_copy(src, dst, sems.at[i]) for i, (src, dst) in enumerate(pairs)]
    for copy in copies:
        copy.start()
    zero = jnp.zeros((PAD, lanes), jnp.float32)

    def clear(p):
        ext[p, :PAD] = zero
        ext[p, PAD + rows :] = zero

    in_groups(planes + 4, clear)
    blank = jnp.zeros((rows, lanes), jnp.float32)
    for p in (0, 1, planes + 2, planes + 3):
        ext[p, PAD : PAD + rows] = blank
    copies[0].wait()

    def fill(p):
        ext[p + 2, PAD : PAD + rows] = u[p].astype(jnp.float32)

    in_groups(planes, fill)
    for copy in copies[1:]:
        copy.wait()
    masks = lane_masks((rows, lanes))
    first = where[3] == 0

    def one(p):
        centre, total = neighbour_sum(ext, (), p + 2, rows, masks)
        prior = jnp.where(first, initial[p].astype(jnp.float32), 0.0)
        part[p] = (
            forcing[p].astype(jnp.float32)
            - centre
            + prior
            - kappa[p].astype(jnp.float32) * (centre_weight * centre - total)
            - reaction[p].astype(jnp.float32) * centre * centre * centre
        )

    in_groups(planes, one)
    for i, p in enumerate((0, 1, planes - 2, planes - 1)):
        rim[i] = kappa[p].astype(jnp.float32)


def residual_kernel(where, part, rim, even_pair, odd_pair, before, out):
    planes, rows, _ = part.shape
    share = out.shape[2]
    per_plane = rows // share
    half = planes // 2

    def put(p, value):
        value = value.astype(jnp.bfloat16)
        side, inner = p // half, p % half
        for piece in range(per_plane):
            out[per_plane * inner + piece, side] = value[piece * share : (piece + 1) * share]

    for p in range(2, planes - 2):
        put(p, part[p] + before[p].astype(jnp.float32))
    upper = where[4] == 1

    def chosen(a, b, i):
        return jnp.where(upper, a[i].astype(jnp.float32), b[i].astype(jnp.float32))

    l0, l1 = (chosen(even_pair, odd_pair, i) for i in range(2))
    h0, h1 = (chosen(odd_pair, even_pair, i) for i in range(2))
    edges = (
        (0, near_weight * l1 + far_weight * l0),
        (1, far_weight * l1),
        (planes - 2, far_weight * h0),
        (planes - 1, near_weight * h0 + far_weight * h1),
    )
    for i, (p, total) in enumerate(edges):
        put(p, part[p] + rim[i] * total + before[p].astype(jnp.float32))


def either_order(where, body, slots):
    @pl.when(where[2] == 0)
    def _():
        body(list(range(slots)))

    @pl.when(where[2] != 0)
    def _():
        body([(j + slots // 2) % slots for j in range(slots)])


def forward_kernel(where, r, out):
    steps, rows, _ = r.shape
    slots = steps // 2

    def body(places):
        for start in range(0, rows, 16):
            part = pl.ds(start, 16)
            scaled = [
                r[n, part].astype(jnp.float32) * (alpha_ratio ** (n / steps)) for n in range(steps)
            ]
            spectrum = real_dft(scaled)
            out[places[0], 0, part] = spectrum[0][0].astype(jnp.bfloat16)
            out[places[0], 1, part] = spectrum[slots][0].astype(jnp.bfloat16)
            for j in range(1, slots):
                out[places[j], 0, part] = spectrum[j][0].astype(jnp.bfloat16)
                out[places[j], 1, part] = spectrum[j][1].astype(jnp.bfloat16)

    either_order(where, body, slots)


def inverse_kernel(where, s, out):
    steps, rows, _ = out.shape
    slots = steps // 2

    def body(places):
        for start in range(0, rows, 16):
            part = pl.ds(start, 16)

            def given(j, c):
                return s[places[j], c, part].astype(jnp.float32)

            spectrum = [(given(0, 0), None)]
            spectrum += [(given(j, 0), given(j, 1)) for j in range(1, slots)]
            spectrum.append((given(0, 1), None))
            values = real_inverse(spectrum)
            for n in range(steps):
                scale = 1.0 / (alpha_ratio ** (n / steps) * steps)
                out[n, part] = (values[n] * scale).astype(jnp.bfloat16)

    either_order(where, body, slots)


def mirrored(core, i, count):
    return jnp.where(core == 0, i, count - 1 - i)


def coefficient_kernel(where, kappa, initial, reaction, outer, inner, inv, kinv):
    planes = kappa.shape[0]
    wide, narrow = outer.shape[1], inner.shape[1]
    core, slot = where[0], where[1]
    members = STEPS
    factor = math.exp(math.log(alpha_ratio) / members)
    s0 = s1 = si = jnp.float32(0.0)
    for j in range(members // 2):
        phase = 2.0 * math.pi * j / members
        real, imag = 1.0 - factor * math.cos(phase), factor * math.sin(phase)
        hit = slot == j
        s0 = jnp.where(hit, jnp.float32(real), s0)
        s1 = jnp.where(hit, jnp.float32(real if j else 1.0 + factor), s1)
        si = jnp.where(hit, jnp.float32(imag if j else 0.0), si)

    def put(e, kv, iv, rv):
        kv, iv, rv = (v.astype(jnp.float32) for v in (kv, iv, rv))
        base = kv * centre_weight + 3.0 * rv * iv * iv
        d0, d1 = s0 + base, s1 + base
        m0, m1 = d0 * d0 + si * si, d1 * d1 + si * si
        both = 1.0 / (m0 * m1)
        inv0, inv1 = m1 * both, m0 * both
        for c, value in enumerate((d0 * inv0, d1 * inv1, si * inv0)):
            inv[e, c] = value
            kinv[e, c] = kv * value

    def own(i):
        put(wide + mirrored(core, i, planes), kappa[i], initial[i], reaction[i])

    def far(i):
        put(mirrored(core, i, wide), outer[0, i], outer[1, i], outer[2, i])

    def close(i):
        put(wide + planes + mirrored(core, i, narrow), inner[0, i], inner[1, i], inner[2, i])

    in_groups(planes, own)
    in_groups(wide, far)
    in_groups(narrow, close)


def row_starts(rows):
    return (PAD, 2 * PAD + rows)


def write_band(band):
    double, lanes = band.shape
    row = lax.broadcasted_iota(jnp.int32, (double, lanes), 0)
    row = jnp.where(row >= lanes, row - lanes, row)
    gap = jnp.abs(row - lax.broadcasted_iota(jnp.int32, (double, lanes), 1))
    weights = jnp.where(gap == 1, near_weight, jnp.where(gap == 2, far_weight, 0.0))
    band[...] = weights.astype(jnp.bfloat16)


def fill(core, ref, base, inv, x0, x):
    share, rows = ref.shape[2], inv.shape[2]
    per_plane = rows // share
    count = ref.shape[0] // per_plane
    starts = row_starts(rows)

    def body(i):
        e = base + mirrored(core, i, count)
        for h in range(per_plane):
            part = pl.ds(h * share, share)
            re, im = (ref[per_plane * i + h, c].astype(jnp.float32) for c in range(2))
            i0, i1, iq = (inv[e, c, part] for c in range(3))
            for c, value in enumerate((re * i0 + im * iq, im * i1 - re * iq)):
                x0[e, c, part] = value
                x[e, pl.ds(starts[c] + h * share, share)] = value

    in_groups(count, body)


def sweep(step, first, stop, x0, kinv, band, buffers, emit=None):
    rows = kinv.shape[2]
    starts = row_starts(rows)
    src, dst = buffers[step % 2], buffers[(step + 1) % 2]
    weight = sweep_weights()[step]
    group = stop - first
    parts = []
    for u in range(group):
        for start in starts:
            value = src[first + u, pl.ds(start, rows)]
            high = value.astype(jnp.bfloat16)
            low = (value - high.astype(jnp.float32)).astype(jnp.bfloat16)
            parts.append(jnp.concatenate([high, low], axis=1))
    along = jnp.dot(jnp.concatenate(parts, axis=0), band[...], preferred_element_type=jnp.float32)
    for r in range(0, rows, CHUNK):
        columns = [
            [src[first + d, pl.ds(start + r, CHUNK)] for d in range(-2, group + 2)]
            for start in starts
        ]
        for u in range(group):
            e = first + u

            def total(c):
                x = columns[c]
                side = [src[e, pl.ds(starts[c] + r + d, CHUNK)] for d in (1, -1, 2, -2)]
                near = (x[u + 3] + x[u + 1]) + (side[0] + side[1])
                far = (x[u + 4] + x[u]) + (side[2] + side[3])
                k = (2 * u + c) * rows + r
                return near_weight * near + far_weight * far + along[k : k + CHUNK]

            re, im = columns[0][u + 2], columns[1][u + 2]
            sum_re, sum_im = total(0), total(1)
            part = pl.ds(r, CHUNK)
            k0, k1, kq = (kinv[e, c, part] for c in range(3))
            pair = (
                (1.0 - weight) * re + weight * (x0[e, 0, part] + k0 * sum_re + kq * sum_im),
                (1.0 - weight) * im + weight * (x0[e, 1, part] + k1 * sum_im - kq * sum_re),
            )
            for c, value in enumerate(pair):
                if emit is None:
                    dst[e, pl.ds(starts[c] + r, CHUNK)] = value
                else:
                    emit(e, r, c, value)


def inside_kernel(where, y, yb, inv, kinv, x0, xs, xt, band):
    rows, lanes = inv.shape[2:]
    own = y.shape[0] * y.shape[2] // rows
    core = where[0]
    base = (inv.shape[0] - own) // 2
    write_band(band)
    zero = jnp.zeros((PAD, lanes), jnp.float32)

    def clear(e):
        for x in (xs, xt):
            for r in (0, PAD + rows, 2 * (PAD + rows)):
                x[e, pl.ds(r, PAD)] = zero

    in_groups(inv.shape[0], clear)
    fill(core, y, base, inv, x0, xs)
    fill(core, yb, base + own, inv, x0, xs)
    for step in range(EARLY):
        edge = 2 * (step + 1)
        sweep(step, base + edge, base + 2 * own - edge, x0, kinv, band, (xs, xt))


def sweeps_kernel(where, y_a, yc, yd, inv, kinv, _x0, _xs, _xt, out, x0, xs, xt, band):
    ext, _, rows, _ = inv.shape
    share = y_a.shape[2]
    per_plane = rows // share
    own = y_a.shape[0] // per_plane
    core = where[0]
    base = (ext - own) // 2
    write_band(band)
    fill(core, y_a, base - own, inv, x0, xs)
    fill(core, yc, 0, inv, x0, xs)
    fill(core, yd, base + 2 * own, inv, x0, xs)

    def emit(e, r, c, value):
        i = mirrored(core, e - base, own)
        out[per_plane * i + r // share, c, pl.ds(r % share, CHUNK)] = value.astype(jnp.bfloat16)

    for step in range(SWEEPS):
        edge = 2 * (step + 1)
        if step < EARLY:
            sweep(step, edge, base + edge, x0, kinv, band, (xs, xt))
            sweep(step, base + 2 * own - edge, ext - edge, x0, kinv, band, (xs, xt))
        else:
            last = step == SWEEPS - 1
            sweep(step, edge, ext - edge, x0, kinv, band, (xs, xt), emit if last else None)


def final_kernel(state, correction, out):
    planes, rows, _ = state.shape
    share = correction.shape[2]
    per_plane = rows // share
    half = planes // 2

    for p in range(planes):
        part, inner = p // half, p % half
        value = jnp.concatenate(
            [
                correction[per_plane * inner + h, part].astype(jnp.float32)
                for h in range(per_plane)
            ],
            axis=0,
        )
        out[p] = (state[p].astype(jnp.float32) + value).astype(jnp.bfloat16)


def place():
    slots = lax.axis_size(CHIPS)
    side, chip, core = (lax.axis_index(a) for a in TM)
    slab = lax.axis_index("space")
    per_side = lax.axis_size("tm_1")
    flip = slab // 2 % 2
    slot = (side * per_side + chip + flip * (slots // 2)) % slots
    timestep = (side * per_side + chip) * lax.axis_size("tm_2") + core
    return core, slot, flip, timestep, slab % 2


def placed(kernel):
    return lambda *refs: kernel(place(), *refs)


def call(kernel, shapes, inputs, scratch=(), anywhere=0, flops=None, aliases=None):
    outs = [jax.ShapeDtypeStruct(s, d) for s, d in shapes]
    cost = None
    if flops is not None:
        cost = pl.CostEstimate(flops=flops, transcendentals=0, bytes_accessed=flops // 8)
    rest = len(inputs) - anywhere
    return pl.pallas_call(
        kernel,
        out_shape=outs,
        in_specs=[HBM] * anywhere + [VMEM] * rest,
        out_specs=[VMEM] * len(outs),
        scratch_shapes=list(scratch),
        cost_estimate=cost,
        input_output_aliases=aliases or {},
        compiler_params=pltpu.CompilerParams(vmem_limit_bytes=24 << 20),
    )(*inputs)


def iteration(state, initial, forcing, kappa, reaction):
    _, planes, rows, lanes = state.shape
    members = lax.axis_size(TM)
    slots = lax.axis_size(CHIPS)
    slabs = lax.axis_size("space")
    own = planes // 2
    share = own * rows // slots
    per_plane = rows // share
    wide = 2 * SWEEPS
    narrow = wide - own
    ext = own + 2 * wide
    bf16, f32 = jnp.bfloat16, jnp.float32
    core = lax.axis_index("tm_2")
    u = state[0]

    outer, same = [], []
    for side in range(2):
        for t in range(slabs - 1):
            near, beside = side * 2 * slabs, (side ^ (t % 2)) * 2 * slabs
            low, high = near + slabs + t, beside + t + 1
            outer += [(low, high), (high, low)]
            same += [(near + t, beside + t + 1), (beside + slabs + t + 1, near + slabs + t)]
    swap = [(i, slabs + i) for i in range(slabs)] + [(slabs + i, i) for i in range(slabs)]
    odd = lax.axis_index("space") % 2
    even_first = [p for s in range(0, slabs - 1, 2) for p in ((s, s + 1), (s + 1, s))]
    odd_first = [p for s in range(1, slabs - 1, 2) for p in ((s, s + 1), (s + 1, s))]
    low, high = u[:2], u[planes - 2 :]
    even_pair = lax.ppermute(jnp.where(odd == 1, low, high), "space", even_first)
    odd_pair = lax.ppermute(jnp.where(odd == 1, high, low), "space", odd_first)
    before = lax.ppermute(u, TM, [(i, i + 1) for i in range(members - 1)])
    coefs = jnp.stack([kappa, initial, reaction])
    rim = jnp.where(core == 0, coefs[:, :wide], coefs[:, planes - wide :])
    rim = lax.ppermute(rim, SIDE_CORE_SPACE, outer)
    inner = jnp.where(core == 0, rim[:, wide - narrow :], rim[:, :narrow])
    inner = lax.ppermute(inner, CORE_SPACE, swap)

    block = ((planes, rows, lanes), bf16)
    part, edge = call(
        placed(local_kernel),
        [((planes, rows, lanes), f32), ((4, rows, lanes), f32)],
        [
            pltpu.with_memory_space_constraint(v, pltpu.HBM)
            for v in (u, initial, forcing[0], kappa, reaction)
        ],
        [pltpu.VMEM((planes + 4, rows + 2 * PAD, lanes), f32)]
        + [pltpu.VMEM(*block)] * 5
        + [pltpu.SemaphoreType.DMA((5,))],
        anywhere=5,
        flops=20_000_000,
    )
    (residual,) = call(
        placed(residual_kernel),
        [((slots, 2, share, lanes), bf16)],
        [part, edge, even_pair, odd_pair, before],
    )
    cells = lax.all_to_all(residual.reshape(members, share, lanes), TM, 0, 0, tiled=True)
    (spectrum,) = call(placed(forward_kernel), [((slots, 2, share, lanes), bf16)], [cells])
    y = lax.all_to_all(spectrum, CHIPS, 0, 0, tiled=True)

    fields = call(
        placed(coefficient_kernel),
        [((ext, 3, rows, lanes), f32)] * 2,
        [kappa, initial, reaction, rim, inner],
    )
    n = per_plane * narrow
    first = core == 0
    ya = lax.ppermute(y, SIDE_CORE_SPACE, outer)
    yc = lax.ppermute(jnp.where(first, y[-n:], y[:n]), SIDE_CORE_SPACE, same)
    yb = lax.ppermute(y, CORE_SPACE, swap)
    yd = lax.ppermute(jnp.where(first, ya[-n:], ya[:n]), CORE_SPACE, swap)
    tall = 2 * rows + 3 * PAD
    buffers = [((ext, 2, rows + PAD, lanes), f32), ((ext, tall, lanes), f32), ((ext, tall, lanes), f32)]
    band = [pltpu.VMEM((2 * lanes, lanes), bf16)]
    state_arrays = call(placed(inside_kernel), buffers, [y, yb, *fields], band)
    solved = call(
        placed(sweeps_kernel),
        [((slots, 2, share, lanes), bf16), *buffers],
        [ya, yc, yd, *fields, *state_arrays],
        band,
        aliases={5: 1, 6: 2, 7: 3},
    )[0]
    modes = lax.all_to_all(solved, CHIPS, 0, 0, tiled=True)
    (correction,) = call(placed(inverse_kernel), [((members, share, lanes), bf16)], [modes])
    returned = lax.all_to_all(correction, TM, 0, 0, tiled=True)
    (updated,) = call(
        final_kernel, [((planes, rows, lanes), bf16)], [u, returned.reshape(slots, 2, share, lanes)]
    )
    return updated[None]


def solution(mesh):
    torus = Mesh(
        mesh.devices.reshape(2, 8, 2, mesh.shape["space"]), ("tm_0", "tm_1", "tm_2", "space")
    )
    in_specs = (
        P(TM, "space", None, None),
        P("space", None, None),
        P(TM, "space", None, None),
        P("space", None, None),
        P("space", None, None),
    )
    out_specs = P(TM, "space", None, None)
    return jax.shard_map(
        iteration, mesh=torus, in_specs=in_specs, out_specs=out_specs, check_vma=False
    )
```

```python
import math

import jax
import jax.numpy as jnp
from jax import lax
from jax.experimental import pallas as pl
from jax.experimental.pallas import tpu as pltpu
from jax.sharding import Mesh
from jax.sharding import PartitionSpec as P

SWEEPS = 6
STEPS = 32
CHUNK = 16
EARLY = 2
TM = ("tm_0", "tm_1", "tm_2")
CHIPS = ("tm_0", "tm_1")
CORE_SPACE = ("tm_2", "space")
SIDE_CORE_SPACE = ("tm_0", "tm_2", "space")

alpha_ratio = 0.25
near_weight = 0.5
far_weight = 1.0
centre_weight = 6.0 * (near_weight + far_weight)
VMEM = pl.BlockSpec(memory_space=pltpu.VMEM)
HBM = pl.BlockSpec(memory_space=pltpu.HBM)
PAD = 8


def sweep_weights():
    return [
        1.0 / (1.0 + 0.4 * math.cos(math.pi * (2 * k + 1) / (2 * SWEEPS))) for k in range(SWEEPS)
    ]


def in_groups(count, body, group=4):
    def step(i, _):
        for u in range(group):
            body(group * i + u)
        return 0

    lax.fori_loop(0, count // group, step, 0)


def rotated(re, im, c, s):
    if abs(s) < 1e-12:
        return re * c, im * c
    if abs(c) < 1e-12:
        return -im * s, re * s
    return re * c - im * s, re * s + im * c


def real_dft(x):
    n = len(x)
    if n == 2:
        return [(x[0] + x[1], None), (x[0] - x[1], None)]
    even, odd = real_dft(x[0::2]), real_dft(x[1::2])
    half = n // 2
    out = [None] * (half + 1)
    out[0] = (even[0][0] + odd[0][0], None)
    out[half] = (even[0][0] - odd[0][0], None)
    for k in range(1, n // 4):
        angle = -2.0 * math.pi * k / n
        re, im = rotated(odd[k][0], odd[k][1], math.cos(angle), math.sin(angle))
        out[k] = (even[k][0] + re, even[k][1] + im)
        out[half - k] = (even[k][0] - re, im - even[k][1])
    quarter = n // 4
    out[quarter] = (even[quarter][0], -odd[quarter][0])
    return out


def real_inverse(X):
    half = len(X) - 1
    n = 2 * half
    if n == 2:
        return [X[0][0] + X[1][0], X[0][0] - X[1][0]]
    quarter = n // 4
    even, odd = [None] * (quarter + 1), [None] * (quarter + 1)
    even[0] = (X[0][0] + X[half][0], None)
    odd[0] = (X[0][0] - X[half][0], None)
    for k in range(1, quarter):
        a, b = X[k], X[half - k]
        even[k] = (a[0] + b[0], a[1] - b[1])
        angle = 2.0 * math.pi * k / n
        odd[k] = rotated(a[0] - b[0], a[1] + b[1], math.cos(angle), math.sin(angle))
    even[quarter] = (2.0 * X[quarter][0], None)
    odd[quarter] = (-2.0 * X[quarter][1], None)
    out = [None] * n
    out[0::2] = real_inverse(even)
    out[1::2] = real_inverse(odd)
    return out


def lane_masks(shape):
    lane = lax.broadcasted_iota(jnp.int32, shape, len(shape) - 1)
    last = shape[-1] - 1
    return (
        (1, jnp.where(lane >= 1, near_weight, 0.0)),
        (last, jnp.where(lane <= last - 1, near_weight, 0.0)),
        (2, jnp.where(lane >= 2, far_weight, 0.0)),
        (last - 1, jnp.where(lane <= last - 2, far_weight, 0.0)),
    )


def neighbour_sum(ref, lead, plane, rows, masks):
    def at(dp, dr):
        return ref[(*lead, plane + dp, pl.ds(PAD + dr, rows), slice(None))]

    centre = at(0, 0)
    near = (at(1, 0) + at(-1, 0)) + (at(0, 1) + at(0, -1))
    far = (at(2, 0) + at(-2, 0)) + (at(0, 2) + at(0, -2))
    total = near_weight * near + far_weight * far
    for amount, mask in masks:
        total = total + pltpu.roll(centre, amount, 1) * mask
    return centre, total


def local_kernel(where, u_hbm, initial_hbm, forcing_hbm, kappa_hbm, reaction_hbm, part, rim, *rest):
    ext, u, initial, forcing, kappa, reaction, sems = rest
    planes, rows, lanes = u.shape
    pairs = ((u_hbm, u), (forcing_hbm, forcing), (kappa_hbm, kappa), (reaction_hbm, reaction))
    pairs += ((initial_hbm, initial),)
    copies = [pltpu.make_async_copy(src, dst, sems.at[i]) for i, (src, dst) in enumerate(pairs)]
    for copy in copies:
        copy.start()
    zero = jnp.zeros((PAD, lanes), jnp.float32)

    def clear(p):
        ext[p, :PAD] = zero
        ext[p, PAD + rows :] = zero

    in_groups(planes + 4, clear)
    blank = jnp.zeros((rows, lanes), jnp.float32)
    for p in (0, 1, planes + 2, planes + 3):
        ext[p, PAD : PAD + rows] = blank
    copies[0].wait()

    def fill(p):
        ext[p + 2, PAD : PAD + rows] = u[p].astype(jnp.float32)

    in_groups(planes, fill)
    for copy in copies[1:]:
        copy.wait()
    masks = lane_masks((rows, lanes))
    first = where[3] == 0

    def one(p):
        centre, total = neighbour_sum(ext, (), p + 2, rows, masks)
        prior = jnp.where(first, initial[p].astype(jnp.float32), 0.0)
        part[p] = (
            forcing[p].astype(jnp.float32)
            - centre
            + prior
            - kappa[p].astype(jnp.float32) * (centre_weight * centre - total)
            - reaction[p].astype(jnp.float32) * centre * centre * centre
        )

    in_groups(planes, one)
    for i, p in enumerate((0, 1, planes - 2, planes - 1)):
        rim[i] = kappa[p].astype(jnp.float32)


def residual_kernel(where, part, rim, even_pair, odd_pair, before, out):
    planes, rows, _ = part.shape
    share = out.shape[2]
    per_plane = rows // share
    half = planes // 2

    def put(p, value):
        value = value.astype(jnp.bfloat16)
        side, inner = p // half, p % half
        for piece in range(per_plane):
            out[per_plane * inner + piece, side] = value[piece * share : (piece + 1) * share]

    for p in range(2, planes - 2):
        put(p, part[p] + before[p].astype(jnp.float32))
    upper = where[4] == 1

    def chosen(a, b, i):
        return jnp.where(upper, a[i].astype(jnp.float32), b[i].astype(jnp.float32))

    l0, l1 = (chosen(even_pair, odd_pair, i) for i in range(2))
    h0, h1 = (chosen(odd_pair, even_pair, i) for i in range(2))
    edges = (
        (0, near_weight * l1 + far_weight * l0),
        (1, far_weight * l1),
        (planes - 2, far_weight * h0),
        (planes - 1, near_weight * h0 + far_weight * h1),
    )
    for i, (p, total) in enumerate(edges):
        put(p, part[p] + rim[i] * total + before[p].astype(jnp.float32))


def either_order(where, body, slots):
    @pl.when(where[2] == 0)
    def _():
        body(list(range(slots)))

    @pl.when(where[2] != 0)
    def _():
        body([(j + slots // 2) % slots for j in range(slots)])


def forward_kernel(where, r, out):
    steps, rows, _ = r.shape
    slots = steps // 2

    def body(places):
        for start in range(0, rows, 16):
            part = pl.ds(start, 16)
            scaled = [
                r[n, part].astype(jnp.float32) * (alpha_ratio ** (n / steps)) for n in range(steps)
            ]
            spectrum = real_dft(scaled)
            out[places[0], 0, part] = spectrum[0][0].astype(jnp.bfloat16)
            out[places[0], 1, part] = spectrum[slots][0].astype(jnp.bfloat16)
            for j in range(1, slots):
                out[places[j], 0, part] = spectrum[j][0].astype(jnp.bfloat16)
                out[places[j], 1, part] = spectrum[j][1].astype(jnp.bfloat16)

    either_order(where, body, slots)


def inverse_kernel(where, s, out):
    steps, rows, _ = out.shape
    slots = steps // 2

    def body(places):
        for start in range(0, rows, 16):
            part = pl.ds(start, 16)

            def given(j, c):
                return s[places[j], c, part].astype(jnp.float32)

            spectrum = [(given(0, 0), None)]
            spectrum += [(given(j, 0), given(j, 1)) for j in range(1, slots)]
            spectrum.append((given(0, 1), None))
            values = real_inverse(spectrum)
            for n in range(steps):
                scale = 1.0 / (alpha_ratio ** (n / steps) * steps)
                out[n, part] = (values[n] * scale).astype(jnp.bfloat16)

    either_order(where, body, slots)


def mirrored(core, i, count):
    return jnp.where(core == 0, i, count - 1 - i)


def coefficients(where, inv, kinv):
    slot = where[1]
    factor = math.exp(math.log(alpha_ratio) / STEPS)
    s0 = s1 = si = jnp.float32(0.0)
    for j in range(STEPS // 2):
        phase = 2.0 * math.pi * j / STEPS
        real, imag = 1.0 - factor * math.cos(phase), factor * math.sin(phase)
        hit = slot == j
        s0 = jnp.where(hit, jnp.float32(real), s0)
        s1 = jnp.where(hit, jnp.float32(real if j else 1.0 + factor), s1)
        si = jnp.where(hit, jnp.float32(imag if j else 0.0), si)

    def put(e, kv, iv, rv):
        kv, iv, rv = (v.astype(jnp.float32) for v in (kv, iv, rv))
        base = kv * centre_weight + 3.0 * rv * iv * iv
        d0, d1 = s0 + base, s1 + base
        m0, m1 = d0 * d0 + si * si, d1 * d1 + si * si
        both = 1.0 / (m0 * m1)
        inv0, inv1 = m1 * both, m0 * both
        for c, value in enumerate((d0 * inv0, d1 * inv1, si * inv0)):
            inv[e, c] = value
            kinv[e, c] = kv * value

    return put


def slab_kernel(where, kappa, initial, reaction, inv, kinv):
    planes = kappa.shape[0]
    put = coefficients(where, inv, kinv)

    def own(i):
        put(mirrored(where[0], i, planes), kappa[i], initial[i], reaction[i])

    in_groups(planes, own)


def rim_kernel(where, outer, inner, inv, kinv):
    wide, narrow = outer.shape[1], inner.shape[1]
    core = where[0]
    put = coefficients(where, inv, kinv)

    def far(i):
        put(mirrored(core, i, wide), outer[0, i], outer[1, i], outer[2, i])

    def close(i):
        put(wide + mirrored(core, i, narrow), inner[0, i], inner[1, i], inner[2, i])

    in_groups(wide, far)
    in_groups(narrow, close)


def row_starts(rows):
    return (PAD, 2 * PAD + rows)


def write_band(band):
    double, lanes = band.shape
    row = lax.broadcasted_iota(jnp.int32, (double, lanes), 0)
    row = jnp.where(row >= lanes, row - lanes, row)
    gap = jnp.abs(row - lax.broadcasted_iota(jnp.int32, (double, lanes), 1))
    weights = jnp.where(gap == 1, near_weight, jnp.where(gap == 2, far_weight, 0.0))
    band[...] = weights.astype(jnp.bfloat16)


def fill(core, ref, base, inv, first, x0, x):
    share, rows = ref.shape[2], inv.shape[2]
    per_plane = rows // share
    count = ref.shape[0] // per_plane
    starts = row_starts(rows)

    def body(i):
        place_in = mirrored(core, i, count)
        e = base + place_in
        for h in range(per_plane):
            part = pl.ds(h * share, share)
            re, im = (ref[per_plane * i + h, c].astype(jnp.float32) for c in range(2))
            i0, i1, iq = (inv[first + place_in, c, part] for c in range(3))
            for c, value in enumerate((re * i0 + im * iq, im * i1 - re * iq)):
                x0[e, c, part] = value
                x[e, pl.ds(starts[c] + h * share, share)] = value

    in_groups(count, body)


def sweep(step, first, stop, x0, kinvs, band, buffers, emit=None):
    slab, rims = kinvs
    rows = slab.shape[2]
    wide = (x0.shape[0] - slab.shape[0] // 2) // 2
    starts = row_starts(rows)
    src, dst = buffers[step % 2], buffers[(step + 1) % 2]
    weight = sweep_weights()[step]
    group = stop - first
    parts = []
    for u in range(group):
        for start in starts:
            value = src[first + u, pl.ds(start, rows)]
            high = value.astype(jnp.bfloat16)
            low = (value - high.astype(jnp.float32)).astype(jnp.bfloat16)
            parts.append(jnp.concatenate([high, low], axis=1))
    along = jnp.dot(jnp.concatenate(parts, axis=0), band[...], preferred_element_type=jnp.float32)
    for r in range(0, rows, CHUNK):
        columns = [
            [src[first + d, pl.ds(start + r, CHUNK)] for d in range(-2, group + 2)]
            for start in starts
        ]
        for u in range(group):
            e = first + u

            def total(c):
                x = columns[c]
                side = [src[e, pl.ds(starts[c] + r + d, CHUNK)] for d in (1, -1, 2, -2)]
                near = (x[u + 3] + x[u + 1]) + (side[0] + side[1])
                far = (x[u + 4] + x[u]) + (side[2] + side[3])
                k = (2 * u + c) * rows + r
                return near_weight * near + far_weight * far + along[k : k + CHUNK]

            re, im = columns[0][u + 2], columns[1][u + 2]
            sum_re, sum_im = total(0), total(1)
            part = pl.ds(r, CHUNK)
            if wide <= e < wide + slab.shape[0]:
                k0, k1, kq = (slab[e - wide, c, part] for c in range(3))
            else:
                k_e = e if e < wide else e - slab.shape[0]
                k0, k1, kq = (rims[k_e, c, part] for c in range(3))
            pair = (
                (1.0 - weight) * re + weight * (x0[e, 0, part] + k0 * sum_re + kq * sum_im),
                (1.0 - weight) * im + weight * (x0[e, 1, part] + k1 * sum_im - kq * sum_re),
            )
            for c, value in enumerate(pair):
                if emit is None:
                    dst[e, pl.ds(starts[c] + r, CHUNK)] = value
                else:
                    emit(e, r, c, value)


def inside_kernel(where, y, yb, inv, kinv, x0, xs, xt, band):
    rows, lanes = inv.shape[2:]
    own = y.shape[0] * y.shape[2] // rows
    core = where[0]
    base = (x0.shape[0] - own) // 2
    write_band(band)
    zero = jnp.zeros((PAD, lanes), jnp.float32)

    def clear(e):
        for x in (xs, xt):
            for r in (0, PAD + rows, 2 * (PAD + rows)):
                x[e, pl.ds(r, PAD)] = zero

    in_groups(x0.shape[0], clear)
    fill(core, y, base, inv, 0, x0, xs)
    fill(core, yb, base + own, inv, own, x0, xs)
    for step in range(EARLY):
        edge = 2 * (step + 1)
        sweep(step, base + edge, base + 2 * own - edge, x0, (kinv, None), band, (xs, xt))


def sweeps_kernel(where, y_a, yc, yd, kslab, inv, krim, _x0, _xs, _xt, out, x0, xs, xt, band):
    rows, _ = inv.shape[2:]
    ext = x0.shape[0]
    share = y_a.shape[2]
    per_plane = rows // share
    own = y_a.shape[0] // per_plane
    core = where[0]
    base = (ext - own) // 2
    kinv = (kslab, krim)
    write_band(band)
    fill(core, y_a, base - own, inv, base - own, x0, xs)
    fill(core, yc, 0, inv, 0, x0, xs)
    fill(core, yd, base + 2 * own, inv, base, x0, xs)

    def emit(e, r, c, value):
        i = mirrored(core, e - base, own)
        out[per_plane * i + r // share, c, pl.ds(r % share, CHUNK)] = value.astype(jnp.bfloat16)

    for step in range(SWEEPS):
        edge = 2 * (step + 1)
        if step < EARLY:
            sweep(step, edge, base + edge, x0, kinv, band, (xs, xt))
            sweep(step, base + 2 * own - edge, ext - edge, x0, kinv, band, (xs, xt))
        else:
            last = step == SWEEPS - 1
            sweep(step, edge, ext - edge, x0, kinv, band, (xs, xt), emit if last else None)


def final_kernel(state, correction, out):
    planes, rows, _ = state.shape
    share = correction.shape[2]
    per_plane = rows // share
    half = planes // 2

    for p in range(planes):
        part, inner = p // half, p % half
        value = jnp.concatenate(
            [
                correction[per_plane * inner + h, part].astype(jnp.float32)
                for h in range(per_plane)
            ],
            axis=0,
        )
        out[p] = (state[p].astype(jnp.float32) + value).astype(jnp.bfloat16)


def place():
    slots = lax.axis_size(CHIPS)
    side, chip, core = (lax.axis_index(a) for a in TM)
    slab = lax.axis_index("space")
    per_side = lax.axis_size("tm_1")
    flip = slab // 2 % 2
    slot = (side * per_side + chip + flip * (slots // 2)) % slots
    timestep = (side * per_side + chip) * lax.axis_size("tm_2") + core
    return core, slot, flip, timestep, slab % 2


def placed(kernel):
    return lambda *refs: kernel(place(), *refs)


def call(kernel, shapes, inputs, scratch=(), anywhere=0, flops=None, aliases=None):
    outs = [jax.ShapeDtypeStruct(s, d) for s, d in shapes]
    cost = None
    if flops is not None:
        cost = pl.CostEstimate(flops=flops, transcendentals=0, bytes_accessed=flops // 8)
    rest = len(inputs) - anywhere
    return pl.pallas_call(
        kernel,
        out_shape=outs,
        in_specs=[HBM] * anywhere + [VMEM] * rest,
        out_specs=[VMEM] * len(outs),
        scratch_shapes=list(scratch),
        cost_estimate=cost,
        input_output_aliases=aliases or {},
        compiler_params=pltpu.CompilerParams(vmem_limit_bytes=24 << 20),
    )(*inputs)


def iteration(state, initial, forcing, kappa, reaction):
    _, planes, rows, lanes = state.shape
    members = lax.axis_size(TM)
    slots = lax.axis_size(CHIPS)
    slabs = lax.axis_size("space")
    own = planes // 2
    share = own * rows // slots
    per_plane = rows // share
    wide = 2 * SWEEPS
    narrow = wide - own
    ext = own + 2 * wide
    bf16, f32 = jnp.bfloat16, jnp.float32
    core = lax.axis_index("tm_2")
    u = state[0]

    outer, same = [], []
    for side in range(2):
        for t in range(slabs - 1):
            near, beside = side * 2 * slabs, (side ^ (t % 2)) * 2 * slabs
            low, high = near + slabs + t, beside + t + 1
            outer += [(low, high), (high, low)]
            same += [(near + t, beside + t + 1), (beside + slabs + t + 1, near + slabs + t)]
    swap = [(i, slabs + i) for i in range(slabs)] + [(slabs + i, i) for i in range(slabs)]
    odd = lax.axis_index("space") % 2
    even_first = [p for s in range(0, slabs - 1, 2) for p in ((s, s + 1), (s + 1, s))]
    odd_first = [p for s in range(1, slabs - 1, 2) for p in ((s, s + 1), (s + 1, s))]
    low, high = u[:2], u[planes - 2 :]
    even_pair = lax.ppermute(jnp.where(odd == 1, low, high), "space", even_first)
    odd_pair = lax.ppermute(jnp.where(odd == 1, high, low), "space", odd_first)
    before = lax.ppermute(u, TM, [(i, i + 1) for i in range(members - 1)])
    coefs = jnp.stack([kappa, initial, reaction])
    rim = jnp.where(core == 0, coefs[:, :wide], coefs[:, planes - wide :])
    rim = lax.ppermute(rim, SIDE_CORE_SPACE, outer)
    inner = jnp.where(core == 0, rim[:, wide - narrow :], rim[:, :narrow])
    inner = lax.ppermute(inner, CORE_SPACE, swap)

    block = ((planes, rows, lanes), bf16)
    part, edge = call(
        placed(local_kernel),
        [((planes, rows, lanes), f32), ((4, rows, lanes), f32)],
        [
            pltpu.with_memory_space_constraint(v, pltpu.HBM)
            for v in (u, initial, forcing[0], kappa, reaction)
        ],
        [pltpu.VMEM((planes + 4, rows + 2 * PAD, lanes), f32)]
        + [pltpu.VMEM(*block)] * 5
        + [pltpu.SemaphoreType.DMA((5,))],
        anywhere=5,
        flops=20_000_000,
    )
    (residual,) = call(
        placed(residual_kernel),
        [((slots, 2, share, lanes), bf16)],
        [part, edge, even_pair, odd_pair, before],
    )
    cells = lax.all_to_all(residual.reshape(members, share, lanes), TM, 0, 0, tiled=True)
    (spectrum,) = call(placed(forward_kernel), [((slots, 2, share, lanes), bf16)], [cells])
    y = lax.all_to_all(spectrum, CHIPS, 0, 0, tiled=True)

    table = [((planes, 3, rows, lanes), f32)] * 2
    inv_slab, kinv_slab = call(placed(slab_kernel), table, [kappa, initial, reaction])
    table = [((wide + narrow, 3, rows, lanes), f32)] * 2
    inv_rim, kinv_rim = call(placed(rim_kernel), table, [rim, inner])
    n = per_plane * narrow
    first = core == 0
    ya = lax.ppermute(y, SIDE_CORE_SPACE, outer)
    yc = lax.ppermute(jnp.where(first, y[-n:], y[:n]), SIDE_CORE_SPACE, same)
    yb = lax.ppermute(y, CORE_SPACE, swap)
    yd = lax.ppermute(jnp.where(first, ya[-n:], ya[:n]), CORE_SPACE, swap)
    tall = 2 * rows + 3 * PAD
    buffers = [((ext, 2, rows + PAD, lanes), f32), ((ext, tall, lanes), f32), ((ext, tall, lanes), f32)]
    band = [pltpu.VMEM((2 * lanes, lanes), bf16)]
    state_arrays = call(placed(inside_kernel), buffers, [y, yb, inv_slab, kinv_slab], band)
    solved = call(
        placed(sweeps_kernel),
        [((slots, 2, share, lanes), bf16), *buffers],
        [ya, yc, yd, kinv_slab, inv_rim, kinv_rim, *state_arrays],
        band,
        aliases={6: 1, 7: 2, 8: 3},
    )[0]
    modes = lax.all_to_all(solved, CHIPS, 0, 0, tiled=True)
    (correction,) = call(placed(inverse_kernel), [((members, share, lanes), bf16)], [modes])
    returned = lax.all_to_all(correction, TM, 0, 0, tiled=True)
    (updated,) = call(
        final_kernel, [((planes, rows, lanes), bf16)], [u, returned.reshape(slots, 2, share, lanes)]
    )
    return updated[None]


def solution(mesh):
    torus = Mesh(
        mesh.devices.reshape(2, 8, 2, mesh.shape["space"]), ("tm_0", "tm_1", "tm_2", "space")
    )
    in_specs = (
        P(TM, "space", None, None),
        P("space", None, None),
        P(TM, "space", None, None),
        P("space", None, None),
        P("space", None, None),
    )
    out_specs = P(TM, "space", None, None)
    return jax.shard_map(
        iteration, mesh=torus, in_specs=in_specs, out_specs=out_specs, check_vma=False
    )
```

```python
import math

import jax
import jax.numpy as jnp
from jax import lax
from jax.experimental import pallas as pl
from jax.experimental.pallas import tpu as pltpu
from jax.sharding import Mesh
from jax.sharding import PartitionSpec as P

SWEEPS = 6
STEPS = 32
CHUNK = 16
EARLY = 3
TM = ("tm_0", "tm_1", "tm_2")
CHIPS = ("tm_0", "tm_1")
CORE_SPACE = ("tm_2", "space")
SIDE_CORE_SPACE = ("tm_0", "tm_2", "space")

alpha_ratio = 0.25
near_weight = 0.5
far_weight = 1.0
centre_weight = 6.0 * (near_weight + far_weight)
VMEM = pl.BlockSpec(memory_space=pltpu.VMEM)
HBM = pl.BlockSpec(memory_space=pltpu.HBM)
PAD = 8


def sweep_weights():
    return [
        1.0 / (1.0 + 0.4 * math.cos(math.pi * (2 * k + 1) / (2 * SWEEPS))) for k in range(SWEEPS)
    ]


def scaled(weight, value):
    return value if weight == 1.0 else weight * value


def in_groups(count, body, group=4):
    def step(i, _):
        for u in range(group):
            body(group * i + u)
        return 0

    lax.fori_loop(0, count // group, step, 0)


def rotated(re, im, c, s):
    if abs(s) < 1e-12:
        return re * c, im * c
    if abs(c) < 1e-12:
        return -im * s, re * s
    return re * c - im * s, re * s + im * c


def real_dft(x):
    n = len(x)
    if n == 2:
        return [(x[0] + x[1], None), (x[0] - x[1], None)]
    even, odd = real_dft(x[0::2]), real_dft(x[1::2])
    half = n // 2
    out = [None] * (half + 1)
    out[0] = (even[0][0] + odd[0][0], None)
    out[half] = (even[0][0] - odd[0][0], None)
    for k in range(1, n // 4):
        angle = -2.0 * math.pi * k / n
        re, im = rotated(odd[k][0], odd[k][1], math.cos(angle), math.sin(angle))
        out[k] = (even[k][0] + re, even[k][1] + im)
        out[half - k] = (even[k][0] - re, im - even[k][1])
    quarter = n // 4
    out[quarter] = (even[quarter][0], -odd[quarter][0])
    return out


def real_inverse(X):
    half = len(X) - 1
    n = 2 * half
    if n == 2:
        return [X[0][0] + X[1][0], X[0][0] - X[1][0]]
    quarter = n // 4
    even, odd = [None] * (quarter + 1), [None] * (quarter + 1)
    even[0] = (X[0][0] + X[half][0], None)
    odd[0] = (X[0][0] - X[half][0], None)
    for k in range(1, quarter):
        a, b = X[k], X[half - k]
        even[k] = (a[0] + b[0], a[1] - b[1])
        angle = 2.0 * math.pi * k / n
        odd[k] = rotated(a[0] - b[0], a[1] + b[1], math.cos(angle), math.sin(angle))
    even[quarter] = (2.0 * X[quarter][0], None)
    odd[quarter] = (-2.0 * X[quarter][1], None)
    out = [None] * n
    out[0::2] = real_inverse(even)
    out[1::2] = real_inverse(odd)
    return out


def lane_masks(shape):
    lane = lax.broadcasted_iota(jnp.int32, shape, len(shape) - 1)
    last = shape[-1] - 1
    return (
        (1, jnp.where(lane >= 1, near_weight, 0.0)),
        (last, jnp.where(lane <= last - 1, near_weight, 0.0)),
        (2, jnp.where(lane >= 2, far_weight, 0.0)),
        (last - 1, jnp.where(lane <= last - 2, far_weight, 0.0)),
    )


def neighbour_sum(ref, lead, plane, rows, masks):
    def at(dp, dr):
        return ref[(*lead, plane + dp, pl.ds(PAD + dr, rows), slice(None))]

    centre = at(0, 0)
    near = (at(1, 0) + at(-1, 0)) + (at(0, 1) + at(0, -1))
    far = (at(2, 0) + at(-2, 0)) + (at(0, 2) + at(0, -2))
    total = scaled(near_weight, near) + scaled(far_weight, far)
    for amount, mask in masks:
        total = total + pltpu.roll(centre, amount, 1) * mask
    return centre, total


def local_kernel(where, u_hbm, initial_hbm, forcing_hbm, kappa_hbm, reaction_hbm, part, rim, *rest):
    ext, u, initial, forcing, kappa, reaction, sems = rest
    planes, rows, lanes = u.shape
    pairs = ((u_hbm, u), (forcing_hbm, forcing), (kappa_hbm, kappa), (reaction_hbm, reaction))
    pairs += ((initial_hbm, initial),)
    copies = [pltpu.make_async_copy(src, dst, sems.at[i]) for i, (src, dst) in enumerate(pairs)]
    for copy in copies:
        copy.start()
    zero = jnp.zeros((PAD, lanes), jnp.float32)

    def clear(p):
        ext[p, :PAD] = zero
        ext[p, PAD + rows :] = zero

    in_groups(planes + 4, clear)
    blank = jnp.zeros((rows, lanes), jnp.float32)
    for p in (0, 1, planes + 2, planes + 3):
        ext[p, PAD : PAD + rows] = blank
    copies[0].wait()

    def fill(p):
        ext[p + 2, PAD : PAD + rows] = u[p].astype(jnp.float32)

    in_groups(planes, fill)
    for copy in copies[1:]:
        copy.wait()
    masks = lane_masks((rows, lanes))
    first = where[3] == 0

    def one(p):
        centre, total = neighbour_sum(ext, (), p + 2, rows, masks)
        prior = jnp.where(first, initial[p].astype(jnp.float32), 0.0)
        part[p] = (
            forcing[p].astype(jnp.float32)
            - centre
            + prior
            - kappa[p].astype(jnp.float32) * (centre_weight * centre - total)
            - reaction[p].astype(jnp.float32) * centre * centre * centre
        )

    in_groups(planes, one)
    for i, p in enumerate((0, 1, planes - 2, planes - 1)):
        rim[i] = kappa[p].astype(jnp.float32)


def residual_kernel(where, part, rim, even_pair, odd_pair, before, out):
    planes, rows, _ = part.shape
    share = out.shape[2]
    per_plane = rows // share
    half = planes // 2

    def put(p, value):
        value = value.astype(jnp.bfloat16)
        side, inner = p // half, p % half
        for piece in range(per_plane):
            out[per_plane * inner + piece, side] = value[piece * share : (piece + 1) * share]

    for p in range(2, planes - 2):
        put(p, part[p] + before[p].astype(jnp.float32))
    upper = where[4] == 1

    def chosen(a, b, i):
        return jnp.where(upper, a[i].astype(jnp.float32), b[i].astype(jnp.float32))

    l0, l1 = (chosen(even_pair, odd_pair, i) for i in range(2))
    h0, h1 = (chosen(odd_pair, even_pair, i) for i in range(2))
    edges = (
        (0, near_weight * l1 + far_weight * l0),
        (1, far_weight * l1),
        (planes - 2, far_weight * h0),
        (planes - 1, near_weight * h0 + far_weight * h1),
    )
    for i, (p, total) in enumerate(edges):
        put(p, part[p] + rim[i] * total + before[p].astype(jnp.float32))


def either_order(where, body, slots):
    @pl.when(where[2] == 0)
    def _():
        body(list(range(slots)))

    @pl.when(where[2] != 0)
    def _():
        body([(j + slots // 2) % slots for j in range(slots)])


def forward_kernel(where, r, out):
    steps, rows, _ = r.shape
    slots = steps // 2

    def body(places):
        for start in range(0, rows, 16):
            part = pl.ds(start, 16)
            scaled = [
                r[n, part].astype(jnp.float32) * (alpha_ratio ** (n / steps)) for n in range(steps)
            ]
            spectrum = real_dft(scaled)
            out[places[0], 0, part] = spectrum[0][0].astype(jnp.bfloat16)
            out[places[0], 1, part] = spectrum[slots][0].astype(jnp.bfloat16)
            for j in range(1, slots):
                out[places[j], 0, part] = spectrum[j][0].astype(jnp.bfloat16)
                out[places[j], 1, part] = spectrum[j][1].astype(jnp.bfloat16)

    either_order(where, body, slots)


def inverse_kernel(where, s, out):
    steps, rows, _ = out.shape
    slots = steps // 2

    def body(places):
        for start in range(0, rows, 16):
            part = pl.ds(start, 16)

            def given(j, c):
                return s[places[j], c, part].astype(jnp.float32)

            spectrum = [(given(0, 0), None)]
            spectrum += [(given(j, 0), given(j, 1)) for j in range(1, slots)]
            spectrum.append((given(0, 1), None))
            values = real_inverse(spectrum)
            for n in range(steps):
                scale = 1.0 / (alpha_ratio ** (n / steps) * steps)
                out[n, part] = (values[n] * scale).astype(jnp.bfloat16)

    either_order(where, body, slots)


def mirrored(core, i, count):
    return jnp.where(core == 0, i, count - 1 - i)


def coefficients(where, inv, kinv):
    slot = where[1]
    factor = math.exp(math.log(alpha_ratio) / STEPS)
    s0 = s1 = si = jnp.float32(0.0)
    for j in range(STEPS // 2):
        phase = 2.0 * math.pi * j / STEPS
        real, imag = 1.0 - factor * math.cos(phase), factor * math.sin(phase)
        hit = slot == j
        s0 = jnp.where(hit, jnp.float32(real), s0)
        s1 = jnp.where(hit, jnp.float32(real if j else 1.0 + factor), s1)
        si = jnp.where(hit, jnp.float32(imag if j else 0.0), si)

    def put(e, kv, iv, rv):
        kv, iv, rv = (v.astype(jnp.float32) for v in (kv, iv, rv))
        base = kv * centre_weight + 3.0 * rv * iv * iv
        d0, d1 = s0 + base, s1 + base
        m0, m1 = d0 * d0 + si * si, d1 * d1 + si * si
        both = 1.0 / (m0 * m1)
        inv0, inv1 = m1 * both, m0 * both
        for c, value in enumerate((d0 * inv0, d1 * inv1, si * inv0)):
            inv[e, c] = value
            kinv[e, c] = kv * value

    return put


def slab_kernel(where, kappa, initial, reaction, inv, kinv):
    planes = kappa.shape[0]
    put = coefficients(where, inv, kinv)

    def own(i):
        put(mirrored(where[0], i, planes), kappa[i], initial[i], reaction[i])

    in_groups(planes, own, 8)


def rim_kernel(where, outer, inner, inv, kinv):
    wide, narrow = outer.shape[1], inner.shape[1]
    core = where[0]
    put = coefficients(where, inv, kinv)

    def far(i):
        put(mirrored(core, i, wide), outer[0, i], outer[1, i], outer[2, i])

    def close(i):
        put(wide + mirrored(core, i, narrow), inner[0, i], inner[1, i], inner[2, i])

    in_groups(wide, far)
    in_groups(narrow, close)


def row_starts(rows):
    return (PAD, 2 * PAD + rows)


def write_band(band):
    double, lanes = band.shape
    row = lax.broadcasted_iota(jnp.int32, (double, lanes), 0)
    row = jnp.where(row >= lanes, row - lanes, row)
    gap = jnp.abs(row - lax.broadcasted_iota(jnp.int32, (double, lanes), 1))
    weights = jnp.where(gap == 1, near_weight, jnp.where(gap == 2, far_weight, 0.0))
    band[...] = weights.astype(jnp.bfloat16)


def fill(core, ref, base, inv, first, x0, x):
    share, rows = ref.shape[2], inv.shape[2]
    per_plane = rows // share
    count = ref.shape[0] // per_plane
    starts = row_starts(rows)

    def body(i):
        place_in = mirrored(core, i, count)
        e = base + place_in
        for h in range(per_plane):
            part = pl.ds(h * share, share)
            re, im = (ref[per_plane * i + h, c].astype(jnp.float32) for c in range(2))
            i0, i1, iq = (inv[first + place_in, c, part] for c in range(3))
            for c, value in enumerate((re * i0 + im * iq, im * i1 - re * iq)):
                x0[e, c, part] = value
                x[e, pl.ds(starts[c] + h * share, share)] = value

    in_groups(count, body, count)


def sweep(step, first, stop, x0, kinvs, band, buffers, emit=None):
    slab, rims = kinvs
    rows = slab.shape[2]
    wide = (x0.shape[0] - slab.shape[0] // 2) // 2
    starts = row_starts(rows)
    src, dst = buffers[step % 2], buffers[(step + 1) % 2]
    weight = sweep_weights()[step]
    group = stop - first
    parts = []
    for u in range(group):
        for start in starts:
            value = src[first + u, pl.ds(start, rows)]
            high = value.astype(jnp.bfloat16)
            low = (value - high.astype(jnp.float32)).astype(jnp.bfloat16)
            parts.append(jnp.concatenate([high, low], axis=1))
    along = jnp.dot(jnp.concatenate(parts, axis=0), band[...], preferred_element_type=jnp.float32)
    for r in range(0, rows, CHUNK):
        columns = [
            [src[first + d, pl.ds(start + r, CHUNK)] for d in range(-2, group + 2)]
            for start in starts
        ]
        for u in range(group):
            e = first + u

            def total(c):
                x = columns[c]
                side = [src[e, pl.ds(starts[c] + r + d, CHUNK)] for d in (1, -1, 2, -2)]
                near = (x[u + 3] + x[u + 1]) + (side[0] + side[1])
                far = (x[u + 4] + x[u]) + (side[2] + side[3])
                k = (2 * u + c) * rows + r
                return scaled(near_weight, near) + scaled(far_weight, far) + along[k : k + CHUNK]

            re, im = columns[0][u + 2], columns[1][u + 2]
            sum_re, sum_im = total(0), total(1)
            part = pl.ds(r, CHUNK)
            if wide <= e < wide + slab.shape[0]:
                k0, k1, kq = (slab[e - wide, c, part] for c in range(3))
            else:
                k_e = e if e < wide else e - slab.shape[0]
                k0, k1, kq = (rims[k_e, c, part] for c in range(3))
            pair = (
                (1.0 - weight) * re + weight * (x0[e, 0, part] + k0 * sum_re + kq * sum_im),
                (1.0 - weight) * im + weight * (x0[e, 1, part] + k1 * sum_im - kq * sum_re),
            )
            for c, value in enumerate(pair):
                if emit is None:
                    dst[e, pl.ds(starts[c] + r, CHUNK)] = value
                else:
                    emit(e, r, c, value)


def inside_kernel(where, y, yb, inv, kinv, x0, xs, xt, band):
    rows, lanes = inv.shape[2:]
    own = y.shape[0] * y.shape[2] // rows
    core = where[0]
    base = (x0.shape[0] - own) // 2
    write_band(band)
    zero = jnp.zeros((PAD, lanes), jnp.float32)

    def clear(e):
        for x in (xs, xt):
            for r in (0, PAD + rows, 2 * (PAD + rows)):
                x[e, pl.ds(r, PAD)] = zero

    in_groups(x0.shape[0], clear)
    fill(core, y, base, inv, 0, x0, xs)
    fill(core, yb, base + own, inv, own, x0, xs)
    for step in range(EARLY):
        edge = 2 * (step + 1)
        sweep(step, base + edge, base + 2 * own - edge, x0, (kinv, None), band, (xs, xt))


def sweeps_kernel(where, y_a, yc, yd, kslab, inv, krim, _x0, _xs, _xt, out, x0, xs, xt, band):
    rows, _ = inv.shape[2:]
    ext = x0.shape[0]
    share = y_a.shape[2]
    per_plane = rows // share
    own = y_a.shape[0] // per_plane
    core = where[0]
    base = (ext - own) // 2
    kinv = (kslab, krim)
    write_band(band)
    fill(core, y_a, base - own, inv, base - own, x0, xs)
    fill(core, yc, 0, inv, 0, x0, xs)
    fill(core, yd, base + 2 * own, inv, base, x0, xs)

    def emit(e, r, c, value):
        i = mirrored(core, e - base, own)
        out[per_plane * i + r // share, c, pl.ds(r % share, CHUNK)] = value.astype(jnp.bfloat16)

    for step in range(SWEEPS):
        edge = 2 * (step + 1)
        if step < EARLY:
            sweep(step, edge, base + edge, x0, kinv, band, (xs, xt))
            sweep(step, base + 2 * own - edge, ext - edge, x0, kinv, band, (xs, xt))
        else:
            last = step == SWEEPS - 1
            sweep(step, edge, ext - edge, x0, kinv, band, (xs, xt), emit if last else None)


def final_kernel(state, correction, out):
    planes, rows, _ = state.shape
    share = correction.shape[2]
    per_plane = rows // share
    half = planes // 2

    for p in range(planes):
        part, inner = p // half, p % half
        value = jnp.concatenate(
            [
                correction[per_plane * inner + h, part].astype(jnp.float32)
                for h in range(per_plane)
            ],
            axis=0,
        )
        out[p] = (state[p].astype(jnp.float32) + value).astype(jnp.bfloat16)


def place():
    slots = lax.axis_size(CHIPS)
    side, chip, core = (lax.axis_index(a) for a in TM)
    slab = lax.axis_index("space")
    per_side = lax.axis_size("tm_1")
    flip = slab // 2 % 2
    slot = (side * per_side + chip + flip * (slots // 2)) % slots
    timestep = (side * per_side + chip) * lax.axis_size("tm_2") + core
    return core, slot, flip, timestep, slab % 2


def placed(kernel):
    return lambda *refs: kernel(place(), *refs)


def call(kernel, shapes, inputs, scratch=(), anywhere=0, flops=None, aliases=None):
    outs = [jax.ShapeDtypeStruct(s, d) for s, d in shapes]
    cost = None
    if flops is not None:
        cost = pl.CostEstimate(flops=flops, transcendentals=0, bytes_accessed=flops // 8)
    rest = len(inputs) - anywhere
    return pl.pallas_call(
        kernel,
        out_shape=outs,
        in_specs=[HBM] * anywhere + [VMEM] * rest,
        out_specs=[VMEM] * len(outs),
        scratch_shapes=list(scratch),
        cost_estimate=cost,
        input_output_aliases=aliases or {},
        compiler_params=pltpu.CompilerParams(vmem_limit_bytes=24 << 20),
    )(*inputs)


def iteration(state, initial, forcing, kappa, reaction):
    _, planes, rows, lanes = state.shape
    members = lax.axis_size(TM)
    slots = lax.axis_size(CHIPS)
    slabs = lax.axis_size("space")
    own = planes // 2
    share = own * rows // slots
    per_plane = rows // share
    wide = 2 * SWEEPS
    narrow = wide - own
    ext = own + 2 * wide
    bf16, f32 = jnp.bfloat16, jnp.float32
    core = lax.axis_index("tm_2")
    u = state[0]

    outer, same = [], []
    for side in range(2):
        for t in range(slabs - 1):
            near, beside = side * 2 * slabs, (side ^ (t % 2)) * 2 * slabs
            low, high = near + slabs + t, beside + t + 1
            outer += [(low, high), (high, low)]
            same += [(near + t, beside + t + 1), (beside + slabs + t + 1, near + slabs + t)]
    swap = [(i, slabs + i) for i in range(slabs)] + [(slabs + i, i) for i in range(slabs)]
    odd = lax.axis_index("space") % 2
    even_first = [p for s in range(0, slabs - 1, 2) for p in ((s, s + 1), (s + 1, s))]
    odd_first = [p for s in range(1, slabs - 1, 2) for p in ((s, s + 1), (s + 1, s))]
    low, high = u[:2], u[planes - 2 :]
    even_pair = lax.ppermute(jnp.where(odd == 1, low, high), "space", even_first)
    odd_pair = lax.ppermute(jnp.where(odd == 1, high, low), "space", odd_first)
    before = lax.ppermute(u, TM, [(i, i + 1) for i in range(members - 1)])
    coefs = jnp.stack([kappa, initial, reaction])
    rim = jnp.where(core == 0, coefs[:, :wide], coefs[:, planes - wide :])
    rim = lax.ppermute(rim, SIDE_CORE_SPACE, outer)
    inner = jnp.where(core == 0, rim[:, wide - narrow :], rim[:, :narrow])
    inner = lax.ppermute(inner, CORE_SPACE, swap)

    block = ((planes, rows, lanes), bf16)
    part, edge = call(
        placed(local_kernel),
        [((planes, rows, lanes), f32), ((4, rows, lanes), f32)],
        [
            pltpu.with_memory_space_constraint(v, pltpu.HBM)
            for v in (u, initial, forcing[0], kappa, reaction)
        ],
        [pltpu.VMEM((planes + 4, rows + 2 * PAD, lanes), f32)]
        + [pltpu.VMEM(*block)] * 5
        + [pltpu.SemaphoreType.DMA((5,))],
        anywhere=5,
        flops=20_000_000,
    )
    (residual,) = call(
        placed(residual_kernel),
        [((slots, 2, share, lanes), bf16)],
        [part, edge, even_pair, odd_pair, before],
    )
    cells = lax.all_to_all(residual.reshape(members, share, lanes), TM, 0, 0, tiled=True)
    (spectrum,) = call(placed(forward_kernel), [((slots, 2, share, lanes), bf16)], [cells])
    y = lax.all_to_all(spectrum, CHIPS, 0, 0, tiled=True)

    table = [((planes, 3, rows, lanes), f32)] * 2
    inv_slab, kinv_slab = call(placed(slab_kernel), table, [kappa, initial, reaction])
    table = [((wide + narrow, 3, rows, lanes), f32)] * 2
    inv_rim, kinv_rim = call(placed(rim_kernel), table, [rim, inner])
    n = per_plane * narrow
    first = core == 0
    ya = lax.ppermute(y, SIDE_CORE_SPACE, outer)
    yc = lax.ppermute(jnp.where(first, y[-n:], y[:n]), SIDE_CORE_SPACE, same)
    yb = lax.ppermute(y, CORE_SPACE, swap)
    yd = lax.ppermute(jnp.where(first, ya[-n:], ya[:n]), CORE_SPACE, swap)
    tall = 2 * rows + 3 * PAD
    buffers = [((ext, 2, rows + PAD, lanes), f32), ((ext, tall, lanes), f32), ((ext, tall, lanes), f32)]
    band = [pltpu.VMEM((2 * lanes, lanes), bf16)]
    state_arrays = call(placed(inside_kernel), buffers, [y, yb, inv_slab, kinv_slab], band)
    solved = call(
        placed(sweeps_kernel),
        [((slots, 2, share, lanes), bf16), *buffers],
        [ya, yc, yd, kinv_slab, inv_rim, kinv_rim, *state_arrays],
        band,
        aliases={6: 1, 7: 2, 8: 3},
    )[0]
    modes = lax.all_to_all(solved, CHIPS, 0, 0, tiled=True)
    (correction,) = call(placed(inverse_kernel), [((members, share, lanes), bf16)], [modes])
    returned = lax.all_to_all(correction, TM, 0, 0, tiled=True)
    (updated,) = call(
        final_kernel, [((planes, rows, lanes), bf16)], [u, returned.reshape(slots, 2, share, lanes)]
    )
    return updated[None]


def solution(mesh):
    torus = Mesh(
        mesh.devices.reshape(2, 8, 2, mesh.shape["space"]), ("tm_0", "tm_1", "tm_2", "space")
    )
    in_specs = (
        P(TM, "space", None, None),
        P("space", None, None),
        P(TM, "space", None, None),
        P("space", None, None),
        P("space", None, None),
    )
    out_specs = P(TM, "space", None, None)
    return jax.shard_map(
        iteration, mesh=torus, in_specs=in_specs, out_specs=out_specs, check_vma=False
    )
```
